16 devices in a mesh: row: 2 (over z), col: 8 (over y, x, core).
Axes of the slice: x: 2, y: 2, z: 2, core: 2. Of those that a mesh axis runs over, the one named last changes fastest.
Arguments:
- v_mat: float32 [8192, 8192], P('row', 'col')
- t_fac: float32 [64, 128, 128], P('col')
- z_vec: float32 [8192, 2048], P(None, ('col', 'row'))
Outputs:
- output: float32 [8192, 2048], P('row', 'col')
All inputs are finite; a program needn't handle non-finite values.
Results may differ from the reference program's by a relative error of at most 0.001.
Values sent between devices are 32-bit elements.
A program may use at most 1 GiB of HBM per device.

```python
import jax
import jax.numpy as jnp
from jax import lax

MAT_ORDER = 8192
PANEL_WIDTH = 128
NUM_VECTORS = 2048
ROW_SHARDS = 2
COL_SHARDS = 8


def stored_to_global(mat_order, panel_width, shards):
    stored_idx = jnp.arange(mat_order, dtype=jnp.int32)
    per_shard = mat_order // shards
    shard_idx = stored_idx // per_shard
    within = stored_idx % per_shard
    block_idx = within // panel_width
    offset = within % panel_width
    return (block_idx * shards + shard_idx) * panel_width + offset


def build_factors(v_mat):
    panels = v_mat.reshape(MAT_ORDER, MAT_ORDER // PANEL_WIDTH, PANEL_WIDTH)
    gram_mat = jnp.einsum('nsb,nse->sbe', panels, panels)
    half_diag = 0.5 * jnp.diagonal(gram_mat, axis1=1, axis2=2)
    inv_factor = jnp.triu(gram_mat, 1) + half_diag[:, :, None] * jnp.eye(PANEL_WIDTH, dtype=jnp.float32)
    return jnp.triu(jnp.linalg.inv(inv_factor))


def setup_inputs(seed: int = 0) -> dict:
    rng_key = jax.random.key(seed)
    key_v, key_z = jax.random.split(rng_key)
    raw_vals = jax.random.normal(key_v, (MAT_ORDER, MAT_ORDER), jnp.float32)
    row_ids = stored_to_global(MAT_ORDER, PANEL_WIDTH, ROW_SHARDS)[:, None]
    col_ids = stored_to_global(MAT_ORDER, PANEL_WIDTH, COL_SHARDS)[None, :]
    unit_diag = (row_ids == col_ids).astype(jnp.float32)
    v_mat = jnp.where(row_ids > col_ids, raw_vals, unit_diag)
    t_fac = build_factors(v_mat)
    z_vec = jax.random.normal(key_z, (MAT_ORDER, NUM_VECTORS), jnp.float32)
    return {'v_mat': v_mat, 't_fac': t_fac, 'z_vec': z_vec}


def reference(v_mat, t_fac, z_vec):
    num_panels = MAT_ORDER // PANEL_WIDTH
    local_panels = num_panels // COL_SHARDS

    def apply_panel(x_cur, panel_idx):
        panel_slot = (panel_idx % COL_SHARDS) * local_panels + panel_idx // COL_SHARDS
        v_pan = lax.dynamic_slice_in_dim(v_mat, panel_slot * PANEL_WIDTH, PANEL_WIDTH, axis=1)
        t_pan = lax.dynamic_index_in_dim(t_fac, panel_slot, axis=0, keepdims=False)
        w_blk = jnp.dot(v_pan.T, x_cur, preferred_element_type=jnp.float32)
        y_blk = jnp.dot(t_pan, w_blk, preferred_element_type=jnp.float32)
        x_new = x_cur - jnp.dot(v_pan, y_blk, preferred_element_type=jnp.float32)
        return x_new, None

    x_out, _ = lax.scan(apply_panel, z_vec, jnp.arange(num_panels - 1, -1, -1))
    return x_out
```

```python
import functools

import jax
import jax.numpy as jnp
from jax import lax
from jax.experimental import pallas as pl
from jax.experimental.pallas import tpu as pltpu
from jax.sharding import PartitionSpec as P

F32 = jnp.float32
BF16 = jnp.bfloat16
MESH_ID = pl.DeviceIdType.MESH

NB = 128
PW = 2 * NB
CH = 4 * NB
RING = 4


def split3(x):
    hi = x.astype(BF16)
    rest = x - hi.astype(F32)
    mid = rest.astype(BF16)
    low = (rest - mid.astype(F32)).astype(BF16)
    return hi, mid, low


def mm(a, b):
    return lax.dot_general(a, b, (((1,), (0,)), ((), ())), preferred_element_type=F32)


def mm_nt(a, b):
    return lax.dot_general(a, b, (((1,), (1,)), ((), ())), preferred_element_type=F32)


def stacked(dot, a3, b_hi, b_mid, b_low):
    m = a3.shape[0] // 3
    r = dot(a3, b_hi)
    s = r[0:m] + r[m : 2 * m] + r[2 * m : 3 * m]
    r = dot(a3[0 : 2 * m], b_mid)
    s = s + r[0:m] + r[m : 2 * m]
    return s + dot(a3[0:m], b_low)


def full_dot(dot, a, b):
    ah, am, al = split3(a)
    bh, bm, bl = split3(b)
    return stacked(dot, jnp.concatenate([ah, am, al], axis=0), bh, bm, bl)


def body(nsb, v_ref, t_ref, z_ref, out_ref, vb, *s):
    (zl, xt, xp, vf, vn, tb, tp, ws, wr, gs, gr, yp,
     z_loc, z_snd, z_rcv, i_rcv, d_rcv, w_snd, w_rcv, g_snd, g_rcv, ld, o_sem, i_snd, d_snd) = s
    rows = nsb * CH
    npair = nsb * RING
    r = lax.axis_index("row")
    col = lax.axis_index("col")
    q = col % 2
    k = col // 2
    ky, kx = k // 2, k % 2
    rho = 2 * ky + (kx + ky) % 2

    def at_ring(i):
        i = i % RING
        y = i // 2
        x = (i % 2 + y) % 2
        return (r, (y * 2 + x) * 2 + q)

    partner = (r, k * 2 + 1 - q)
    across = (1 - r, col)

    def pair_of(t):
        return npair - 1 - t

    def sb_of(t):
        return pair_of(t) // RING

    def owner_dist(t):
        kk = pair_of(t) % RING
        y = kk // 2
        ro = 2 * y + (kk % 2 + y) % 2
        return (rho - ro + RING) % RING

    def by_chunk(t, c, fn):
        l = sb_of(t)
        kk = pair_of(t) % RING

        @pl.when(c > l)
        def _():
            fn(pl.multiple_of(c * CH, CH), CH)

        for j in range(RING):

            @pl.when((c == l) & (kk == j))
            def _(j=j):
                fn(pl.multiple_of(c * CH + j * NB, NB), CH - j * NB)

    def own_rows(t, r0, n):
        return v_ref.at[pl.ds(r0, n), pl.ds(pl.multiple_of(sb_of(t) * NB, NB), NB)]

    def copy(src, dst, ssem, rsem, dev):
        return pltpu.make_async_remote_copy(src, dst, ssem, rsem, device_id=dev, device_id_type=MESH_ID)

    def ici(t, c, r0, n, half, own):
        src = own_rows(t, r0, n) if own else vb.at[q, pair_of(t), pl.ds(r0, n), :]
        return copy(src, vb.at[q, pair_of(t), pl.ds(r0, n), :], i_snd.at[t % 8, c], i_rcv.at[t, c],
                    at_ring(rho + 1 - 2 * half + RING))

    def d2d(t, c, r0, n, own):
        src = own_rows(t, r0, n) if own else vb.at[q, pair_of(t), pl.ds(r0, n), :]
        return copy(src, vb.at[q, pair_of(t), pl.ds(r0, n), :], d_snd.at[t % 8, c], d_rcv.at[t, c], partner)

    def ici_t(t, own):
        src = t_ref.at[sb_of(t)] if own else tb.at[q, pair_of(t)]
        return copy(src, tb.at[q, pair_of(t)], i_snd.at[t % 8, nsb], i_rcv.at[t, nsb], at_ring(rho - 1 + RING))

    def d2d_t(t, own):
        src = t_ref.at[sb_of(t)] if own else tb.at[q, pair_of(t)]
        return copy(src, tb.at[q, pair_of(t)], d_snd.at[t % 8, nsb], d_rcv.at[t, nsb], partner)

    def wait_sent(t, c, ring):
        def fn(r0, n):
            if ring:
                ici(t, c, r0, n, 0, False).wait_send()
            d2d(t, c, r0, n, False).wait_send()

        by_chunk(t, c, fn)

    def wait_sent_t(t, ring):
        if ring:
            ici_t(t, False).wait_send()
        d2d_t(t, False).wait_send()

    def send_own(t):
        l = sb_of(t)

        def one(c, _):
            half = (c - l) % 2

            @pl.when((t >= 8) & (c >= sb_of(t - 8)))
            def _():
                wait_sent(t - 8, c, True)

            def fn(r0, n):
                ici(t, c, r0, n, half, True).start()
                d2d(t, c, r0, n, True).start()

            by_chunk(t, c, fn)
            return 0

        lax.fori_loop(l, nsb, one, 0)

        @pl.when(t >= 8)
        def _():
            wait_sent_t(t - 8, True)

        ici_t(t, True).start()
        d2d_t(t, True).start()

    def pass_on(t, half, hop):
        l = sb_of(t)
        forward = hop < RING - 1

        def one(i, _):
            c = l + half + 2 * i

            def got(r0, n):
                ici(t, c, r0, n, half, False).wait_recv()

            by_chunk(t, c, got)

            @pl.when((t >= 8) & (c >= sb_of(t - 8)))
            def _():
                @pl.when(forward)
                def _():
                    wait_sent(t - 8, c, True)

                @pl.when(jnp.logical_not(forward))
                def _():
                    wait_sent(t - 8, c, False)

            def fn(r0, n):
                d2d(t, c, r0, n, False).start()

                @pl.when(forward)
                def _():
                    ici(t, c, r0, n, half, False).start()

            by_chunk(t, c, fn)
            return 0

        lax.fori_loop(0, (nsb - l - half + 1) // 2, one, 0)

        @pl.when(half == 1)
        def _():
            ici_t(t, False).wait_recv()

            @pl.when(t >= 8)
            def _():
                @pl.when(forward)
                def _():
                    wait_sent_t(t - 8, True)

                @pl.when(jnp.logical_not(forward))
                def _():
                    wait_sent_t(t - 8, False)

            d2d_t(t, False).start()

            @pl.when(forward)
            def _():
                ici_t(t, False).start()

    def service(slot):
        def hops(j, _):
            hop = RING - 1 - j // 2
            half = j % 2
            t = slot + 6 - 2 * hop
            d = owner_dist(t)
            arrives = jnp.where(half == 0, d, RING - d)

            @pl.when((t >= 0) & (t < npair) & (arrives == hop))
            def _():
                pass_on(t, half, hop)

            return 0

        lax.fori_loop(0, 6, hops, 0)
        t = slot + 6

        @pl.when((t >= 0) & (t < npair) & (owner_dist(t) == 0))
        def _():
            send_own(t)

    def lead(i):
        return jnp.clip(jnp.minimum(i + 1, (24 - i) // 4), 0, 2)

    def last_slot(i):
        return jnp.minimum(i + 1 + lead(i), npair - 1)

    def z_copies(c):
        r0 = pl.multiple_of(c * CH, CH)
        mine = pl.multiple_of(r * rows + c * CH, CH)
        theirs = pl.multiple_of((1 - r) * rows + c * CH, CH)
        loc = pltpu.make_async_copy(z_ref.at[pl.ds(mine, CH), :], zl.at[r, pl.ds(r0, CH), :], z_loc.at[c])
        rem = copy(z_ref.at[pl.ds(theirs, CH), :], zl.at[r, pl.ds(r0, CH), :], z_snd.at[c], z_rcv.at[c], across)
        return loc, rem

    def start_z(c):
        loc, rem = z_copies(c)
        loc.start()
        rem.start()

    def admit(c):
        loc, rem = z_copies(c)
        loc.wait()
        rem.wait()
        r0 = pl.multiple_of(c * CH, CH)

        def one(g, _):
            x = zl[g, pl.ds(r0, CH), :].T
            xt[g, :, pl.ds(r0, CH)] = x
            h, m, lo = split3(x)
            xp[g, 0:NB, pl.ds(r0, CH)] = h
            xp[g, NB : 2 * NB, pl.ds(r0, CH)] = m
            xp[g, 2 * NB : 3 * NB, pl.ds(r0, CH)] = lo
            return 0

        lax.fori_loop(0, 2, one, 0)

    def load(t, c, side, r0, n):
        src = vb.at[side, pair_of(t), pl.ds(r0, n), :]
        return pltpu.make_async_copy(
            src, vf.at[pl.ds(r0, n), pl.ds(pl.multiple_of(side * NB, NB), NB)], ld.at[side, c])

    def load_own(t, c, r0, n):
        return pltpu.make_async_copy(
            own_rows(t, r0, n), vf.at[pl.ds(r0, n), pl.ds(pl.multiple_of(q * NB, NB), NB)], ld.at[q, c])

    def t_own(t):
        return pltpu.make_async_copy(t_ref.at[sb_of(t)], tb.at[q, pair_of(t)], ld.at[q, nsb])

    def start_loads(t):
        l = sb_of(t)
        mine = owner_dist(t) == 0

        def one(c, _):
            def fn(r0, n):
                @pl.when(mine)
                def _():
                    load_own(t, c, r0, n).start()

                @pl.when(jnp.logical_not(mine))
                def _():
                    load(t, c, q, r0, n).start()

                d2d(t, c, r0, n, False).wait_recv()
                load(t, c, 1 - q, r0, n).start()

            by_chunk(t, c, fn)
            return 0

        lax.fori_loop(l, nsb, one, 0)

        @pl.when(mine)
        def _():
            t_own(t).start()

        d2d_t(t, False).wait_recv()

    def prep(t):
        l = sb_of(t)
        first = pair_of(t) * NB
        slot = t % 2

        def one(c, _):
            def fn(r0, n):
                load(t, c, 0, r0, n).wait()
                load(t, c, 1, r0, n).wait()

            by_chunk(t, c, fn)

            def sub(j, _):
                r0 = pl.multiple_of(c * CH + j * NB, NB)
                x = vf[pl.ds(r0, NB), :]
                x = jnp.where(lax.broadcasted_iota(jnp.int32, (NB, PW), 0) + r0 >= first, x, 0.0)
                h, m, lo = split3(x)
                vn[slot, pl.ds(r0, NB), 0:PW] = h
                vn[slot, pl.ds(r0, NB), PW : 2 * PW] = m
                vn[slot, pl.ds(r0, NB), 2 * PW : 3 * PW] = lo
                return 0

            lax.fori_loop(0, CH // NB, sub, 0)
            return 0

        lax.fori_loop(l, nsb, one, 0)

        @pl.when(owner_dist(t) == 0)
        def _():
            t_own(t).wait()

    def gram_copy(t):
        return copy(gs.at[t % 2], gr.at[t % 2], g_snd.at[t % 2], g_rcv.at[t % 2], across)

    def gram(t):
        slot = t % 2

        @pl.when(t >= 2)
        def _():
            gram_copy(t - 2).wait_send()

        gs[slot] = jnp.zeros((NB, NB), F32)

        def one(c, _):
            r0 = pl.multiple_of(c * CH, CH)
            a3 = jnp.concatenate(
                [vn[slot, pl.ds(r0, CH), i * PW : i * PW + NB].T for i in range(3)], axis=0)
            b = [vn[slot, pl.ds(r0, CH), i * PW + NB : (i + 1) * PW] for i in range(3)]
            gs[slot] += stacked(mm, a3, *b)
            return 0

        lax.fori_loop(sb_of(t), nsb, one, 0)
        gram_copy(t).start()

    def block_factor(t):
        slot = t % 2
        gram_copy(t).wait_recv()
        g = gs[slot] + gr[slot]
        ta = tb[0, pair_of(t)]
        tbb = tb[1, pair_of(t)]
        upper = -full_dot(mm, ta, full_dot(mm, g, tbb))
        for i, piece in enumerate(split3(ta)):
            tp[0:NB, i * PW : i * PW + NB] = piece
        for i, piece in enumerate(split3(upper)):
            tp[0:NB, i * PW + NB : (i + 1) * PW] = piece
        for i, piece in enumerate(split3(tbb)):
            tp[NB:PW, i * PW : i * PW + NB] = jnp.zeros((NB, NB), BF16)
            tp[NB:PW, i * PW + NB : (i + 1) * PW] = piece

    def w_copy(t, g):
        return copy(ws.at[t % 2, g], wr.at[t % 2, g], w_snd.at[t % 2, g], w_rcv.at[t % 2, g], across)

    def coefficients(t, g):
        w_copy(t, g).wait_recv()
        w = ws[t % 2, g] + wr[t % 2, g]
        y = stacked(mm_nt, jnp.concatenate(split3(w), axis=0),
                    tp[:, 0:PW], tp[:, PW : 2 * PW], tp[:, 2 * PW : 3 * PW])
        h, m, lo = split3(y)
        yp[0:NB] = h
        yp[NB : 2 * NB] = m
        yp[2 * NB : 3 * NB] = lo

    def update(t, g, c):
        r0 = pl.multiple_of(c * CH, CH)
        slot = t % 2
        b = [vn[slot, pl.ds(r0, CH), i * PW : (i + 1) * PW] for i in range(3)]
        x = xt[g, :, pl.ds(r0, CH)] - stacked(mm_nt, yp[...], *b)
        xt[g, :, pl.ds(r0, CH)] = x
        h, m, lo = split3(x)
        xp[g, 0:NB, pl.ds(r0, CH)] = h
        xp[g, NB : 2 * NB, pl.ds(r0, CH)] = m
        xp[g, 2 * NB : 3 * NB, pl.ds(r0, CH)] = lo

    def product(t, g, c):
        r0 = pl.multiple_of(c * CH, CH)
        slot = t % 2
        b = [vn[slot, pl.ds(r0, CH), i * PW : (i + 1) * PW] for i in range(3)]
        ws[slot, g] += stacked(mm, xp[g, :, pl.ds(r0, CH)], *b)

    def both(i, g):
        c0 = sb_of(i)
        c1 = sb_of(i + 1)
        n = i + 1
        update(i, g, c0)

        @pl.when(c1 < c0)
        def _():
            product(n, g, c1)

        def one(c, _):
            product(n, g, c - 1)
            update(i, g, c)
            return 0

        lax.fori_loop(c0 + 1, nsb, one, 0)
        product(n, g, nsb - 1)

    def step(i, _):
        n = i + 1

        @pl.when(i >= 0)
        def _():
            @pl.when((i % RING == 0) & (i // RING + 2 < nsb))
            def _():
                start_z(nsb - 1 - (i // RING + 2))

        @pl.when(n < npair)
        def _():
            first = jnp.where(i < 0, -6, last_slot(i - 1) + 1)
            lax.fori_loop(first, last_slot(i) + 1, lambda slot, _: (service(slot), 0)[1], 0)
            start_loads(n)

        @pl.when(i >= 0)
        def _():
            block_factor(i)

        @pl.when(n < npair)
        def _():
            prep(n)
            gram(n)

            @pl.when(n % RING == 0)
            def _():
                admit(sb_of(n))

        def group(g, _):
            @pl.when(i >= 0)
            def _():
                coefficients(i, g)

            @pl.when(n < npair)
            def _():
                @pl.when(n >= 2)
                def _():
                    w_copy(n - 2, g).wait_send()

                ws[n % 2, g] = jnp.zeros((NB, PW), F32)

            @pl.when(i < 0)
            def _():
                product(n, g, nsb - 1)

            @pl.when((i >= 0) & (n < npair))
            def _():
                both(i, g)

            @pl.when(n < npair)
            def _():
                w_copy(n, g).start()

            @pl.when(n == npair)
            def _():
                def one(c, _):
                    update(i, g, c)
                    r0 = pl.multiple_of(c * CH, CH)
                    zl[g, pl.ds(r0, CH), :] = xt[g, :, pl.ds(r0, CH)].T
                    out_copy(g, c).start()
                    return 0

                lax.fori_loop(0, nsb, one, 0)

            return 0

        lax.fori_loop(0, 2, group, 0)
        return 0

    def out_copy(g, c):
        r0 = pl.multiple_of(c * CH, CH)
        return pltpu.make_async_copy(
            zl.at[g, pl.ds(r0, CH), :],
            out_ref.at[pl.ds(r0, CH), pl.ds(pl.multiple_of(g * NB, NB), NB)], o_sem.at[g, c])

    barrier = pltpu.get_barrier_semaphore()
    for dev in (at_ring(rho + 1), at_ring(rho + RING - 1), partner, across):
        pl.semaphore_signal(barrier, inc=1, device_id=dev, device_id_type=MESH_ID)
    pl.semaphore_wait(barrier, 4)

    start_z(nsb - 1)
    if nsb > 1:
        start_z(nsb - 2)
    lax.fori_loop(-1, npair, step, 0)

    for t in (npair - 2, npair - 1):
        gram_copy(t).wait_send()
        for g in range(2):
            w_copy(t, g).wait_send()

    def drain(t, _):
        d = owner_dist(t)

        def one(c, _):
            half = (c - sb_of(t)) % 2
            hop = jnp.where(half == 0, d, (RING - d) % RING)

            @pl.when(hop < RING - 1)
            def _():
                wait_sent(t, c, True)

            @pl.when(hop == RING - 1)
            def _():
                wait_sent(t, c, False)

            return 0

        lax.fori_loop(sb_of(t), nsb, one, 0)

        @pl.when(d != 1)
        def _():
            wait_sent_t(t, True)

        @pl.when(d == 1)
        def _():
            wait_sent_t(t, False)

        return 0

    lax.fori_loop(max(0, npair - 8), npair, drain, 0)

    def out_done(c, _):
        for g in range(2):
            out_copy(g, c).wait()
        return 0

    lax.fori_loop(0, nsb, out_done, 0)


def solution(mesh):
    def local(v, t, z):
        rows, cols = v.shape
        nsb = cols // NB
        npair = nsb * RING
        dma = pltpu.SemaphoreType.DMA
        hbm = pl.BlockSpec(memory_space=pltpu.MemorySpace.HBM)
        out, _ = pl.pallas_call(
            functools.partial(body, nsb),
            out_shape=(
                jax.ShapeDtypeStruct((rows, PW), F32),
                jax.ShapeDtypeStruct((2, npair, rows, NB), F32),
            ),
            in_specs=[hbm] * 3,
            out_specs=(hbm, hbm),
            scratch_shapes=[
                pltpu.VMEM((2, rows, NB), F32),
                pltpu.VMEM((2, NB, rows), F32),
                pltpu.VMEM((2, 3 * NB, rows), BF16),
                pltpu.VMEM((rows, PW), F32),
                pltpu.VMEM((2, rows, 3 * PW), BF16),
                pltpu.VMEM((2, npair, NB, NB), F32),
                pltpu.VMEM((PW, 3 * PW), BF16),
                pltpu.VMEM((2, 2, NB, PW), F32),
                pltpu.VMEM((2, 2, NB, PW), F32),
                pltpu.VMEM((2, NB, NB), F32),
                pltpu.VMEM((2, NB, NB), F32),
                pltpu.VMEM((3 * NB, PW), BF16),
                dma((nsb,)),
                dma((nsb,)),
                dma((nsb,)),
                dma((npair, nsb + 1)),
                dma((npair, nsb + 1)),
                dma((2, 2)),
                dma((2, 2)),
                dma((2,)),
                dma((2,)),
                dma((2, nsb + 1)),
                dma((2, nsb)),
                dma((8, nsb + 1)),
                dma((8, nsb + 1)),
            ],
            compiler_params=pltpu.CompilerParams(
                collective_id=0, has_side_effects=True, vmem_limit_bytes=60 * 2**20),
            name="backtransform",
        )(v, t, z)
        return out

    return jax.shard_map(local, mesh=mesh,
                         in_specs=(P("row", "col"), P("col", None, None), P(None, ("col", "row"))),
                         out_specs=P("row", "col"), check_vma=False)
```

```python
import functools

import jax
import jax.numpy as jnp
from jax import lax
from jax.experimental import pallas as pl
from jax.experimental.pallas import tpu as pltpu
from jax.sharding import PartitionSpec as P

F32 = jnp.float32
BF16 = jnp.bfloat16
MESH_ID = pl.DeviceIdType.MESH

NB = 128
PW = 2 * NB
CH = 4 * NB
BIG = 2 * CH
RING = 4
OWN_LEAD = 12


def split3(x):
    hi = x.astype(BF16)
    rest = x - hi.astype(F32)
    mid = rest.astype(BF16)
    low = (rest - mid.astype(F32)).astype(BF16)
    return hi, mid, low


def mm(a, b):
    return lax.dot_general(a, b, (((1,), (0,)), ((), ())), preferred_element_type=F32)


def mm_nt(a, b):
    return lax.dot_general(a, b, (((1,), (1,)), ((), ())), preferred_element_type=F32)


def add_rows(total, x, n):
    for i in range(0, x.shape[0], n):
        part = x[i : i + n]
        total = part if total is None else total + part
    return total


def stacked(dot, a3, b):
    m = a3.shape[0] // 3
    s = None
    for i in range(3):
        s = add_rows(s, dot(a3[0 : (3 - i) * m], b[i]), m)
    return s


def full_dot(dot, a, b):
    return stacked(dot, jnp.concatenate(split3(a), axis=0), split3(b))


def body(nsb, v_ref, t_ref, z_ref, out_ref, vb, *scratch):
    rows = nsb * CH
    dma = pltpu.SemaphoreType.DMA
    npair = nsb * RING
    nc = nsb + 2
    pl.run_scoped(
        functools.partial(run, nsb, rows, npair, v_ref, t_ref, z_ref, out_ref, vb, scratch),
        dma((nsb,)),
        dma((nsb,)),
        dma((nsb,)),
        dma((npair, nc)),
        dma((npair, nc)),
        dma((2, 2)),
        dma((2, 2)),
        dma((2,)),
        dma((2,)),
        dma((8,)),
        dma((8,)),
        dma((2, nc)),
        dma((2, nsb)),
        dma((2, 8, nc)),
        dma((8, nc)),
        dma((2, nsb)),
    )


def run(nsb, rows, npair, v_ref, t_ref, z_ref, out_ref, vb, scratch, *sems):
    (zl, xt, xp, vf, vn, tb, tc, tp, ws, wr, gs, gr, gf, yp, eb, et) = scratch
    (z_loc, z_snd, z_rcv, i_rcv, d_rcv, w_snd, w_rcv, g_snd, g_rcv, f_snd, f_rcv, ld, o_sem, i_snd, d_snd, h_sem) = sems
    HEAD, TEE = nsb, nsb + 1
    r = lax.axis_index("row")
    col = lax.axis_index("col")
    q = col % 2
    k = col // 2
    ky, kx = k // 2, k % 2
    rho = 2 * ky + (kx + ky) % 2

    def at_ring(i):
        i = i % RING
        y = i // 2
        x = (i % 2 + y) % 2
        return (r, (y * 2 + x) * 2 + q)

    partner = (r, k * 2 + 1 - q)
    across = (1 - r, col)
    apart = (r == 1) & (q == 0)

    def pair_of(t):
        return npair - 1 - t

    def sb_of(t):
        return pair_of(t) // RING

    def chip_of(t):
        return pair_of(t) % RING

    def owner_dist(t):
        kk = chip_of(t)
        y = kk // 2
        ro = 2 * y + (kk % 2 + y) % 2
        return (rho - ro + RING) % RING

    def height(t):
        return nsb - sb_of(t)

    def half_of(t, c):
        return (c - sb_of(t) + (height(t) - 1) // 2) % 2

    def head_half(t):
        return height(t) % 2

    def partial(t, fn):
        kk = chip_of(t)
        for j in range(RING - 1):

            @pl.when(kk == j)
            def _(j=j):
                fn(pl.multiple_of(sb_of(t) * CH + (j + 1) * NB, NB), CH - (j + 1) * NB)

    def full(t, fn):
        def one(c, _):
            fn(c, pl.multiple_of(c * CH, CH), CH)
            return 0

        lax.fori_loop(sb_of(t) + 1, nsb, one, 0)

    def head_rows(t):
        return pl.ds(pl.multiple_of(pair_of(t) * NB, NB), NB)

    def lanes(l):
        return pl.ds(pl.multiple_of(l * NB, NB), NB)

    def rcopy(src, dst, ssem, rsem, dev):
        return pltpu.make_async_remote_copy(src, dst, ssem, rsem, device_id=dev, device_id_type=MESH_ID)

    def panel(t, r0, n, own):
        if own:
            return v_ref.at[pl.ds(r0, n), lanes(sb_of(t))]
        return vb.at[q, pair_of(t), pl.ds(r0, n), :]

    def side_copy(src, dst, t, c, d):
        return rcopy(src, dst, i_snd.at[d, t % 8, c], i_rcv.at[t, c], at_ring(rho + 1 - 2 * d + RING))

    def core_copy(src, dst, t, c):
        return rcopy(src, dst, d_snd.at[t % 8, c], d_rcv.at[t, c], partner)

    def ends(t, c, own, r0=None, n=None):
        if c is HEAD:
            dst = vb.at[q, pair_of(t), head_rows(t), :]
            return (eb.at[sb_of(t)] if own else dst), dst
        if c is TEE:
            dst = tb.at[pair_of(t)]
            return (t_ref.at[sb_of(t)] if own else dst), dst
        return panel(t, r0, n, own), panel(t, r0, n, False)

    def wait_sent(t, c, half, r0=None, n=None):
        src, dst = ends(t, c, False, r0, n)
        d = owner_dist(t)

        @pl.when((d == 0) | ((d == 1) & (half == 0)))
        def _():
            side_copy(src, dst, t, c, 0).wait_send()

        @pl.when((d == 0) | ((d == 3) & (half == 1)))
        def _():
            side_copy(src, dst, t, c, 1).wait_send()

        core_copy(src, dst, t, c).wait_send()

    def all_sent(t):
        wait_sent(t, HEAD, head_half(t))

        @pl.when(apart)
        def _():
            wait_sent(t, TEE, 1 - head_half(t))

        partial(t, lambda r0, n: wait_sent(t, sb_of(t), half_of(t, sb_of(t)), r0, n))
        full(t, lambda c, r0, n: wait_sent(t, c, half_of(t, c), r0, n))

    def free_slot(t):
        @pl.when(t >= 8)
        def _():
            all_sent(t - 8)

    def send_own(u):
        first = RING - 1 - k
        part = (u - first + 2 * RING) % RING
        t = u - part
        quarter = RING

        @pl.when((t >= 0) & (t < npair))
        def _():
            def out(c, r0=None, n=None):
                src, dst = ends(t, c, True, r0, n)
                for d in range(2):
                    side_copy(src, dst, t, c, d).start()
                core_copy(src, dst, t, c).start()

            @pl.when(part == 0)
            def _():
                free_slot(t)
                out(HEAD)

                @pl.when(apart)
                def _():
                    out(TEE)

                partial(t, lambda r0, n: out(sb_of(t), r0, n))

            m = height(t)
            lo = (part * m + quarter - 1) // quarter
            hi = ((part + 1) * m + quarter - 1) // quarter

            def one(i, _):
                c = sb_of(t) + i
                out(c, pl.multiple_of(c * CH, CH), CH)
                return 0

            lax.fori_loop(jnp.maximum(lo, 1), hi, one, 0)

    def pass_on(t, near):
        d = owner_dist(t)
        free_slot(t)

        def got(c, half, r0=None, n=None):
            src, dst = ends(t, c, False, r0, n)
            side_copy(src, dst, t, c, 0).wait_recv()
            core_copy(src, dst, t, c).start()
            if near:

                @pl.when((d == 1) & (half == 0))
                def _():
                    side_copy(src, dst, t, c, 0).start()

                @pl.when((d == 3) & (half == 1))
                def _():
                    side_copy(src, dst, t, c, 1).start()

        got(HEAD, head_half(t))

        @pl.when(apart)
        def _():
            got(TEE, 1 - head_half(t))

        partial(t, lambda r0, n: got(sb_of(t), half_of(t, sb_of(t)), r0, n))
        full(t, lambda c, r0, n: got(c, half_of(t, c), r0, n))

    def near_lead(i):
        return jnp.minimum(npair - 1, i + 6 - jnp.maximum(0, (3 * (i - 20) + 10) // 11))

    def far_lead(i):
        return jnp.minimum(npair - 1, jnp.where(i <= 20, i + 2, jnp.maximum(22, i + 1)))

    def own_lead(i):
        return jnp.minimum(npair + RING - 2, i + 1 + OWN_LEAD)

    def span(lead, i):
        return jnp.where(i < 0, 0, lead(i - 1) + 1), lead(i) + 1

    def service(i):
        def one(j, _):
            kind = jnp.where(i < 0, j, 2 - j)

            @pl.when(kind == 0)
            def _():
                lo, hi = span(own_lead, i)
                lax.fori_loop(lo, hi, lambda u, _: (send_own(u), 0)[1], 0)

            @pl.when(kind == 1)
            def _():
                def near(t, _):
                    @pl.when(owner_dist(t) % 2 == 1)
                    def _():
                        pass_on(t, True)

                    return 0

                lo, hi = span(near_lead, i)
                lax.fori_loop(lo, hi, near, 0)

            @pl.when(kind == 2)
            def _():
                def far(t, _):
                    @pl.when(owner_dist(t) == 2)
                    def _():
                        pass_on(t, False)

                    return 0

                lo, hi = span(far_lead, i)
                lax.fori_loop(lo, hi, far, 0)

            return 0

        lax.fori_loop(0, 3, one, 0)

    def make_heads():
        def copies(l):
            rr = pl.ds(pl.multiple_of((l * RING + k) * NB, NB), NB)
            return (pltpu.make_async_copy(v_ref.at[rr, lanes(l)], eb.at[l], h_sem.at[0, l]),
                    pltpu.make_async_copy(t_ref.at[l], et.at[l], h_sem.at[1, l]))

        def begin(l, _):
            for c in copies(l):
                c.start()
            return 0

        lax.fori_loop(0, nsb, begin, 0)

        def one(l, _):
            for c in copies(l):
                c.wait()
            x = eb[l]
            tt = et[l]
            below = lax.broadcasted_iota(jnp.int32, (NB, NB), 0) > lax.broadcasted_iota(jnp.int32, (NB, NB), 1)
            both_in = jnp.where(below, x, tt)
            eb[l] = jnp.where(r == q, both_in, jnp.where(r == 0, tt, x))
            return 0

        lax.fori_loop(0, nsb, one, 0)

    def z_copies(c):
        r0 = pl.multiple_of(c * CH, CH)
        mine = pl.multiple_of(r * rows + c * CH, CH)
        theirs = pl.multiple_of((1 - r) * rows + c * CH, CH)
        loc = pltpu.make_async_copy(z_ref.at[pl.ds(mine, CH), :], zl.at[r, pl.ds(r0, CH), :], z_loc.at[c])
        rem = rcopy(z_ref.at[pl.ds(theirs, CH), :], zl.at[r, pl.ds(r0, CH), :], z_snd.at[c], z_rcv.at[c], across)
        return loc, rem

    def start_z(c):
        for x in z_copies(c):
            x.start()

    def put_x(g, x, at):
        xt[g, :, at] = x
        for i, piece in enumerate(split3(x)):
            xp[g, i * NB : (i + 1) * NB, at] = piece

    def admit(c):
        for x in z_copies(c):
            x.wait()
        r0 = pl.multiple_of(c * CH, CH)

        def one(g, _):
            put_x(g, zl[g, pl.ds(r0, CH), :].T, pl.ds(r0, CH))
            return 0

        lax.fori_loop(0, 2, one, 0)

    def load(t, c, side, src, at):
        return pltpu.make_async_copy(src, vf.at[at, lanes(side)], ld.at[side, c])

    def start_loads(t):
        mine = owner_dist(t) == 0
        p = pair_of(t)

        def one(c, r0, n):
            at = pl.ds(r0, n)

            @pl.when(mine)
            def _():
                load(t, c, q, panel(t, r0, n, True), at).start()

            @pl.when(jnp.logical_not(mine))
            def _():
                load(t, c, q, panel(t, r0, n, False), at).start()

            src, dst = ends(t, c, False, r0, n)
            core_copy(src, dst, t, c).wait_recv()
            load(t, c, 1 - q, vb.at[1 - q, p, at, :], at).start()

        at = head_rows(t)

        @pl.when(jnp.logical_not(mine))
        def _():
            load(t, HEAD, q, vb.at[q, p, at, :], at).start()

        core_copy(*ends(t, HEAD, False), t, HEAD).wait_recv()
        load(t, HEAD, 1 - q, vb.at[1 - q, p, at, :], at).start()

        @pl.when(r == 1)
        def _():
            @pl.when(q == 1)
            def _():
                core_copy(*ends(t, TEE, False), t, TEE).wait_recv()

            @pl.when((q == 0) & mine)
            def _():
                tb[p] = et[sb_of(t)]

        partial(t, lambda r0, n: one(sb_of(t), r0, n))
        full(t, one)

    def pieces(slot, at, x):
        for i, piece in enumerate(split3(x)):
            vn[slot, at, i * PW : (i + 1) * PW] = piece

    def prep(t):
        slot = t % 2
        mine = owner_dist(t) == 0
        at = head_rows(t)
        l = sb_of(t)

        load(t, HEAD, 1 - q, vb.at[0, 0, at, :], at).wait()

        @pl.when(mine)
        def _():
            vf[at, lanes(q)] = eb[l]

        @pl.when(jnp.logical_not(mine))
        def _():
            load(t, HEAD, q, vb.at[0, 0, at, :], at).wait()

        def above(j, _):
            pieces(slot, pl.ds(pl.multiple_of(l * CH + j * NB, NB), NB), jnp.zeros((NB, PW), F32))
            return 0

        lax.fori_loop(0, chip_of(t), above, 0)

        i0 = lax.broadcasted_iota(jnp.int32, (NB, NB), 0)
        i1 = lax.broadcasted_iota(jnp.int32, (NB, NB), 1)
        one = jnp.where(i0 == i1, 1.0, 0.0).astype(F32)
        x0 = vf[at, 0:NB]
        x1 = vf[at, NB:PW]
        first = r == 0
        v0 = jnp.where(first, jnp.where(i0 > i1, x0, one), x0)
        v1 = jnp.where(first, 0.0, jnp.where(i0 > i1, x1, one))
        tc[slot, 0] = jnp.where(first, jnp.where(i0 > i1, 0.0, x0), tb[pair_of(t)])
        tc[slot, 1] = jnp.where(i0 > i1, 0.0, x1)
        pieces(slot, at, jnp.concatenate([v0, v1], axis=1))

        def rest(r0, n):
            a = pl.ds(r0, n)
            for side in range(2):
                load(t, l, side, vb.at[0, 0, a, :], a).wait()

            def sub(j, _):
                b = pl.ds(pl.multiple_of(r0 + j * NB, NB), NB)
                pieces(slot, b, vf[b, :])
                return 0

            lax.fori_loop(0, n // NB, sub, 0)

        partial(t, rest)

        def chunk(c, r0, n):
            a = pl.ds(r0, n)
            for side in range(2):
                load(t, c, side, vb.at[0, 0, a, :], a).wait()
            for j in range(0, n, NB):
                b = pl.ds(pl.multiple_of(r0 + j, NB), NB)
                pieces(slot, b, vf[b, :])

        full(t, chunk)

    def gram_copy(t):
        s = (t // 2) % 2
        return rcopy(gs.at[s], gr.at[s], g_snd.at[s], g_rcv.at[s], across)

    def gram_share_copy(t):
        return rcopy(gf.at[t % 8], gf.at[t % 8], f_snd.at[t % 8], f_rcv.at[t % 8], partner)

    def gram(t):
        slot = t % 2
        s = (t // 2) % 2

        @pl.when(t >= 4)
        def _():
            gram_copy(t - 4).wait_send()

        gs[s] = jnp.zeros((NB, NB), F32)

        def one(c, _):
            at = pl.ds(pl.multiple_of(c * CH, CH), CH)
            a = [vn[slot, at, i * PW : i * PW + NB].T for i in range(3)]
            b = [vn[slot, at, i * PW + NB : (i + 1) * PW] for i in range(3)]
            x = mm(jnp.concatenate(a, axis=0), jnp.concatenate(b[0:2], axis=1))
            gs[s] += add_rows(add_rows(mm(a[0], b[2]), x[:, 0:NB], NB), x[0 : 2 * NB, NB:PW], NB)
            return 0

        lax.fori_loop(sb_of(t), nsb, one, 0)
        gram_copy(t).start()

    def gram_share(t):
        s = (t // 2) % 2
        gram_copy(t).wait_recv()

        @pl.when(t >= 8)
        def _():
            gram_share_copy(t - 8).wait_send()

        gf[t % 8] = gs[s] + gr[s]
        gram_share_copy(t).start()

    def block_factor(t):
        slot = t % 2

        @pl.when(slot != q)
        def _():
            gram_share_copy(t).wait_recv()

        g = gf[t % 8]
        ta = tc[slot, 0]
        tbb = tc[slot, 1]
        upper = -full_dot(mm, ta, full_dot(mm, g, tbb))
        for i, piece in enumerate(split3(ta)):
            tp[0:NB, i * PW : i * PW + NB] = piece
        for i, piece in enumerate(split3(upper)):
            tp[0:NB, i * PW + NB : (i + 1) * PW] = piece
        for i, piece in enumerate(split3(tbb)):
            tp[NB:PW, i * PW : i * PW + NB] = jnp.zeros((NB, NB), BF16)
            tp[NB:PW, i * PW + NB : (i + 1) * PW] = piece

    def w_copy(t, g):
        return rcopy(ws.at[t % 2, g], wr.at[t % 2, g], w_snd.at[t % 2, g], w_rcv.at[t % 2, g], across)

    def coefficients(t, g):
        with jax.named_scope("wwait"):
            w_copy(t, g).wait_recv()
        w = ws[t % 2, g] + wr[t % 2, g]
        y = stacked(mm_nt, jnp.concatenate(split3(w), axis=0), [tp[:, i * PW : (i + 1) * PW] for i in range(3)])
        for i, piece in enumerate(split3(y)):
            yp[i * NB : (i + 1) * NB] = piece

    def piece_of(t, i, at):
        return vn[t % 2, at, i * PW : (i + 1) * PW]

    def update_and_product(t, g, at, n, an):
        u = w = None
        for i in range(3):
            m = (3 - i) * NB
            if an is not None:
                w = add_rows(w, mm(xp[g, 0:m, an], piece_of(n, i, an)), NB)
            if at is not None:
                u = add_rows(u, mm_nt(yp[0:m], piece_of(t, i, at)), NB)
        if an is not None:
            ws[n % 2, g] += w
        if at is not None:
            put_x(g, xt[g, :, at] - u, at)

    def chunk_at(c):
        return pl.ds(pl.multiple_of(c * CH, CH), CH)

    def both(i, g):
        c0 = sb_of(i)
        n = i + 1
        odd = (nsb - c0) % 2
        e0 = c0 + odd
        nbig = (nsb - e0) // 2

        def big_at(b):
            return pl.ds(pl.multiple_of((e0 + 2 * b) * CH, CH), BIG)

        @pl.when(odd == 1)
        def _():
            update_and_product(i, g, chunk_at(c0), n, None)

        def small(c, _):
            update_and_product(i, g, None, n, chunk_at(c))
            return 0

        lax.fori_loop(sb_of(n), e0, small, 0)

        @pl.when(nbig > 0)
        def _():
            update_and_product(i, g, big_at(0), n, None)

            def one(b, _):
                update_and_product(i, g, big_at(b), n, big_at(b - 1))
                return 0

            lax.fori_loop(1, nbig, one, 0)
            update_and_product(i, g, None, n, big_at(nbig - 1))

    def out_copy(g, c):
        return pltpu.make_async_copy(zl.at[g, chunk_at(c), :], out_ref.at[chunk_at(c), lanes(g)], o_sem.at[g, c])

    def step(i, _):
        n = i + 1

        @pl.when((i >= 0) & (i % RING == 0) & (i // RING + 2 < nsb))
        def _():
            start_z(nsb - 1 - (i // RING + 2))

        @pl.when(n < npair)
        def _():
            with jax.named_scope("svc"):
                service(i)
            with jax.named_scope("loads"):
                start_loads(n)

        @pl.when(i >= 0)
        def _():
            with jax.named_scope("bfac"):
                block_factor(i)

        @pl.when(n < npair)
        def _():
            with jax.named_scope("prep"):
                prep(n)

            @pl.when(n % 2 == q)
            def _():
                with jax.named_scope("gram"):
                    gram(n)

            @pl.when(n % RING == 0)
            def _():
                admit(sb_of(n))

        def group(g, _):
            @pl.when(i >= 0)
            def _():
                with jax.named_scope("coef"):
                    coefficients(i, g)

            @pl.when(n < npair)
            def _():
                @pl.when(n >= 2)
                def _():
                    w_copy(n - 2, g).wait_send()

                ws[n % 2, g] = jnp.zeros((NB, PW), F32)

            @pl.when(i < 0)
            def _():
                update_and_product(n, g, None, n, chunk_at(nsb - 1))

            @pl.when((i >= 0) & (n < npair))
            def _():
                with jax.named_scope("both"):
                    both(i, g)

            @pl.when(n < npair)
            def _():
                w_copy(n, g).start()

                @pl.when((g == 0) & (n % 2 == q))
                def _():
                    with jax.named_scope("share"):
                        gram_share(n)

            @pl.when(n == npair)
            def _():
                def one(c, _):
                    update_and_product(i, g, chunk_at(c), n, None)
                    zl[g, chunk_at(c), :] = xt[g, :, chunk_at(c)].T
                    out_copy(g, c).start()
                    return 0

                lax.fori_loop(0, nsb, one, 0)

            return 0

        lax.fori_loop(0, 2, group, 0)
        return 0

    barrier = pltpu.get_barrier_semaphore()
    for dev in (at_ring(rho + 1), at_ring(rho + RING - 1), partner, across):
        pl.semaphore_signal(barrier, inc=1, device_id=dev, device_id_type=MESH_ID)
    pl.semaphore_wait(barrier, 4)

    start_z(nsb - 1)
    if nsb > 1:
        start_z(nsb - 2)
    with jax.named_scope("heads"):
        make_heads()
    lax.fori_loop(-1, npair, step, 0)

    for t in (npair - 2, npair - 1):
        for g in range(2):
            w_copy(t, g).wait_send()
    for t in (npair - 4, npair - 3, npair - 2, npair - 1):

        @pl.when(t % 2 == q)
        def _(t=t):
            gram_copy(t).wait_send()

    def drain(t, _):
        @pl.when(t % 2 == q)
        def _():
            gram_share_copy(t).wait_send()

        all_sent(t)
        return 0

    lax.fori_loop(max(0, npair - 8), npair, drain, 0)

    def out_done(c, _):
        for g in range(2):
            out_copy(g, c).wait()
        return 0

    lax.fori_loop(0, nsb, out_done, 0)


def solution(mesh):
    def local(v, t, z):
        rows, cols = v.shape
        nsb = cols // NB
        npair = nsb * RING
        hbm = pl.BlockSpec(memory_space=pltpu.MemorySpace.HBM)
        out, _ = pl.pallas_call(
            functools.partial(body, nsb),
            out_shape=(
                jax.ShapeDtypeStruct((rows, PW), F32),
                jax.ShapeDtypeStruct((2, npair, rows, NB), F32),
            ),
            in_specs=[hbm] * 3,
            out_specs=(hbm, hbm),
            scratch_shapes=[
                pltpu.VMEM((2, rows, NB), F32),
                pltpu.VMEM((2, NB, rows), F32),
                pltpu.VMEM((2, 3 * NB, rows), BF16),
                pltpu.VMEM((rows, PW), F32),
                pltpu.VMEM((2, rows, 3 * PW), BF16),
                pltpu.VMEM((npair, NB, NB), F32),
                pltpu.VMEM((2, 2, NB, NB), F32),
                pltpu.VMEM((PW, 3 * PW), BF16),
                pltpu.VMEM((2, 2, NB, PW), F32),
                pltpu.VMEM((2, 2, NB, PW), F32),
                pltpu.VMEM((2, NB, NB), F32),
                pltpu.VMEM((2, NB, NB), F32),
                pltpu.VMEM((8, NB, NB), F32),
                pltpu.VMEM((3 * NB, PW), BF16),
                pltpu.VMEM((nsb, NB, NB), F32),
                pltpu.VMEM((nsb, NB, NB), F32),
            ],
            compiler_params=pltpu.CompilerParams(
                collective_id=0, has_side_effects=True, vmem_limit_bytes=60 * 2**20),
            name="backtransform",
        )(v, t, z)
        return out

    return jax.shard_map(local, mesh=mesh,
                         in_specs=(P("row", "col"), P("col", None, None), P(None, ("col", "row"))),
                         out_specs=P("row", "col"), check_vma=False)
```

```python
import functools

import jax
import jax.numpy as jnp
from jax import lax
from jax.experimental import pallas as pl
from jax.experimental.pallas import tpu as pltpu
from jax.sharding import PartitionSpec as P

F32 = jnp.float32
BF16 = jnp.bfloat16
MESH_ID = pl.DeviceIdType.MESH

NB = 128
PW = 2 * NB
CH = 4 * NB
BIG = 2 * CH
RING = 4
OWN_LEAD = 12


def split3(x):
    hi = x.astype(BF16)
    rest = x - hi.astype(F32)
    mid = rest.astype(BF16)
    low = (rest - mid.astype(F32)).astype(BF16)
    return hi, mid, low


def mm(a, b):
    return lax.dot_general(a, b, (((1,), (0,)), ((), ())), preferred_element_type=F32)


def mm_nt(a, b):
    return lax.dot_general(a, b, (((1,), (1,)), ((), ())), preferred_element_type=F32)


def add_rows(total, x, n):
    for i in range(0, x.shape[0], n):
        part = x[i : i + n]
        total = part if total is None else total + part
    return total


def stacked(dot, a3, b):
    m = a3.shape[0] // 3
    s = None
    for i in range(3):
        s = add_rows(s, dot(a3[0 : (3 - i) * m], b[i]), m)
    return s


def full_dot(dot, a, b):
    return stacked(dot, jnp.concatenate(split3(a), axis=0), split3(b))


def body(nsb, v_ref, t_ref, z_ref, out_ref, vb, *scratch):
    rows = nsb * CH
    dma = pltpu.SemaphoreType.DMA
    npair = nsb * RING
    nc = nsb + 2
    pl.run_scoped(
        functools.partial(run, nsb, rows, npair, v_ref, t_ref, z_ref, out_ref, vb, scratch),
        dma((nsb,)),
        dma((npair,)),
        dma((npair,)),
        dma((npair, nc)),
        dma((npair, nc)),
        dma((2, 2)),
        dma((2, 2)),
        dma((2,)),
        dma((2,)),
        dma((8,)),
        dma((8,)),
        dma((2, nc)),
        dma((2, nsb)),
        dma((2, 8, nc)),
        dma((8, nc)),
        dma((2, nsb)),
    )


def run(nsb, rows, npair, v_ref, t_ref, z_ref, out_ref, vb, scratch, *sems):
    (zl, xt, xp, vf, vn, tb, tc, tp, ws, wr, gs, gr, gf, yp, eb, et) = scratch
    (z_loc, z_snd, z_rcv, i_rcv, d_rcv, w_snd, w_rcv, g_snd, g_rcv, f_snd, f_rcv, ld, o_sem, i_snd, d_snd, h_sem) = sems
    HEAD, TEE = nsb, nsb + 1
    r = lax.axis_index("row")
    col = lax.axis_index("col")
    q = col % 2
    k = col // 2
    ky, kx = k // 2, k % 2
    rho = 2 * ky + (kx + ky) % 2

    def at_ring(i):
        i = i % RING
        y = i // 2
        x = (i % 2 + y) % 2
        return (r, (y * 2 + x) * 2 + q)

    partner = (r, k * 2 + 1 - q)
    across = (1 - r, col)
    apart = (r == 1) & (q == 0)

    def pair_of(t):
        return npair - 1 - t

    def sb_of(t):
        return pair_of(t) // RING

    def chip_of(t):
        return pair_of(t) % RING

    def owner_dist(t):
        kk = chip_of(t)
        y = kk // 2
        ro = 2 * y + (kk % 2 + y) % 2
        return (rho - ro + RING) % RING

    def height(t):
        return nsb - sb_of(t)

    def half_of(t, c):
        return (c - sb_of(t) + (height(t) - 1) // 2) % 2

    def head_half(t):
        return height(t) % 2

    def partial(t, fn):
        kk = chip_of(t)
        for j in range(RING - 1):

            @pl.when(kk == j)
            def _(j=j):
                fn(pl.multiple_of(sb_of(t) * CH + (j + 1) * NB, NB), CH - (j + 1) * NB)

    def full(t, fn):
        def one(c, _):
            fn(c, pl.multiple_of(c * CH, CH), CH)
            return 0

        lax.fori_loop(sb_of(t) + 1, nsb, one, 0)

    def head_rows(t):
        return pl.ds(pl.multiple_of(pair_of(t) * NB, NB), NB)

    def lanes(l):
        return pl.ds(pl.multiple_of(l * NB, NB), NB)

    def rcopy(src, dst, ssem, rsem, dev):
        return pltpu.make_async_remote_copy(src, dst, ssem, rsem, device_id=dev, device_id_type=MESH_ID)

    def panel(t, r0, n, own):
        if own:
            return v_ref.at[pl.ds(r0, n), lanes(sb_of(t))]
        return vb.at[q, pair_of(t), pl.ds(r0, n), :]

    def side_copy(src, dst, t, c, d):
        return rcopy(src, dst, i_snd.at[d, t % 8, c], i_rcv.at[t, c], at_ring(rho + 1 - 2 * d + RING))

    def core_copy(src, dst, t, c):
        return rcopy(src, dst, d_snd.at[t % 8, c], d_rcv.at[t, c], partner)

    def ends(t, c, own, r0=None, n=None):
        if c is HEAD:
            dst = vb.at[q, pair_of(t), head_rows(t), :]
            return (eb.at[sb_of(t)] if own else dst), dst
        if c is TEE:
            dst = tb.at[pair_of(t)]
            return (t_ref.at[sb_of(t)] if own else dst), dst
        return panel(t, r0, n, own), panel(t, r0, n, False)

    def wait_sent(t, c, half, r0=None, n=None):
        src, dst = ends(t, c, False, r0, n)
        d = owner_dist(t)

        @pl.when((d == 0) | ((d == 1) & (half == 0)))
        def _():
            side_copy(src, dst, t, c, 0).wait_send()

        @pl.when((d == 0) | ((d == 3) & (half == 1)))
        def _():
            side_copy(src, dst, t, c, 1).wait_send()

        core_copy(src, dst, t, c).wait_send()

    def all_sent(t):
        wait_sent(t, HEAD, head_half(t))

        @pl.when(apart)
        def _():
            wait_sent(t, TEE, 1 - head_half(t))

        partial(t, lambda r0, n: wait_sent(t, sb_of(t), half_of(t, sb_of(t)), r0, n))
        full(t, lambda c, r0, n: wait_sent(t, c, half_of(t, c), r0, n))

    def free_slot(t):
        @pl.when(t >= 8)
        def _():
            all_sent(t - 8)

    def send_own(u):
        first = RING - 1 - k
        part = (u - first + 2 * RING) % RING
        t = u - part
        quarter = RING

        @pl.when((t >= 0) & (t < npair))
        def _():
            def out(c, r0=None, n=None):
                src, dst = ends(t, c, True, r0, n)
                for d in range(2):
                    side_copy(src, dst, t, c, d).start()
                core_copy(src, dst, t, c).start()

            @pl.when(part == 0)
            def _():
                free_slot(t)
                out(HEAD)

                @pl.when(apart)
                def _():
                    out(TEE)

                partial(t, lambda r0, n: out(sb_of(t), r0, n))

            m = height(t)
            lo = (part * m + quarter - 1) // quarter
            hi = ((part + 1) * m + quarter - 1) // quarter

            def one(i, _):
                c = sb_of(t) + i
                out(c, pl.multiple_of(c * CH, CH), CH)
                return 0

            lax.fori_loop(jnp.maximum(lo, 1), hi, one, 0)

    def pass_on(t, near):
        d = owner_dist(t)
        free_slot(t)

        def got(c, half, r0=None, n=None):
            src, dst = ends(t, c, False, r0, n)
            side_copy(src, dst, t, c, 0).wait_recv()
            core_copy(src, dst, t, c).start()
            if near:

                @pl.when((d == 1) & (half == 0))
                def _():
                    side_copy(src, dst, t, c, 0).start()

                @pl.when((d == 3) & (half == 1))
                def _():
                    side_copy(src, dst, t, c, 1).start()

        got(HEAD, head_half(t))

        @pl.when(apart)
        def _():
            got(TEE, 1 - head_half(t))

        partial(t, lambda r0, n: got(sb_of(t), half_of(t, sb_of(t)), r0, n))
        full(t, lambda c, r0, n: got(c, half_of(t, c), r0, n))

    def near_lead(i):
        lead = jnp.minimum(i + 2, 5 - jnp.maximum(0, (3 * (i - 20) + 10) // 11))
        return jnp.minimum(npair - 1, i + 1 + lead)

    def far_lead(i):
        return jnp.minimum(npair - 1, jnp.where(i <= 20, i + 1 + jnp.minimum(i + 1, 1), jnp.maximum(22, i + 1)))

    def own_lead(i):
        return jnp.minimum(npair + RING - 2, i + 1 + jnp.minimum(OWN_LEAD, 4 + 3 * (i + 1)))

    def span(lead, i):
        return jnp.where(i < 0, 0, lead(i - 1) + 1), lead(i) + 1

    def service(i):
        def one(j, _):
            kind = jnp.where(i < 0, j, 2 - j)

            @pl.when(kind == 0)
            def _():
                lo, hi = span(own_lead, i)
                lax.fori_loop(lo, hi, lambda u, _: (send_own(u), 0)[1], 0)

            @pl.when(kind == 1)
            def _():
                def near(t, _):
                    @pl.when(owner_dist(t) % 2 == 1)
                    def _():
                        pass_on(t, True)

                    return 0

                lo, hi = span(near_lead, i)
                lax.fori_loop(lo, hi, near, 0)

            @pl.when(kind == 2)
            def _():
                def far(t, _):
                    @pl.when(owner_dist(t) == 2)
                    def _():
                        pass_on(t, False)

                    return 0

                lo, hi = span(far_lead, i)
                lax.fori_loop(lo, hi, far, 0)

            return 0

        lax.fori_loop(0, 3, one, 0)

    def make_heads():
        def copies(l):
            rr = pl.ds(pl.multiple_of((l * RING + k) * NB, NB), NB)
            return (pltpu.make_async_copy(v_ref.at[rr, lanes(l)], eb.at[l], h_sem.at[0, l]),
                    pltpu.make_async_copy(t_ref.at[l], et.at[l], h_sem.at[1, l]))

        def begin(l, _):
            for c in copies(l):
                c.start()
            return 0

        lax.fori_loop(0, nsb, begin, 0)

        def one(l, _):
            for c in copies(l):
                c.wait()
            x = eb[l]
            tt = et[l]
            below = lax.broadcasted_iota(jnp.int32, (NB, NB), 0) > lax.broadcasted_iota(jnp.int32, (NB, NB), 1)
            both_in = jnp.where(below, x, tt)
            eb[l] = jnp.where(r == q, both_in, jnp.where(r == 0, tt, x))
            return 0

        lax.fori_loop(0, nsb, one, 0)

    def z_local(c):
        mine = pl.multiple_of(r * rows + c * CH, CH)
        return pltpu.make_async_copy(z_ref.at[pl.ds(mine, CH), :], zl.at[r, chunk_at(c), :], z_loc.at[c])

    def z_piece(w):
        c = nsb - 1 - w // RING
        r0 = c * CH + w % RING * NB
        theirs = pl.multiple_of((1 - r) * rows + r0, NB)
        return rcopy(z_ref.at[pl.ds(theirs, NB), :], zl.at[r, pl.ds(pl.multiple_of(r0, NB), NB), :],
                     z_snd.at[w], z_rcv.at[w], across)

    def put_x(g, x, at):
        xt[g, :, at] = x
        for i, piece in enumerate(split3(x)):
            xp[g, i * NB : (i + 1) * NB, at] = piece

    def admit(c):
        for j in range(RING):
            z_piece((nsb - 1 - c) * RING + j).wait()
        z_local(c).wait()

        def one(g, _):
            put_x(g, zl[g, chunk_at(c), :].T, chunk_at(c))
            return 0

        lax.fori_loop(0, 2, one, 0)

    def load(t, c, side, src, at):
        return pltpu.make_async_copy(src, vf.at[at, lanes(side)], ld.at[side, c])

    def start_loads(t):
        mine = owner_dist(t) == 0
        p = pair_of(t)

        def one(c, r0, n):
            at = pl.ds(r0, n)

            @pl.when(mine)
            def _():
                load(t, c, q, panel(t, r0, n, True), at).start()

            @pl.when(jnp.logical_not(mine))
            def _():
                load(t, c, q, panel(t, r0, n, False), at).start()

            src, dst = ends(t, c, False, r0, n)
            core_copy(src, dst, t, c).wait_recv()
            load(t, c, 1 - q, vb.at[1 - q, p, at, :], at).start()

        at = head_rows(t)

        @pl.when(jnp.logical_not(mine))
        def _():
            load(t, HEAD, q, vb.at[q, p, at, :], at).start()

        core_copy(*ends(t, HEAD, False), t, HEAD).wait_recv()
        load(t, HEAD, 1 - q, vb.at[1 - q, p, at, :], at).start()

        @pl.when(r == 1)
        def _():
            @pl.when(q == 1)
            def _():
                core_copy(*ends(t, TEE, False), t, TEE).wait_recv()

            @pl.when((q == 0) & mine)
            def _():
                tb[p] = et[sb_of(t)]

        partial(t, lambda r0, n: one(sb_of(t), r0, n))
        full(t, one)

    def pieces(slot, at, x):
        for i, piece in enumerate(split3(x)):
            vn[slot, at, i * PW : (i + 1) * PW] = piece

    def prep(t):
        slot = t % 2
        mine = owner_dist(t) == 0
        at = head_rows(t)
        l = sb_of(t)

        load(t, HEAD, 1 - q, vb.at[0, 0, at, :], at).wait()

        @pl.when(mine)
        def _():
            vf[at, lanes(q)] = eb[l]

        @pl.when(jnp.logical_not(mine))
        def _():
            load(t, HEAD, q, vb.at[0, 0, at, :], at).wait()

        def above(j, _):
            pieces(slot, pl.ds(pl.multiple_of(l * CH + j * NB, NB), NB), jnp.zeros((NB, PW), F32))
            return 0

        lax.fori_loop(0, chip_of(t), above, 0)

        i0 = lax.broadcasted_iota(jnp.int32, (NB, NB), 0)
        i1 = lax.broadcasted_iota(jnp.int32, (NB, NB), 1)
        one = jnp.where(i0 == i1, 1.0, 0.0).astype(F32)
        x0 = vf[at, 0:NB]
        x1 = vf[at, NB:PW]
        first = r == 0
        v0 = jnp.where(first, jnp.where(i0 > i1, x0, one), x0)
        v1 = jnp.where(first, 0.0, jnp.where(i0 > i1, x1, one))
        tc[slot, 0] = jnp.where(first, jnp.where(i0 > i1, 0.0, x0), tb[pair_of(t)])
        tc[slot, 1] = jnp.where(i0 > i1, 0.0, x1)
        pieces(slot, at, jnp.concatenate([v0, v1], axis=1))

        def rest(r0, n):
            a = pl.ds(r0, n)
            for side in range(2):
                load(t, l, side, vb.at[0, 0, a, :], a).wait()

            def sub(j, _):
                b = pl.ds(pl.multiple_of(r0 + j * NB, NB), NB)
                pieces(slot, b, vf[b, :])
                return 0

            lax.fori_loop(0, n // NB, sub, 0)

        partial(t, rest)

        def chunk(c, r0, n):
            a = pl.ds(r0, n)
            for side in range(2):
                load(t, c, side, vb.at[0, 0, a, :], a).wait()
            for j in range(0, n, NB):
                b = pl.ds(pl.multiple_of(r0 + j, NB), NB)
                pieces(slot, b, vf[b, :])

        full(t, chunk)

    def gram_copy(t):
        s = (t // 2) % 2
        return rcopy(gs.at[s], gr.at[s], g_snd.at[s], g_rcv.at[s], across)

    def gram_share_copy(t):
        return rcopy(gf.at[t % 8], gf.at[t % 8], f_snd.at[t % 8], f_rcv.at[t % 8], partner)

    def gram(t):
        slot = t % 2
        s = (t // 2) % 2

        @pl.when(t >= 4)
        def _():
            gram_copy(t - 4).wait_send()

        gs[s] = jnp.zeros((NB, NB), F32)

        def one(c, _):
            at = pl.ds(pl.multiple_of(c * CH, CH), CH)
            a = [vn[slot, at, i * PW : i * PW + NB].T for i in range(3)]
            b = [vn[slot, at, i * PW + NB : (i + 1) * PW] for i in range(3)]
            x = mm(jnp.concatenate(a, axis=0), jnp.concatenate(b[0:2], axis=1))
            gs[s] += add_rows(add_rows(mm(a[0], b[2]), x[:, 0:NB], NB), x[0 : 2 * NB, NB:PW], NB)
            return 0

        lax.fori_loop(sb_of(t), nsb, one, 0)
        gram_copy(t).start()

    def gram_share(t):
        s = (t // 2) % 2
        gram_copy(t).wait_recv()

        @pl.when(t >= 8)
        def _():
            gram_share_copy(t - 8).wait_send()

        gf[t % 8] = gs[s] + gr[s]
        gram_share_copy(t).start()

    def block_factor(t):
        slot = t % 2

        @pl.when(slot != q)
        def _():
            gram_share_copy(t).wait_recv()

        g = gf[t % 8]
        ta = tc[slot, 0]
        tbb = tc[slot, 1]
        upper = -full_dot(mm, ta, full_dot(mm, g, tbb))
        for i, piece in enumerate(split3(ta)):
            tp[0:NB, i * PW : i * PW + NB] = piece
        for i, piece in enumerate(split3(upper)):
            tp[0:NB, i * PW + NB : (i + 1) * PW] = piece
        for i, piece in enumerate(split3(tbb)):
            tp[NB:PW, i * PW : i * PW + NB] = jnp.zeros((NB, NB), BF16)
            tp[NB:PW, i * PW + NB : (i + 1) * PW] = piece

    def w_copy(t, g):
        return rcopy(ws.at[t % 2, g], wr.at[t % 2, g], w_snd.at[t % 2, g], w_rcv.at[t % 2, g], across)

    def coefficients(t, g):
        with jax.named_scope("wwait"):
            w_copy(t, g).wait_recv()
        w = ws[t % 2, g] + wr[t % 2, g]
        y = stacked(mm_nt, jnp.concatenate(split3(w), axis=0), [tp[:, i * PW : (i + 1) * PW] for i in range(3)])
        for i, piece in enumerate(split3(y)):
            yp[i * NB : (i + 1) * NB] = piece

    def piece_of(t, i, at):
        return vn[t % 2, at, i * PW : (i + 1) * PW]

    def update_and_product(t, g, at, n, an):
        u = w = None
        for i in range(3):
            m = (3 - i) * NB
            if an is not None:
                w = add_rows(w, mm(xp[g, 0:m, an], piece_of(n, i, an)), NB)
            if at is not None:
                u = add_rows(u, mm_nt(yp[0:m], piece_of(t, i, at)), NB)
        if an is not None:
            ws[n % 2, g] += w
        if at is not None:
            put_x(g, xt[g, :, at] - u, at)

    def chunk_at(c):
        return pl.ds(pl.multiple_of(c * CH, CH), CH)

    def both(i, g):
        c0 = sb_of(i)
        n = i + 1
        odd = (nsb - c0) % 2
        e0 = c0 + odd
        nbig = (nsb - e0) // 2

        def big_at(b):
            return pl.ds(pl.multiple_of((e0 + 2 * b) * CH, CH), BIG)

        @pl.when(odd == 1)
        def _():
            update_and_product(i, g, chunk_at(c0), n, None)

        def small(c, _):
            update_and_product(i, g, None, n, chunk_at(c))
            return 0

        lax.fori_loop(sb_of(n), e0, small, 0)

        @pl.when(nbig > 0)
        def _():
            update_and_product(i, g, big_at(0), n, None)

            def one(b, _):
                update_and_product(i, g, big_at(b), n, big_at(b - 1))
                return 0

            lax.fori_loop(1, nbig, one, 0)
            update_and_product(i, g, None, n, big_at(nbig - 1))

    def out_copy(g, c):
        return pltpu.make_async_copy(zl.at[g, chunk_at(c), :], out_ref.at[chunk_at(c), lanes(g)], o_sem.at[g, c])

    def step(i, _):
        n = i + 1

        @pl.when(n < npair)
        def _():
            with jax.named_scope("svc"):
                service(i)
            with jax.named_scope("loads"):
                start_loads(n)

        @pl.when(i >= 0)
        def _():
            with jax.named_scope("bfac"):
                block_factor(i)

        @pl.when(n < npair)
        def _():
            with jax.named_scope("prep"):
                prep(n)

            @pl.when(n % 2 == q)
            def _():
                with jax.named_scope("gram"):
                    gram(n)

            @pl.when(n % RING == 0)
            def _():
                admit(sb_of(n))

        def group(g, _):
            @pl.when(i >= 0)
            def _():
                with jax.named_scope("coef"):
                    coefficients(i, g)

            @pl.when(n < npair)
            def _():
                @pl.when(n >= 2)
                def _():
                    w_copy(n - 2, g).wait_send()

                ws[n % 2, g] = jnp.zeros((NB, PW), F32)

            @pl.when(i < 0)
            def _():
                update_and_product(n, g, None, n, chunk_at(nsb - 1))

            @pl.when((i >= 0) & (n < npair))
            def _():
                with jax.named_scope("both"):
                    both(i, g)

            @pl.when(n < npair)
            def _():
                w_copy(n, g).start()

                @pl.when((g == 0) & (n % 2 == q))
                def _():
                    with jax.named_scope("share"):
                        gram_share(n)

            @pl.when(n == npair)
            def _():
                def one(c, _):
                    update_and_product(i, g, chunk_at(c), n, None)
                    zl[g, chunk_at(c), :] = xt[g, :, chunk_at(c)].T
                    out_copy(g, c).start()
                    return 0

                lax.fori_loop(0, nsb, one, 0)

            return 0

        lax.fori_loop(0, 2, group, 0)

        @pl.when(n + RING < npair)
        def _():
            z_piece(n + RING).start()

        @pl.when((n % RING == 2) & (n + RING < npair))
        def _():
            z_local(sb_of(n) - 1).start()

        return 0

    barrier = pltpu.get_barrier_semaphore()
    for dev in (at_ring(rho + 1), at_ring(rho + RING - 1), partner, across):
        pl.semaphore_signal(barrier, inc=1, device_id=dev, device_id_type=MESH_ID)
    pl.semaphore_wait(barrier, 4)

    for j in range(RING):
        z_piece(j).start()
    z_local(nsb - 1).start()
    with jax.named_scope("heads"):
        make_heads()
    lax.fori_loop(-1, npair, step, 0)

    for t in (npair - 2, npair - 1):
        for g in range(2):
            w_copy(t, g).wait_send()
    for t in (npair - 4, npair - 3, npair - 2, npair - 1):

        @pl.when(t % 2 == q)
        def _(t=t):
            gram_copy(t).wait_send()

    def drain(t, _):
        @pl.when(t % 2 == q)
        def _():
            gram_share_copy(t).wait_send()

        all_sent(t)
        return 0

    lax.fori_loop(max(0, npair - 8), npair, drain, 0)

    def out_done(c, _):
        for g in range(2):
            out_copy(g, c).wait()
        return 0

    lax.fori_loop(0, nsb, out_done, 0)


def solution(mesh):
    def local(v, t, z):
        rows, cols = v.shape
        nsb = cols // NB
        npair = nsb * RING
        hbm = pl.BlockSpec(memory_space=pltpu.MemorySpace.HBM)
        out, _ = pl.pallas_call(
            functools.partial(body, nsb),
            out_shape=(
                jax.ShapeDtypeStruct((rows, PW), F32),
                jax.ShapeDtypeStruct((2, npair, rows, NB), F32),
            ),
            in_specs=[hbm] * 3,
            out_specs=(hbm, hbm),
            scratch_shapes=[
                pltpu.VMEM((2, rows, NB), F32),
                pltpu.VMEM((2, NB, rows), F32),
                pltpu.VMEM((2, 3 * NB, rows), BF16),
                pltpu.VMEM((rows, PW), F32),
                pltpu.VMEM((2, rows, 3 * PW), BF16),
                pltpu.VMEM((npair, NB, NB), F32),
                pltpu.VMEM((2, 2, NB, NB), F32),
                pltpu.VMEM((PW, 3 * PW), BF16),
                pltpu.VMEM((2, 2, NB, PW), F32),
                pltpu.VMEM((2, 2, NB, PW), F32),
                pltpu.VMEM((2, NB, NB), F32),
                pltpu.VMEM((2, NB, NB), F32),
                pltpu.VMEM((8, NB, NB), F32),
                pltpu.VMEM((3 * NB, PW), BF16),
                pltpu.VMEM((nsb, NB, NB), F32),
                pltpu.VMEM((nsb, NB, NB), F32),
            ],
            compiler_params=pltpu.CompilerParams(
                collective_id=0, has_side_effects=True, vmem_limit_bytes=60 * 2**20),
            name="backtransform",
        )(v, t, z)
        return out

    return jax.shard_map(local, mesh=mesh,
                         in_specs=(P("row", "col"), P("col", None, None), P(None, ("col", "row"))),
                         out_specs=P("row", "col"), check_vma=False)
```

```python
import functools

import jax
import jax.numpy as jnp
from jax import lax
from jax.experimental import pallas as pl
from jax.experimental.pallas import tpu as pltpu
from jax.sharding import PartitionSpec as P

F32 = jnp.float32
BF16 = jnp.bfloat16
MESH_ID = pl.DeviceIdType.MESH

NB = 128
PW = 2 * NB
CH = 4 * NB
UNIT = PW
LAG = 2
RING = 4
OWN_LEAD = 10
AHEAD = 20


def split3(x):
    hi = x.astype(BF16)
    rest = x - hi.astype(F32)
    mid = rest.astype(BF16)
    low = (rest - mid.astype(F32)).astype(BF16)
    return hi, mid, low


def mm(a, b):
    return lax.dot_general(a, b, (((1,), (0,)), ((), ())), preferred_element_type=F32)


def mm_nt(a, b):
    return lax.dot_general(a, b, (((1,), (1,)), ((), ())), preferred_element_type=F32)


def add_rows(total, x, n):
    for i in range(0, x.shape[0], n):
        part = x[i : i + n]
        total = part if total is None else total + part
    return total


def stacked(dot, a3, b):
    m = a3.shape[0] // 3
    s = None
    for i in range(3):
        s = add_rows(s, dot(a3[0 : (3 - i) * m], b[i]), m)
    return s


def full_dot(dot, a, b):
    return stacked(dot, jnp.concatenate(split3(a), axis=0), split3(b))


def body(nsb, v_ref, t_ref, z_ref, out_ref, vb, *scratch):
    rows = nsb * CH
    dma = pltpu.SemaphoreType.DMA
    npair = nsb * RING
    nc = nsb + 1
    pl.run_scoped(
        functools.partial(run, nsb, rows, npair, v_ref, t_ref, z_ref, out_ref, vb, scratch),
        dma((nsb,)),
        dma((npair,)),
        dma((npair,)),
        dma((npair, nc)),
        dma((npair, nc)),
        dma((2, 2)),
        dma((2, 2)),
        dma((2,)),
        dma((2,)),
        dma((8,)),
        dma((8,)),
        dma((2, nc)),
        dma((2, nsb)),
        dma((2, 8, nc)),
        dma((8, nc)),
        dma((2, nsb)),
        dma((2, 8)),
        dma((2, 8)),
    )


def run(nsb, rows, npair, v_ref, t_ref, z_ref, out_ref, vb, scratch, *sems):
    (zl, xt, xp, vf, vn, tb, tc, tp, ws, wr, gs, gr, gf, yp, eb, et) = scratch
    (z_loc, z_snd, z_rcv, i_rcv, d_rcv, w_snd, w_rcv, g_snd, g_rcv, f_snd, f_rcv, ld, o_sem, i_snd, d_snd, h_sem, t_snd, t_rcv) = sems
    HEAD = nsb
    r = lax.axis_index("row")
    col = lax.axis_index("col")
    q = col % 2
    k = col // 2
    ky, kx = k // 2, k % 2
    rho = 2 * ky + (kx + ky) % 2

    def at_ring(i):
        i = i % RING
        y = i // 2
        x = (i % 2 + y) % 2
        return (r, (y * 2 + x) * 2 + q)

    partner = (r, k * 2 + 1 - q)
    across = (1 - r, col)

    def pair_of(t):
        return npair - 1 - t

    def sb_of(t):
        return pair_of(t) // RING

    def chip_of(t):
        return pair_of(t) % RING

    def owner_dist(t):
        kk = chip_of(t)
        y = kk // 2
        ro = 2 * y + (kk % 2 + y) % 2
        return (rho - ro + RING) % RING

    def height(t):
        return nsb - sb_of(t)

    def half_of(t, c):
        return (c - sb_of(t) + (height(t) - 1) // 2) % 2

    def head_half(t):
        return height(t) % 2

    def partial(t, fn):
        kk = chip_of(t)
        for j in range(RING - 1):

            @pl.when(kk == j)
            def _(j=j):
                fn(pl.multiple_of(sb_of(t) * CH + (j + 1) * NB, NB), CH - (j + 1) * NB)

    def full(t, fn):
        def one(c, _):
            fn(c, pl.multiple_of(c * CH, CH), CH)
            return 0

        lax.fori_loop(sb_of(t) + 1, nsb, one, 0)

    def head_rows(t):
        return pl.ds(pl.multiple_of(pair_of(t) * NB, NB), NB)

    def lanes(l):
        return pl.ds(pl.multiple_of(l * NB, NB), NB)

    def rcopy(src, dst, ssem, rsem, dev):
        return pltpu.make_async_remote_copy(src, dst, ssem, rsem, device_id=dev, device_id_type=MESH_ID)

    def panel(t, r0, n, own):
        if own:
            return v_ref.at[pl.ds(r0, n), lanes(sb_of(t))]
        return vb.at[q, pair_of(t), pl.ds(r0, n), :]

    def side_copy(src, dst, t, c, d):
        return rcopy(src, dst, i_snd.at[d, t % 8, c], i_rcv.at[t, c], at_ring(rho + 1 - 2 * d + RING))

    def core_copy(src, dst, t, c):
        return rcopy(src, dst, d_snd.at[t % 8, c], d_rcv.at[t, c], partner)

    def ends(t, c, own, r0=None, n=None):
        if c is HEAD:
            dst = vb.at[q, pair_of(t), head_rows(t), :]
            return (eb.at[sb_of(t)] if own else dst), dst
        return panel(t, r0, n, own), panel(t, r0, n, False)

    def wait_sent(t, c, half, r0=None, n=None):
        src, dst = ends(t, c, False, r0, n)
        d = owner_dist(t)

        @pl.when((d == 0) | ((d == 1) & (half == 0)))
        def _():
            side_copy(src, dst, t, c, 0).wait_send()

        @pl.when((d == 0) | ((d == 3) & (half == 1)))
        def _():
            side_copy(src, dst, t, c, 1).wait_send()

        core_copy(src, dst, t, c).wait_send()

    def all_sent(t):
        wait_sent(t, HEAD, head_half(t))

        partial(t, lambda r0, n: wait_sent(t, sb_of(t), half_of(t, sb_of(t)), r0, n))
        full(t, lambda c, r0, n: wait_sent(t, c, half_of(t, c), r0, n))

    def free_slot(t):
        @pl.when(t >= 8)
        def _():
            all_sent(t - 8)

    def send_own(u):
        first = RING - 1 - k
        part = (u - first + 2 * RING) % RING
        t = u - part
        quarter = RING

        @pl.when((t >= 0) & (t < npair))
        def _():
            def out(c, r0=None, n=None):
                src, dst = ends(t, c, True, r0, n)
                for d in range(2):
                    side_copy(src, dst, t, c, d).start()
                core_copy(src, dst, t, c).start()

            @pl.when(part == 0)
            def _():
                free_slot(t)
                out(HEAD)

                partial(t, lambda r0, n: out(sb_of(t), r0, n))

            m = height(t)
            lo = (part * m + quarter - 1) // quarter
            hi = ((part + 1) * m + quarter - 1) // quarter

            def one(i, _):
                c = sb_of(t) + i
                out(c, pl.multiple_of(c * CH, CH), CH)
                return 0

            lax.fori_loop(jnp.maximum(lo, 1), hi, one, 0)

    def pass_on(t, near):
        d = owner_dist(t)
        free_slot(t)

        def got(c, half, r0=None, n=None):
            src, dst = ends(t, c, False, r0, n)
            side_copy(src, dst, t, c, 0).wait_recv()
            core_copy(src, dst, t, c).start()
            if near:

                @pl.when((d == 1) & (half == 0))
                def _():
                    side_copy(src, dst, t, c, 0).start()

                @pl.when((d == 3) & (half == 1))
                def _():
                    side_copy(src, dst, t, c, 1).start()

        got(HEAD, head_half(t))

        partial(t, lambda r0, n: got(sb_of(t), half_of(t, sb_of(t)), r0, n))
        full(t, lambda c, r0, n: got(c, half_of(t, c), r0, n))

    def brought(i):
        return jnp.minimum(npair - 1, jnp.minimum(i + 2, jnp.maximum(AHEAD + 1, i + 1)))

    def near_lead(i):
        return jnp.minimum(npair - 1, brought(i) + jnp.minimum(3, i + 3))

    def far_lead(i):
        return brought(i)

    def own_lead(i):
        return jnp.minimum(npair + RING - 2, brought(i) + jnp.minimum(OWN_LEAD, 6 + 2 * (i + 2)))

    def span(lead, i):
        return jnp.where(i < -1, 0, lead(i - 1) + 1), lead(i) + 1

    def service(i):
        def one(j, _):
            kind = jnp.where(i < -1, j, 2 - j)

            @pl.when(kind == 0)
            def _():
                lo, hi = span(own_lead, i)
                lax.fori_loop(lo, hi, lambda u, _: (send_own(u), 0)[1], 0)

            @pl.when(kind == 1)
            def _():
                def near(t, _):
                    @pl.when(owner_dist(t) % 2 == 1)
                    def _():
                        pass_on(t, True)

                    return 0

                lo, hi = span(near_lead, i)
                lax.fori_loop(lo, hi, near, 0)

            @pl.when(kind == 2)
            def _():
                def far(t, _):
                    @pl.when(owner_dist(t) == 2)
                    def _():
                        pass_on(t, False)

                    return 0

                lo, hi = span(far_lead, i)
                lax.fori_loop(lo, hi, far, 0)

            return 0

        lax.fori_loop(0, 3, one, 0)

    def make_heads():
        def copies(l):
            rr = pl.ds(pl.multiple_of((l * RING + k) * NB, NB), NB)
            return (pltpu.make_async_copy(v_ref.at[rr, lanes(l)], eb.at[l], h_sem.at[0, l]),
                    pltpu.make_async_copy(t_ref.at[l], et.at[l], h_sem.at[1, l]))

        def begin(l, _):
            for c in copies(l):
                c.start()
            return 0

        lax.fori_loop(0, nsb, begin, 0)

        def one(l, _):
            for c in copies(l):
                c.wait()
            x = eb[l]
            tt = et[l]
            below = lax.broadcasted_iota(jnp.int32, (NB, NB), 0) > lax.broadcasted_iota(jnp.int32, (NB, NB), 1)
            both_in = jnp.where(below, x, tt)
            eb[l] = jnp.where(r == q, both_in, jnp.where(r == 0, tt, x))
            return 0

        lax.fori_loop(0, nsb, one, 0)

    def z_local(c):
        mine = pl.multiple_of(r * rows + c * CH, CH)
        return pltpu.make_async_copy(z_ref.at[pl.ds(mine, CH), :], zl.at[r, chunk_at(c), :], z_loc.at[c])

    def z_piece(w):
        c = nsb - 1 - w // RING
        r0 = c * CH + w % RING * NB
        theirs = pl.multiple_of((1 - r) * rows + r0, NB)
        return rcopy(z_ref.at[pl.ds(theirs, NB), :], zl.at[r, pl.ds(pl.multiple_of(r0, NB), NB), :],
                     z_snd.at[w], z_rcv.at[w], across)

    def put_x(g, x, at):
        xt[g, :, at] = x
        for i, piece in enumerate(split3(x)):
            xp[g, i * NB : (i + 1) * NB, at] = piece

    def admit(c):
        for j in range(RING):
            z_piece((nsb - 1 - c) * RING + j).wait()
        z_local(c).wait()

        def one(g, _):
            put_x(g, zl[g, chunk_at(c), :].T, chunk_at(c))
            return 0

        lax.fori_loop(0, 2, one, 0)

    def load(t, c, side, src, at):
        return pltpu.make_async_copy(src, vf.at[at, lanes(side)], ld.at[side, c])

    def start_loads(t):
        mine = owner_dist(t) == 0
        p = pair_of(t)

        def one(c, r0, n):
            at = pl.ds(r0, n)

            @pl.when(mine)
            def _():
                load(t, c, q, panel(t, r0, n, True), at).start()

            @pl.when(jnp.logical_not(mine))
            def _():
                load(t, c, q, panel(t, r0, n, False), at).start()

            src, dst = ends(t, c, False, r0, n)
            core_copy(src, dst, t, c).wait_recv()
            load(t, c, 1 - q, vb.at[1 - q, p, at, :], at).start()

        at = head_rows(t)

        @pl.when(jnp.logical_not(mine))
        def _():
            load(t, HEAD, q, vb.at[q, p, at, :], at).start()

        core_copy(*ends(t, HEAD, False), t, HEAD).wait_recv()
        load(t, HEAD, 1 - q, vb.at[1 - q, p, at, :], at).start()

        partial(t, lambda r0, n: one(sb_of(t), r0, n))
        full(t, one)

    def pieces(slot, at, x):
        for i, piece in enumerate(split3(x)):
            vn[slot, at, i * PW : (i + 1) * PW] = piece

    def prep(t):
        slot = t % 3
        mine = owner_dist(t) == 0
        at = head_rows(t)
        l = sb_of(t)

        load(t, HEAD, 1 - q, vb.at[0, 0, at, :], at).wait()

        @pl.when((r == 0) & (q == 0) & (t >= 3))
        def _():
            factor_across(t - 3).wait_send()

        @pl.when(mine)
        def _():
            vf[at, lanes(q)] = eb[l]

        @pl.when(jnp.logical_not(mine))
        def _():
            load(t, HEAD, q, vb.at[0, 0, at, :], at).wait()

        def above(j, _):
            pieces(slot, pl.ds(pl.multiple_of(l * CH + j * NB, NB), NB), jnp.zeros((NB, PW), F32))
            return 0

        lax.fori_loop(0, chip_of(t), above, 0)

        i0 = lax.broadcasted_iota(jnp.int32, (NB, NB), 0)
        i1 = lax.broadcasted_iota(jnp.int32, (NB, NB), 1)
        one = jnp.where(i0 == i1, 1.0, 0.0).astype(F32)
        x0 = vf[at, 0:NB]
        x1 = vf[at, NB:PW]
        first = r == 0
        v0 = jnp.where(first, jnp.where(i0 > i1, x0, one), x0)
        v1 = jnp.where(first, 0.0, jnp.where(i0 > i1, x1, one))
        tc[slot, 0] = jnp.where(i0 > i1, 0.0, x0)
        tc[slot, 1] = jnp.where(i0 > i1, 0.0, x1)
        pieces(slot, at, jnp.concatenate([v0, v1], axis=1))

        @pl.when(first & (q == 0))
        def _():
            factor_across(t).start()

        def rest(r0, n):
            a = pl.ds(r0, n)
            for side in range(2):
                load(t, l, side, vb.at[0, 0, a, :], a).wait()

            def sub(j, _):
                b = pl.ds(pl.multiple_of(r0 + j * NB, NB), NB)
                pieces(slot, b, vf[b, :])
                return 0

            lax.fori_loop(0, n // NB, sub, 0)

        partial(t, rest)

        def chunk(c, r0, n):
            a = pl.ds(r0, n)
            for side in range(2):
                load(t, c, side, vb.at[0, 0, a, :], a).wait()
            for j in range(0, n, NB):
                b = pl.ds(pl.multiple_of(r0 + j, NB), NB)
                pieces(slot, b, vf[b, :])

        full(t, chunk)

    def factor_across(t):
        return rcopy(tc.at[t % 3, 0], tb.at[t % 8], t_snd.at[0, t % 8], t_rcv.at[0, t % 8], across)

    def factor_over(t):
        return rcopy(tb.at[t % 8], tb.at[t % 8], t_snd.at[1, t % 8], t_rcv.at[1, t % 8], partner)

    def share_factor(t):
        @pl.when((r == 1) & (q == 0))
        def _():
            factor_across(t).wait_recv()

            @pl.when(t >= 2)
            def _():
                factor_over(t - 2).wait_send()

            factor_over(t).start()

    def gram_copy(t):
        s = (t // 2) % 2
        return rcopy(gs.at[s], gr.at[s], g_snd.at[s], g_rcv.at[s], across)

    def gram_share_copy(t):
        return rcopy(gf.at[t % 8], gf.at[t % 8], f_snd.at[t % 8], f_rcv.at[t % 8], partner)

    def gram(t):
        slot = t % 3
        s = (t // 2) % 2

        @pl.when(t >= 4)
        def _():
            gram_copy(t - 4).wait_send()

        gs[s] = jnp.zeros((NB, NB), F32)

        def one(c, _):
            at = pl.ds(pl.multiple_of(c * CH, CH), CH)
            a = [vn[slot, at, i * PW : i * PW + NB].T for i in range(3)]
            b = [vn[slot, at, i * PW + NB : (i + 1) * PW] for i in range(3)]
            x = mm(jnp.concatenate(a, axis=0), jnp.concatenate(b[0:2], axis=1))
            gs[s] += add_rows(add_rows(mm(a[0], b[2]), x[:, 0:NB], NB), x[0 : 2 * NB, NB:PW], NB)
            return 0

        lax.fori_loop(sb_of(t), nsb, one, 0)
        gram_copy(t).start()

    def gram_share(t):
        s = (t // 2) % 2
        gram_copy(t).wait_recv()

        @pl.when(t >= 8)
        def _():
            gram_share_copy(t - 8).wait_send()

        gf[t % 8] = gs[s] + gr[s]
        gram_share_copy(t).start()

    def block_factor(t):
        slot = t % 3

        @pl.when(t % 2 != q)
        def _():
            gram_share_copy(t).wait_recv()

        @pl.when((r == 1) & (q == 1))
        def _():
            factor_over(t).wait_recv()

        g = gf[t % 8]
        ta = jnp.where(r == 0, tc[slot, 0], tb[t % 8])
        tbb = tc[slot, 1]
        upper = -full_dot(mm, ta, full_dot(mm, g, tbb))
        for i, piece in enumerate(split3(ta)):
            tp[0:NB, i * PW : i * PW + NB] = piece
        for i, piece in enumerate(split3(upper)):
            tp[0:NB, i * PW + NB : (i + 1) * PW] = piece
        for i, piece in enumerate(split3(tbb)):
            tp[NB:PW, i * PW : i * PW + NB] = jnp.zeros((NB, NB), BF16)
            tp[NB:PW, i * PW + NB : (i + 1) * PW] = piece

    def w_copy(t, g):
        return rcopy(ws.at[t % 2, g], wr.at[t % 2, g], w_snd.at[t % 2, g], w_rcv.at[t % 2, g], across)

    def coefficients(t, g):
        with jax.named_scope("wwait"):
            w_copy(t, g).wait_recv()
        w = ws[t % 2, g] + wr[t % 2, g]
        y = stacked(mm_nt, jnp.concatenate(split3(w), axis=0), [tp[:, i * PW : (i + 1) * PW] for i in range(3)])
        for i, piece in enumerate(split3(y)):
            yp[i * NB : (i + 1) * NB] = piece

    def piece_of(t, i, at):
        return vn[t % 3, at, i * PW : (i + 1) * PW]

    def chunk_at(c):
        return pl.ds(pl.multiple_of(c * CH, CH), CH)

    def passes(m, i, g, n, finish):
        units = m * CH // UNIT
        base = rows - m * CH
        w = None
        for c in range(units + (0 if n is None else LAG)):
            at = pl.ds(base + c * UNIT, UNIT)
            an = pl.ds(max(0, base + (c - LAG) * UNIT), UNIT)
            u = None
            for j in range(3):
                k3 = (3 - j) * NB
                if n is not None and c >= LAG:
                    w = add_rows(w, mm(xp[g, 0:k3, an], piece_of(n, j, an)), NB)
                if c < units:
                    u = add_rows(u, mm_nt(yp[0:k3], piece_of(i, j, at)), NB)
            if c < units:
                finish(at, xt[g, :, at] - u)
        if n is not None:
            ws[n % 2, g] += w

    def product(n, g, at):
        w = None
        for j in range(3):
            w = add_rows(w, mm(xp[g, 0 : (3 - j) * NB, at], piece_of(n, j, at)), NB)
        ws[n % 2, g] += w

    def both(i, g):
        n = i + 1

        @pl.when(sb_of(n) < sb_of(i))
        def _():
            product(n, g, chunk_at(sb_of(n)))

        for m in range(1, nsb + 1):

            @pl.when(height(i) == m)
            def _(m=m):
                passes(m, i, g, n, lambda at, x: put_x(g, x, at))

    def out_copy(g, c):
        return pltpu.make_async_copy(zl.at[g, chunk_at(c), :], out_ref.at[chunk_at(c), lanes(g)], o_sem.at[g, c])

    def last(i, g):
        def finish(at, x):
            zl[g, at, :] = x.T

        passes(nsb, i, g, None, finish)

        def out(c, _):
            out_copy(g, c).start()
            return 0

        lax.fori_loop(0, nsb, out, 0)

    def step(i, _):
        n = i + 1
        early = i < AHEAD
        b = jnp.where(early, i + 2, n)
        brings = (i != AHEAD) & (b < npair)

        @pl.when(i < npair - 1)
        def _():
            with jax.named_scope("svc"):
                service(i)

        @pl.when(brings)
        def _():
            with jax.named_scope("loads"):
                start_loads(b)

        @pl.when(i >= 0)
        def _():
            with jax.named_scope("bfac"):
                block_factor(i)

        @pl.when(brings & jnp.logical_not(early))
        def _():
            with jax.named_scope("prep"):
                prep(b)

        @pl.when((n >= 0) & (n < npair) & (n % RING == 0))
        def _():
            admit(sb_of(n))

        def group(g, _):
            @pl.when(i >= 0)
            def _():
                with jax.named_scope("coef"):
                    coefficients(i, g)

            @pl.when((n >= 0) & (n < npair))
            def _():
                @pl.when(n >= 2)
                def _():
                    w_copy(n - 2, g).wait_send()

                ws[n % 2, g] = jnp.zeros((NB, PW), F32)

            @pl.when(i == -1)
            def _():
                product(n, g, chunk_at(nsb - 1))

            @pl.when((i >= 0) & (n < npair))
            def _():
                with jax.named_scope("both"):
                    both(i, g)

            @pl.when((n >= 0) & (n < npair))
            def _():
                w_copy(n, g).start()

                @pl.when(g == jnp.where(i <= AHEAD, 0, 1))
                def _():
                    with jax.named_scope("fshare"):
                        share_factor(n)

                    @pl.when(n % 2 == q)
                    def _():
                        with jax.named_scope("share"):
                            gram_share(n)

            @pl.when((g == 0) & brings)
            def _():
                @pl.when(early)
                def _():
                    with jax.named_scope("prep"):
                        prep(b)

                @pl.when(b % 2 == q)
                def _():
                    with jax.named_scope("gram"):
                        gram(b)

            @pl.when(n == npair)
            def _():
                with jax.named_scope("last"):
                    last(i, g)

            return 0

        lax.fori_loop(0, 2, group, 0)

        @pl.when((n >= 0) & (n + 2 * RING < npair))
        def _():
            z_piece(n + 2 * RING).start()

        @pl.when((n >= 0) & (n % RING == 2) & (n + RING < npair))
        def _():
            z_local(sb_of(n) - 1).start()

        return 0

    barrier = pltpu.get_barrier_semaphore()
    for dev in (at_ring(rho + 1), at_ring(rho + RING - 1), partner, across):
        pl.semaphore_signal(barrier, inc=1, device_id=dev, device_id_type=MESH_ID)
    pl.semaphore_wait(barrier, 4)

    for j in range(min(2 * RING, npair)):
        z_piece(j).start()
    z_local(nsb - 1).start()
    with jax.named_scope("heads"):
        make_heads()
    lax.fori_loop(-2, npair, step, 0)

    for t in (npair - 2, npair - 1):
        for g in range(2):
            w_copy(t, g).wait_send()
    for t in (npair - 4, npair - 3, npair - 2, npair - 1):

        @pl.when(t % 2 == q)
        def _(t=t):
            gram_copy(t).wait_send()

    for t in range(npair - 3, npair):

        @pl.when((r == 0) & (q == 0))
        def _(t=t):
            factor_across(t).wait_send()

    for t in range(npair - 2, npair):

        @pl.when((r == 1) & (q == 0))
        def _(t=t):
            factor_over(t).wait_send()

    def drain(t, _):
        @pl.when(t % 2 == q)
        def _():
            gram_share_copy(t).wait_send()

        all_sent(t)
        return 0

    lax.fori_loop(max(0, npair - 8), npair, drain, 0)

    def out_done(c, _):
        for g in range(2):
            out_copy(g, c).wait()
        return 0

    lax.fori_loop(0, nsb, out_done, 0)


def solution(mesh):
    def local(v, t, z):
        rows, cols = v.shape
        nsb = cols // NB
        npair = nsb * RING
        hbm = pl.BlockSpec(memory_space=pltpu.MemorySpace.HBM)
        out, _ = pl.pallas_call(
            functools.partial(body, nsb),
            out_shape=(
                jax.ShapeDtypeStruct((rows, PW), F32),
                jax.ShapeDtypeStruct((2, npair, rows, NB), F32),
            ),
            in_specs=[hbm] * 3,
            out_specs=(hbm, hbm),
            scratch_shapes=[
                pltpu.VMEM((2, rows, NB), F32),
                pltpu.VMEM((2, NB, rows), F32),
                pltpu.VMEM((2, 3 * NB, rows), BF16),
                pltpu.VMEM((rows, PW), F32),
                pltpu.VMEM((3, rows, 3 * PW), BF16),
                pltpu.VMEM((8, NB, NB), F32),
                pltpu.VMEM((3, 2, NB, NB), F32),
                pltpu.VMEM((PW, 3 * PW), BF16),
                pltpu.VMEM((2, 2, NB, PW), F32),
                pltpu.VMEM((2, 2, NB, PW), F32),
                pltpu.VMEM((2, NB, NB), F32),
                pltpu.VMEM((2, NB, NB), F32),
                pltpu.VMEM((8, NB, NB), F32),
                pltpu.VMEM((3 * NB, PW), BF16),
                pltpu.VMEM((nsb, NB, NB), F32),
                pltpu.VMEM((nsb, NB, NB), F32),
            ],
            compiler_params=pltpu.CompilerParams(
                collective_id=0, has_side_effects=True, vmem_limit_bytes=60 * 2**20),
            name="backtransform",
        )(v, t, z)
        return out

    return jax.shard_map(local, mesh=mesh,
                         in_specs=(P("row", "col"), P("col", None, None), P(None, ("col", "row"))),
                         out_specs=P("row", "col"), check_vma=False)
```

```python
import functools

import jax
import jax.numpy as jnp
from jax import lax
from jax.experimental import pallas as pl
from jax.experimental.pallas import tpu as pltpu
from jax.sharding import PartitionSpec as P

F32 = jnp.float32
BF16 = jnp.bfloat16
MESH_ID = pl.DeviceIdType.MESH

NB = 128
PW = 2 * NB
CH = 4 * NB
UNIT = PW
LAG = 2
RING = 4
OWN_LEAD = 10
AHEAD = 20


def split3(x):
    hi = x.astype(BF16)
    rest = x - hi.astype(F32)
    mid = rest.astype(BF16)
    low = (rest - mid.astype(F32)).astype(BF16)
    return hi, mid, low


def mm(a, b):
    return lax.dot_general(a, b, (((1,), (0,)), ((), ())), preferred_element_type=F32)


def mm_nt(a, b):
    return lax.dot_general(a, b, (((1,), (1,)), ((), ())), preferred_element_type=F32)


def add_rows(total, x, n):
    for i in range(0, x.shape[0], n):
        part = x[i : i + n]
        total = part if total is None else total + part
    return total


def stacked(dot, a3, b):
    m = a3.shape[0] // 3
    s = None
    for i in range(3):
        s = add_rows(s, dot(a3[0 : (3 - i) * m], b[i]), m)
    return s


def full_dot(dot, a, b):
    return stacked(dot, jnp.concatenate(split3(a), axis=0), split3(b))


def body(nsb, v_ref, t_ref, z_ref, out_ref, vb, *scratch):
    rows = nsb * CH
    dma = pltpu.SemaphoreType.DMA
    npair = nsb * RING
    nc = nsb + 1
    pl.run_scoped(
        functools.partial(run, nsb, rows, npair, v_ref, t_ref, z_ref, out_ref, vb, scratch),
        dma((nsb,)),
        dma((npair,)),
        dma((npair,)),
        dma((npair, nc)),
        dma((npair, nc)),
        dma((2, 2)),
        dma((2, 2)),
        dma((2,)),
        dma((2,)),
        dma((8,)),
        dma((8,)),
        dma((2, nc)),
        dma((2, nsb)),
        dma((2, 8, nc)),
        dma((8, nc)),
        dma((2, nsb)),
        dma((2,)),
        dma((2,)),
        dma((2, 8)),
        dma((2, 8)),
    )


def run(nsb, rows, npair, v_ref, t_ref, z_ref, out_ref, vb, scratch, *sems):
    (zl, xt, xp, vf, vn, tb, tc, tp, ws, wr, gs, gp, gz, gr, gf, yp, eb, et) = scratch
    (z_loc, z_snd, z_rcv, i_rcv, d_rcv, w_snd, w_rcv, g_snd, g_rcv, f_snd, f_rcv, ld, o_sem, i_snd, d_snd, h_sem, p_snd, p_rcv, t_snd, t_rcv) = sems
    HEAD = nsb
    r = lax.axis_index("row")
    col = lax.axis_index("col")
    q = col % 2
    k = col // 2
    ky, kx = k // 2, k % 2
    rho = 2 * ky + (kx + ky) % 2

    def at_ring(i):
        i = i % RING
        y = i // 2
        x = (i % 2 + y) % 2
        return (r, (y * 2 + x) * 2 + q)

    partner = (r, k * 2 + 1 - q)
    across = (1 - r, col)

    def pair_of(t):
        return npair - 1 - t

    def sb_of(t):
        return pair_of(t) // RING

    def chip_of(t):
        return pair_of(t) % RING

    def owner_dist(t):
        kk = chip_of(t)
        y = kk // 2
        ro = 2 * y + (kk % 2 + y) % 2
        return (rho - ro + RING) % RING

    def height(t):
        return nsb - sb_of(t)

    def half_of(t, c):
        return (c - sb_of(t) + (height(t) - 1) // 2) % 2

    def head_half(t):
        return height(t) % 2

    def partial(t, fn):
        kk = chip_of(t)
        for j in range(RING - 1):

            @pl.when(kk == j)
            def _(j=j):
                fn(pl.multiple_of(sb_of(t) * CH + (j + 1) * NB, NB), CH - (j + 1) * NB)

    def full(t, fn):
        def one(c, _):
            fn(c, pl.multiple_of(c * CH, CH), CH)
            return 0

        lax.fori_loop(sb_of(t) + 1, nsb, one, 0)

    def head_rows(t):
        return pl.ds(pl.multiple_of(pair_of(t) * NB, NB), NB)

    def lanes(l):
        return pl.ds(pl.multiple_of(l * NB, NB), NB)

    def rcopy(src, dst, ssem, rsem, dev):
        return pltpu.make_async_remote_copy(src, dst, ssem, rsem, device_id=dev, device_id_type=MESH_ID)

    def panel(t, r0, n, own):
        if own:
            return v_ref.at[pl.ds(r0, n), lanes(sb_of(t))]
        return vb.at[q, pair_of(t), pl.ds(r0, n), :]

    def side_copy(src, dst, t, c, d):
        return rcopy(src, dst, i_snd.at[d, t % 8, c], i_rcv.at[t, c], at_ring(rho + 1 - 2 * d + RING))

    def core_copy(src, dst, t, c):
        return rcopy(src, dst, d_snd.at[t % 8, c], d_rcv.at[t, c], partner)

    def ends(t, c, own, r0=None, n=None):
        if c is HEAD:
            dst = vb.at[q, pair_of(t), head_rows(t), :]
            return (eb.at[sb_of(t)] if own else dst), dst
        return panel(t, r0, n, own), panel(t, r0, n, False)

    def wait_sent(t, c, half, r0=None, n=None):
        src, dst = ends(t, c, False, r0, n)
        d = owner_dist(t)

        @pl.when((d == 0) | ((d == 1) & (half == 0)))
        def _():
            side_copy(src, dst, t, c, 0).wait_send()

        @pl.when((d == 0) | ((d == 3) & (half == 1)))
        def _():
            side_copy(src, dst, t, c, 1).wait_send()

        core_copy(src, dst, t, c).wait_send()

    def all_sent(t):
        wait_sent(t, HEAD, head_half(t))

        partial(t, lambda r0, n: wait_sent(t, sb_of(t), half_of(t, sb_of(t)), r0, n))
        full(t, lambda c, r0, n: wait_sent(t, c, half_of(t, c), r0, n))

    def free_slot(t):
        @pl.when(t >= 8)
        def _():
            all_sent(t - 8)

    def send_own(u):
        first = RING - 1 - k
        part = (u - first + 2 * RING) % RING
        t = u - part
        quarter = RING

        @pl.when((t >= 0) & (t < npair))
        def _():
            def out(c, r0=None, n=None):
                src, dst = ends(t, c, True, r0, n)
                for d in range(2):
                    side_copy(src, dst, t, c, d).start()
                core_copy(src, dst, t, c).start()

            @pl.when(part == 0)
            def _():
                free_slot(t)
                out(HEAD)

                partial(t, lambda r0, n: out(sb_of(t), r0, n))

            m = height(t)
            lo = (part * m + quarter - 1) // quarter
            hi = ((part + 1) * m + quarter - 1) // quarter

            def one(i, _):
                c = sb_of(t) + i
                out(c, pl.multiple_of(c * CH, CH), CH)
                return 0

            lax.fori_loop(jnp.maximum(lo, 1), hi, one, 0)

    def pass_on(t, near):
        d = owner_dist(t)
        free_slot(t)

        def got(c, half, r0=None, n=None):
            src, dst = ends(t, c, False, r0, n)
            side_copy(src, dst, t, c, 0).wait_recv()
            core_copy(src, dst, t, c).start()
            if near:

                @pl.when((d == 1) & (half == 0))
                def _():
                    side_copy(src, dst, t, c, 0).start()

                @pl.when((d == 3) & (half == 1))
                def _():
                    side_copy(src, dst, t, c, 1).start()

        got(HEAD, head_half(t))

        partial(t, lambda r0, n: got(sb_of(t), half_of(t, sb_of(t)), r0, n))
        full(t, lambda c, r0, n: got(c, half_of(t, c), r0, n))

    def brought(i):
        return jnp.minimum(npair - 1, jnp.minimum(i + 2, jnp.maximum(AHEAD + 1, i + 1)))

    def near_lead(i):
        return jnp.minimum(npair - 1, brought(i) + jnp.minimum(4, i + 3))

    def far_lead(i):
        return jnp.minimum(npair - 1, brought(i) + jnp.where((i >= 0) & (i < 15), 1, 0))

    def own_lead(i):
        return jnp.minimum(npair + RING - 2, brought(i) + jnp.minimum(OWN_LEAD, 2 + 4 * (i + 2)))

    def span(lead, i):
        return jnp.where(i < -1, 0, lead(i - 1) + 1), lead(i) + 1

    def service(i):
        def one(j, _):
            kind = jnp.where(i < -1, j, 2 - j)

            @pl.when(kind == 0)
            def _():
                lo, hi = span(own_lead, i)
                lax.fori_loop(lo, hi, lambda u, _: (send_own(u), 0)[1], 0)

            @pl.when(kind == 1)
            def _():
                def near(t, _):
                    @pl.when(owner_dist(t) % 2 == 1)
                    def _():
                        pass_on(t, True)

                    return 0

                lo, hi = span(near_lead, i)
                lax.fori_loop(lo, hi, near, 0)

            @pl.when(kind == 2)
            def _():
                def far(t, _):
                    @pl.when(owner_dist(t) == 2)
                    def _():
                        pass_on(t, False)

                    return 0

                lo, hi = span(far_lead, i)
                lax.fori_loop(lo, hi, far, 0)

            return 0

        lax.fori_loop(0, 3, one, 0)

    def make_heads():
        def copies(l):
            rr = pl.ds(pl.multiple_of((l * RING + k) * NB, NB), NB)
            return (pltpu.make_async_copy(v_ref.at[rr, lanes(l)], eb.at[l], h_sem.at[0, l]),
                    pltpu.make_async_copy(t_ref.at[l], et.at[l], h_sem.at[1, l]))

        def begin(l, _):
            for c in copies(l):
                c.start()
            return 0

        lax.fori_loop(0, nsb, begin, 0)

        def one(l, _):
            for c in copies(l):
                c.wait()
            x = eb[l]
            tt = et[l]
            below = lax.broadcasted_iota(jnp.int32, (NB, NB), 0) > lax.broadcasted_iota(jnp.int32, (NB, NB), 1)
            both_in = jnp.where(below, x, tt)
            eb[l] = jnp.where(r == q, both_in, jnp.where(r == 0, tt, x))
            return 0

        lax.fori_loop(0, nsb, one, 0)

    def z_local(c):
        mine = pl.multiple_of(r * rows + c * CH, CH)
        return pltpu.make_async_copy(z_ref.at[pl.ds(mine, CH), :], zl.at[r, chunk_at(c), :], z_loc.at[c])

    def z_piece(w):
        c = nsb - 1 - w // RING
        r0 = c * CH + w % RING * NB
        theirs = pl.multiple_of((1 - r) * rows + r0, NB)
        return rcopy(z_ref.at[pl.ds(theirs, NB), :], zl.at[r, pl.ds(pl.multiple_of(r0, NB), NB), :],
                     z_snd.at[w], z_rcv.at[w], across)

    def put_x(g, x, at):
        xt[g, :, at] = x
        for i, piece in enumerate(split3(x)):
            xp[g, i * NB : (i + 1) * NB, at] = piece

    def admit(c):
        for j in range(RING):
            z_piece((nsb - 1 - c) * RING + j).wait()
        z_local(c).wait()

        def one(g, _):
            put_x(g, zl[g, chunk_at(c), :].T, chunk_at(c))
            return 0

        lax.fori_loop(0, 2, one, 0)

    def load(t, c, side, src, at):
        return pltpu.make_async_copy(src, vf.at[at, lanes(side)], ld.at[side, c])

    def start_loads(t):
        mine = owner_dist(t) == 0
        p = pair_of(t)

        def one(c, r0, n):
            at = pl.ds(r0, n)

            @pl.when(mine)
            def _():
                load(t, c, q, panel(t, r0, n, True), at).start()

            @pl.when(jnp.logical_not(mine))
            def _():
                load(t, c, q, panel(t, r0, n, False), at).start()

            src, dst = ends(t, c, False, r0, n)
            core_copy(src, dst, t, c).wait_recv()
            load(t, c, 1 - q, vb.at[1 - q, p, at, :], at).start()

        at = head_rows(t)

        @pl.when(jnp.logical_not(mine))
        def _():
            load(t, HEAD, q, vb.at[q, p, at, :], at).start()

        core_copy(*ends(t, HEAD, False), t, HEAD).wait_recv()
        load(t, HEAD, 1 - q, vb.at[1 - q, p, at, :], at).start()

        partial(t, lambda r0, n: one(sb_of(t), r0, n))
        full(t, one)

    def pieces(slot, at, x):
        for i, piece in enumerate(split3(x)):
            vn[slot, at, i * PW : (i + 1) * PW] = piece

    def prep(t):
        slot = t % 3
        mine = owner_dist(t) == 0
        at = head_rows(t)
        l = sb_of(t)

        load(t, HEAD, 1 - q, vb.at[0, 0, at, :], at).wait()

        @pl.when((r == 0) & (q == 0) & (t >= 3))
        def _():
            factor_across(t - 3).wait_send()

        @pl.when(mine)
        def _():
            vf[at, lanes(q)] = eb[l]

        @pl.when(jnp.logical_not(mine))
        def _():
            load(t, HEAD, q, vb.at[0, 0, at, :], at).wait()

        def above(j, _):
            pieces(slot, pl.ds(pl.multiple_of(l * CH + j * NB, NB), NB), jnp.zeros((NB, PW), F32))
            return 0

        lax.fori_loop(0, chip_of(t), above, 0)

        i0 = lax.broadcasted_iota(jnp.int32, (NB, NB), 0)
        i1 = lax.broadcasted_iota(jnp.int32, (NB, NB), 1)
        one = jnp.where(i0 == i1, 1.0, 0.0).astype(F32)
        x0 = vf[at, 0:NB]
        x1 = vf[at, NB:PW]
        first = r == 0
        v0 = jnp.where(first, jnp.where(i0 > i1, x0, one), x0)
        v1 = jnp.where(first, 0.0, jnp.where(i0 > i1, x1, one))
        tc[slot, 0] = jnp.where(i0 > i1, 0.0, x0)
        tc[slot, 1] = jnp.where(i0 > i1, 0.0, x1)
        pieces(slot, at, jnp.concatenate([v0, v1], axis=1))

        @pl.when(first & (q == 0))
        def _():
            factor_across(t).start()

        def rest(r0, n):
            a = pl.ds(r0, n)
            for side in range(2):
                load(t, l, side, vb.at[0, 0, a, :], a).wait()

            def sub(j, _):
                b = pl.ds(pl.multiple_of(r0 + j * NB, NB), NB)
                pieces(slot, b, vf[b, :])
                return 0

            lax.fori_loop(0, n // NB, sub, 0)

        partial(t, rest)

        def chunk(c, r0, n):
            a = pl.ds(r0, n)
            for side in range(2):
                load(t, c, side, vb.at[0, 0, a, :], a).wait()
            for j in range(0, n, NB):
                b = pl.ds(pl.multiple_of(r0 + j, NB), NB)
                pieces(slot, b, vf[b, :])

        full(t, chunk)

    def factor_across(t):
        return rcopy(tc.at[t % 3, 0], tb.at[t % 8], t_snd.at[0, t % 8], t_rcv.at[0, t % 8], across)

    def factor_over(t):
        return rcopy(tb.at[t % 8], tb.at[t % 8], t_snd.at[1, t % 8], t_rcv.at[1, t % 8], partner)

    def share_factor(t):
        @pl.when((r == 1) & (q == 0))
        def _():
            factor_across(t).wait_recv()

            @pl.when(t >= 2)
            def _():
                factor_over(t - 2).wait_send()

            factor_over(t).start()

    def late(t):
        return t > AHEAD + 1

    def part_copy(t):
        return rcopy(gs.at[t % 2], gp.at[t % 2], p_snd.at[t % 2], p_rcv.at[t % 2], partner)

    def plane_copy(t):
        return rcopy(gz.at[t % 2], gr.at[t % 2], g_snd.at[t % 2], g_rcv.at[t % 2], across)

    def total_copy(t):
        return rcopy(gf.at[t % 8], gf.at[t % 8], f_snd.at[t % 8], f_rcv.at[t % 8], partner)

    def gram_part(t):
        slot = t % 3
        s = t % 2

        @pl.when(t >= 2)
        def _():
            part_copy(t - 2).wait_send()

        gs[s] = jnp.zeros((NB, NB), F32)
        off = (sb_of(t) + t + q) % 2

        def one(j, _):
            at = chunk_at(sb_of(t) + off + 2 * j)
            a = [vn[slot, at, i * PW : i * PW + NB].T for i in range(3)]
            b = [vn[slot, at, i * PW + NB : (i + 1) * PW] for i in range(3)]
            x = mm(jnp.concatenate(a, axis=0), jnp.concatenate(b[0:2], axis=1))
            gs[s] += add_rows(add_rows(mm(a[0], b[2]), x[:, 0:NB], NB), x[0 : 2 * NB, NB:PW], NB)
            return 0

        lax.fori_loop(0, (height(t) - off + 1) // 2, one, 0)
        part_copy(t).start()

    def sends_plane(t):
        return late(t) | (t % 2 == q)

    def gram_plane(t):
        s = t % 2
        part_copy(t).wait_recv()

        @pl.when((t >= 2) & sends_plane(t - 2))
        def _():
            plane_copy(t - 2).wait_send()

        gz[s] = gs[s] + gp[s]

        @pl.when(sends_plane(t))
        def _():
            plane_copy(t).start()

    def gram_total(t):
        s = t % 2

        @pl.when(sends_plane(t))
        def _():
            plane_copy(t).wait_recv()

            @pl.when((t >= 8) & (t % 2 == q) & jnp.logical_not(late(t - 8)))
            def _():
                total_copy(t - 8).wait_send()

            gf[t % 8] = gz[s] + gr[s]

            @pl.when(jnp.logical_not(late(t)))
            def _():
                total_copy(t).start()

    def block_factor(t):
        slot = t % 3

        @pl.when(jnp.logical_not(sends_plane(t)))
        def _():
            total_copy(t).wait_recv()

        @pl.when((r == 1) & (q == 1))
        def _():
            factor_over(t).wait_recv()

        g = gf[t % 8]
        ta = jnp.where(r == 0, tc[slot, 0], tb[t % 8])
        tbb = tc[slot, 1]
        upper = -full_dot(mm, ta, full_dot(mm, g, tbb))
        for i, piece in enumerate(split3(ta)):
            tp[0:NB, i * PW : i * PW + NB] = piece
        for i, piece in enumerate(split3(upper)):
            tp[0:NB, i * PW + NB : (i + 1) * PW] = piece
        for i, piece in enumerate(split3(tbb)):
            tp[NB:PW, i * PW : i * PW + NB] = jnp.zeros((NB, NB), BF16)
            tp[NB:PW, i * PW + NB : (i + 1) * PW] = piece

    def w_copy(t, g):
        return rcopy(ws.at[t % 2, g], wr.at[t % 2, g], w_snd.at[t % 2, g], w_rcv.at[t % 2, g], across)

    def coefficients(t, g):
        with jax.named_scope("wwait"):
            w_copy(t, g).wait_recv()
        w = ws[t % 2, g] + wr[t % 2, g]
        y = stacked(mm_nt, jnp.concatenate(split3(w), axis=0), [tp[:, i * PW : (i + 1) * PW] for i in range(3)])
        for i, piece in enumerate(split3(y)):
            yp[i * NB : (i + 1) * NB] = piece

    def piece_of(t, i, at):
        return vn[t % 3, at, i * PW : (i + 1) * PW]

    def chunk_at(c):
        return pl.ds(pl.multiple_of(c * CH, CH), CH)

    def passes(m, i, g, n, finish):
        units = m * CH // UNIT
        base = rows - m * CH
        w = None
        for c in range(units + (0 if n is None else LAG)):
            at = pl.ds(base + c * UNIT, UNIT)
            an = pl.ds(max(0, base + (c - LAG) * UNIT), UNIT)
            u = None
            for j in range(3):
                k3 = (3 - j) * NB
                if n is not None and c >= LAG:
                    w = add_rows(w, mm(xp[g, 0:k3, an], piece_of(n, j, an)), NB)
                if c < units:
                    u = add_rows(u, mm_nt(yp[0:k3], piece_of(i, j, at)), NB)
            if c < units:
                finish(at, xt[g, :, at] - u)
        if n is not None:
            ws[n % 2, g] += w

    def product(n, g, at):
        w = None
        for j in range(3):
            w = add_rows(w, mm(xp[g, 0 : (3 - j) * NB, at], piece_of(n, j, at)), NB)
        ws[n % 2, g] += w

    def both(i, g):
        n = i + 1

        @pl.when(sb_of(n) < sb_of(i))
        def _():
            product(n, g, chunk_at(sb_of(n)))

        for m in range(1, nsb + 1):

            @pl.when(height(i) == m)
            def _(m=m):
                passes(m, i, g, n, lambda at, x: put_x(g, x, at))

    def out_copy(g, c):
        return pltpu.make_async_copy(zl.at[g, chunk_at(c), :], out_ref.at[chunk_at(c), lanes(g)], o_sem.at[g, c])

    def last(i, g):
        def finish(at, x):
            zl[g, at, :] = x.T

        passes(nsb, i, g, None, finish)

        def out(c, _):
            out_copy(g, c).start()
            return 0

        lax.fori_loop(0, nsb, out, 0)

    def step(i, _):
        n = i + 1
        early = i < AHEAD
        b = jnp.where(early, i + 2, n)
        brings = (i != AHEAD) & (b < npair)

        @pl.when(i < npair - 1)
        def _():
            with jax.named_scope("svc"):
                service(i)

        @pl.when(brings)
        def _():
            with jax.named_scope("loads"):
                start_loads(b)

        @pl.when(i >= 0)
        def _():
            with jax.named_scope("bfac"):
                block_factor(i)

        @pl.when(brings & jnp.logical_not(early))
        def _():
            with jax.named_scope("prep"):
                prep(b)
            with jax.named_scope("gram"):
                gram_part(b)

        @pl.when((n >= 0) & (n < npair) & (n % RING == 0))
        def _():
            with jax.named_scope("admit"):
                admit(sb_of(n))

        def group(g, _):
            @pl.when(i >= 0)
            def _():
                with jax.named_scope("coef"):
                    coefficients(i, g)

            @pl.when((n >= 0) & (n < npair))
            def _():
                @pl.when(n >= 2)
                def _():
                    w_copy(n - 2, g).wait_send()

                ws[n % 2, g] = jnp.zeros((NB, PW), F32)

            @pl.when(i == -1)
            def _():
                product(n, g, chunk_at(nsb - 1))

            @pl.when((i >= 0) & (n < npair))
            def _():
                with jax.named_scope("both"):
                    both(i, g)

            @pl.when((n >= 0) & (n < npair))
            def _():
                w_copy(n, g).start()

                @pl.when(g == jnp.where(i <= AHEAD, 0, 1))
                def _():
                    with jax.named_scope("fshare"):
                        share_factor(n)
                    with jax.named_scope("gtot"):
                        gram_total(n)

            @pl.when((g == 0) & brings & early)
            def _():
                with jax.named_scope("prep"):
                    prep(b)
                with jax.named_scope("gram"):
                    gram_part(b)

            @pl.when((g == jnp.where(early, 1, 0)) & brings)
            def _():
                with jax.named_scope("gplane"):
                    gram_plane(b)

            @pl.when(n == npair)
            def _():
                with jax.named_scope("last"):
                    last(i, g)

            return 0

        lax.fori_loop(0, 2, group, 0)

        @pl.when((n >= RING - 1) & (n + RING + 1 < npair))
        def _():
            z_piece(n + RING + 1).start()

        @pl.when((n >= 0) & (n % RING == 2) & (n + RING < npair))
        def _():
            z_local(sb_of(n) - 1).start()

        return 0

    barrier = pltpu.get_barrier_semaphore()
    for dev in (at_ring(rho + 1), at_ring(rho + RING - 1), partner, across):
        pl.semaphore_signal(barrier, inc=1, device_id=dev, device_id_type=MESH_ID)
    pl.semaphore_wait(barrier, 4)

    for j in range(min(2 * RING, npair)):
        z_piece(j).start()
    z_local(nsb - 1).start()
    with jax.named_scope("heads"):
        make_heads()
    lax.fori_loop(-2, npair, step, 0)

    for t in (npair - 2, npair - 1):
        for g in range(2):
            w_copy(t, g).wait_send()
    for t in (npair - 2, npair - 1):
        part_copy(t).wait_send()

        @pl.when(sends_plane(t))
        def _(t=t):
            plane_copy(t).wait_send()

    newest = min(npair - 1, AHEAD + 1)
    for t in range(max(0, npair - 8), newest + 1):

        @pl.when(t % 2 == q)
        def _(t=t):
            total_copy(t).wait_send()

    for t in range(npair - 3, npair):

        @pl.when((r == 0) & (q == 0))
        def _(t=t):
            factor_across(t).wait_send()

    for t in range(npair - 2, npair):

        @pl.when((r == 1) & (q == 0))
        def _(t=t):
            factor_over(t).wait_send()

    def drain(t, _):
        all_sent(t)
        return 0

    lax.fori_loop(max(0, npair - 8), npair, drain, 0)

    def out_done(c, _):
        for g in range(2):
            out_copy(g, c).wait()
        return 0

    lax.fori_loop(0, nsb, out_done, 0)


def solution(mesh):
    def local(v, t, z):
        rows, cols = v.shape
        nsb = cols // NB
        npair = nsb * RING
        hbm = pl.BlockSpec(memory_space=pltpu.MemorySpace.HBM)
        out, _ = pl.pallas_call(
            functools.partial(body, nsb),
            out_shape=(
                jax.ShapeDtypeStruct((rows, PW), F32),
                jax.ShapeDtypeStruct((2, npair, rows, NB), F32),
            ),
            in_specs=[hbm] * 3,
            out_specs=(hbm, hbm),
            scratch_shapes=[
                pltpu.VMEM((2, rows, NB), F32),
                pltpu.VMEM((2, NB, rows), F32),
                pltpu.VMEM((2, 3 * NB, rows), BF16),
                pltpu.VMEM((rows, PW), F32),
                pltpu.VMEM((3, rows, 3 * PW), BF16),
                pltpu.VMEM((8, NB, NB), F32),
                pltpu.VMEM((3, 2, NB, NB), F32),
                pltpu.VMEM((PW, 3 * PW), BF16),
                pltpu.VMEM((2, 2, NB, PW), F32),
                pltpu.VMEM((2, 2, NB, PW), F32),
                pltpu.VMEM((2, NB, NB), F32),
                pltpu.VMEM((2, NB, NB), F32),
                pltpu.VMEM((2, NB, NB), F32),
                pltpu.VMEM((2, NB, NB), F32),
                pltpu.VMEM((8, NB, NB), F32),
                pltpu.VMEM((3 * NB, PW), BF16),
                pltpu.VMEM((nsb, NB, NB), F32),
                pltpu.VMEM((nsb, NB, NB), F32),
            ],
            compiler_params=pltpu.CompilerParams(
                collective_id=0, has_side_effects=True, vmem_limit_bytes=60 * 2**20),
            name="backtransform",
        )(v, t, z)
        return out

    return jax.shard_map(local, mesh=mesh,
                         in_specs=(P("row", "col"), P("col", None, None), P(None, ("col", "row"))),
                         out_specs=P("row", "col"), check_vma=False)
```

```python
import functools

import jax
import jax.numpy as jnp
from jax import lax
from jax.experimental import pallas as pl
from jax.experimental.pallas import tpu as pltpu
from jax.sharding import PartitionSpec as P

F32 = jnp.float32
BF16 = jnp.bfloat16
MESH_ID = pl.DeviceIdType.MESH

NB = 128
PW = 2 * NB
CH = 4 * NB
UNIT = PW
LAG = 2
RING = 4
OWN_LEAD = 10
AHEAD = 20


def split3(x):
    hi = x.astype(BF16)
    rest = x - hi.astype(F32)
    mid = rest.astype(BF16)
    low = (rest - mid.astype(F32)).astype(BF16)
    return hi, mid, low


def mm(a, b):
    return lax.dot_general(a, b, (((1,), (0,)), ((), ())), preferred_element_type=F32)


def mm_nt(a, b):
    return lax.dot_general(a, b, (((1,), (1,)), ((), ())), preferred_element_type=F32)


def add_rows(total, x, n):
    for i in range(0, x.shape[0], n):
        part = x[i : i + n]
        total = part if total is None else total + part
    return total


def stacked(dot, a3, b):
    m = a3.shape[0] // 3
    s = None
    for i in range(3):
        s = add_rows(s, dot(a3[0 : (3 - i) * m], b[i]), m)
    return s


def full_dot(dot, a, b):
    return stacked(dot, jnp.concatenate(split3(a), axis=0), split3(b))


def body(nsb, v_ref, t_ref, z_ref, out_ref, vb, *scratch):
    rows = nsb * CH
    dma = pltpu.SemaphoreType.DMA
    npair = nsb * RING
    nc = nsb + 1
    pl.run_scoped(
        functools.partial(run, nsb, rows, npair, v_ref, t_ref, z_ref, out_ref, vb, scratch),
        dma((nsb,)),
        dma((npair,)),
        dma((npair,)),
        dma((npair, nc)),
        dma((npair, nc)),
        dma((2, 2)),
        dma((2, 2)),
        dma((2,)),
        dma((2,)),
        dma((8,)),
        dma((8,)),
        dma((2, nc)),
        dma((2, nsb)),
        dma((2, 8, nc)),
        dma((8, nc)),
        dma((2, nsb)),
        dma((2,)),
        dma((2,)),
        dma((2, 8)),
        dma((2, 8)),
    )


def run(nsb, rows, npair, v_ref, t_ref, z_ref, out_ref, vb, scratch, *sems):
    (zl, xt, xp, vf, vn, tb, tc, tp, ws, wr, gs, gp, gz, gr, gf, yp, eb, et) = scratch
    (z_loc, z_snd, z_rcv, i_rcv, d_rcv, w_snd, w_rcv, g_snd, g_rcv, f_snd, f_rcv, ld, o_sem, i_snd, d_snd, h_sem, p_snd, p_rcv, t_snd, t_rcv) = sems
    HEAD = nsb
    r = lax.axis_index("row")
    col = lax.axis_index("col")
    q = col % 2
    k = col // 2
    ky, kx = k // 2, k % 2
    rho = 2 * ky + (kx + ky) % 2

    def at_ring(i):
        i = i % RING
        y = i // 2
        x = (i % 2 + y) % 2
        return (r, (y * 2 + x) * 2 + q)

    partner = (r, k * 2 + 1 - q)
    across = (1 - r, col)

    def pair_of(t):
        return npair - 1 - t

    def sb_of(t):
        return pair_of(t) // RING

    def chip_of(t):
        return pair_of(t) % RING

    def owner_dist(t):
        kk = chip_of(t)
        y = kk // 2
        ro = 2 * y + (kk % 2 + y) % 2
        return (rho - ro + RING) % RING

    def height(t):
        return nsb - sb_of(t)

    def half_of(t, c):
        return (c - sb_of(t) + (height(t) - 1) // 2) % 2

    def head_half(t):
        return height(t) % 2

    def partial(t, fn):
        kk = chip_of(t)
        for j in range(RING - 1):

            @pl.when(kk == j)
            def _(j=j):
                fn(pl.multiple_of(sb_of(t) * CH + (j + 1) * NB, NB), CH - (j + 1) * NB)

    def full(t, fn):
        def one(c, _):
            fn(c, pl.multiple_of(c * CH, CH), CH)
            return 0

        lax.fori_loop(sb_of(t) + 1, nsb, one, 0)

    def head_rows(t):
        return pl.ds(pl.multiple_of(pair_of(t) * NB, NB), NB)

    def lanes(l):
        return pl.ds(pl.multiple_of(l * NB, NB), NB)

    def rcopy(src, dst, ssem, rsem, dev):
        return pltpu.make_async_remote_copy(src, dst, ssem, rsem, device_id=dev, device_id_type=MESH_ID)

    def panel(t, r0, n, own):
        if own:
            return v_ref.at[pl.ds(r0, n), lanes(sb_of(t))]
        return vb.at[q, pair_of(t), pl.ds(r0, n), :]

    def side_copy(src, dst, t, c, d):
        return rcopy(src, dst, i_snd.at[d, t % 8, c], i_rcv.at[t, c], at_ring(rho + 1 - 2 * d + RING))

    def core_copy(src, dst, t, c):
        return rcopy(src, dst, d_snd.at[t % 8, c], d_rcv.at[t, c], partner)

    def ends(t, c, own, r0=None, n=None):
        if c is HEAD:
            dst = vb.at[q, pair_of(t), head_rows(t), :]
            return (eb.at[sb_of(t)] if own else dst), dst
        return panel(t, r0, n, own), panel(t, r0, n, False)

    def wait_sent(t, c, half, r0=None, n=None):
        src, dst = ends(t, c, False, r0, n)
        d = owner_dist(t)

        @pl.when((d == 0) | ((d == 1) & (half == 0)))
        def _():
            side_copy(src, dst, t, c, 0).wait_send()

        @pl.when((d == 0) | ((d == 3) & (half == 1)))
        def _():
            side_copy(src, dst, t, c, 1).wait_send()

        core_copy(src, dst, t, c).wait_send()

    def all_sent(t):
        wait_sent(t, HEAD, head_half(t))

        partial(t, lambda r0, n: wait_sent(t, sb_of(t), half_of(t, sb_of(t)), r0, n))
        full(t, lambda c, r0, n: wait_sent(t, c, half_of(t, c), r0, n))

    def free_slot(t):
        @pl.when(t >= 8)
        def _():
            all_sent(t - 8)

    def send_own(u):
        first = RING - 1 - k
        part = (u - first + 2 * RING) % RING
        t = u - part
        quarter = RING

        @pl.when((t >= 0) & (t < npair))
        def _():
            def out(c, r0=None, n=None):
                src, dst = ends(t, c, True, r0, n)
                for d in range(2):
                    side_copy(src, dst, t, c, d).start()
                core_copy(src, dst, t, c).start()

            @pl.when(part == 0)
            def _():
                free_slot(t)
                out(HEAD)

                partial(t, lambda r0, n: out(sb_of(t), r0, n))

            m = height(t)
            lo = (part * m + quarter - 1) // quarter
            hi = ((part + 1) * m + quarter - 1) // quarter

            def one(i, _):
                c = sb_of(t) + i
                out(c, pl.multiple_of(c * CH, CH), CH)
                return 0

            lax.fori_loop(jnp.maximum(lo, 1), hi, one, 0)

    def pass_on(t, near):
        d = owner_dist(t)
        free_slot(t)

        def got(c, half, r0=None, n=None):
            src, dst = ends(t, c, False, r0, n)
            side_copy(src, dst, t, c, 0).wait_recv()
            core_copy(src, dst, t, c).start()
            if near:

                @pl.when((d == 1) & (half == 0))
                def _():
                    side_copy(src, dst, t, c, 0).start()

                @pl.when((d == 3) & (half == 1))
                def _():
                    side_copy(src, dst, t, c, 1).start()

        got(HEAD, head_half(t))

        partial(t, lambda r0, n: got(sb_of(t), half_of(t, sb_of(t)), r0, n))
        full(t, lambda c, r0, n: got(c, half_of(t, c), r0, n))

    def brought(i):
        return jnp.minimum(npair - 1, jnp.minimum(i + 2, jnp.maximum(AHEAD + 1, i + 1)))

    def near_lead(i):
        return jnp.minimum(npair - 1, brought(i) + jnp.minimum(3, i + 3))

    def far_lead(i):
        return brought(i)

    def own_lead(i):
        return jnp.minimum(npair + RING - 2, brought(i) + jnp.minimum(OWN_LEAD, 3 + 5 * (i + 2)))

    def span(lead, i):
        return jnp.where(i < -1, 0, lead(i - 1) + 1), lead(i) + 1

    def service(i):
        def one(j, _):
            kind = jnp.where(i < -1, j, 2 - j)

            @pl.when(kind == 0)
            def _():
                lo, hi = span(own_lead, i)
                lax.fori_loop(lo, hi, lambda u, _: (send_own(u), 0)[1], 0)

            @pl.when(kind == 1)
            def _():
                def near(t, _):
                    @pl.when(owner_dist(t) % 2 == 1)
                    def _():
                        pass_on(t, True)

                    return 0

                lo, hi = span(near_lead, i)
                lax.fori_loop(lo, hi, near, 0)

            @pl.when(kind == 2)
            def _():
                def far(t, _):
                    @pl.when(owner_dist(t) == 2)
                    def _():
                        pass_on(t, False)

                    return 0

                lo, hi = span(far_lead, i)
                lax.fori_loop(lo, hi, far, 0)

            return 0

        lax.fori_loop(0, 3, one, 0)

    def make_heads():
        def copies(l):
            rr = pl.ds(pl.multiple_of((l * RING + k) * NB, NB), NB)
            return (pltpu.make_async_copy(v_ref.at[rr, lanes(l)], eb.at[l], h_sem.at[0, l]),
                    pltpu.make_async_copy(t_ref.at[l], et.at[l], h_sem.at[1, l]))

        def begin(l, _):
            for c in copies(l):
                c.start()
            return 0

        lax.fori_loop(0, nsb, begin, 0)

        def one(l, _):
            for c in copies(l):
                c.wait()
            x = eb[l]
            tt = et[l]
            below = lax.broadcasted_iota(jnp.int32, (NB, NB), 0) > lax.broadcasted_iota(jnp.int32, (NB, NB), 1)
            both_in = jnp.where(below, x, tt)
            eb[l] = jnp.where(r == q, both_in, jnp.where(r == 0, tt, x))
            return 0

        lax.fori_loop(0, nsb, one, 0)

    def z_local(c):
        mine = pl.multiple_of(r * rows + c * CH, CH)
        return pltpu.make_async_copy(z_ref.at[pl.ds(mine, CH), :], zl.at[r, chunk_at(c), :], z_loc.at[c])

    def z_piece(w):
        c = nsb - 1 - w // RING
        r0 = c * CH + w % RING * NB
        theirs = pl.multiple_of((1 - r) * rows + r0, NB)
        return rcopy(z_ref.at[pl.ds(theirs, NB), :], zl.at[r, pl.ds(pl.multiple_of(r0, NB), NB), :],
                     z_snd.at[w], z_rcv.at[w], across)

    def put_x(g, x, at):
        xt[g, :, at] = x
        for i, piece in enumerate(split3(x)):
            xp[g, i * NB : (i + 1) * NB, at] = piece

    def admit(c):
        for j in range(RING):
            z_piece((nsb - 1 - c) * RING + j).wait()
        z_local(c).wait()

        def one(g, _):
            put_x(g, zl[g, chunk_at(c), :].T, chunk_at(c))
            return 0

        lax.fori_loop(0, 2, one, 0)

    def load(t, c, side, src, at):
        return pltpu.make_async_copy(src, vf.at[at, lanes(side)], ld.at[side, c])

    def start_loads(t):
        mine = owner_dist(t) == 0
        p = pair_of(t)

        def one(c, r0, n):
            at = pl.ds(r0, n)

            @pl.when(mine)
            def _():
                load(t, c, q, panel(t, r0, n, True), at).start()

            @pl.when(jnp.logical_not(mine))
            def _():
                load(t, c, q, panel(t, r0, n, False), at).start()

            src, dst = ends(t, c, False, r0, n)
            core_copy(src, dst, t, c).wait_recv()
            load(t, c, 1 - q, vb.at[1 - q, p, at, :], at).start()

        at = head_rows(t)

        @pl.when(jnp.logical_not(mine))
        def _():
            load(t, HEAD, q, vb.at[q, p, at, :], at).start()

        core_copy(*ends(t, HEAD, False), t, HEAD).wait_recv()
        load(t, HEAD, 1 - q, vb.at[1 - q, p, at, :], at).start()

        partial(t, lambda r0, n: one(sb_of(t), r0, n))
        full(t, one)

    def pieces(slot, at, x):
        for i, piece in enumerate(split3(x)):
            vn[slot, at, i * PW : (i + 1) * PW] = piece

    def prep(t):
        slot = t % 3
        mine = owner_dist(t) == 0
        at = head_rows(t)
        l = sb_of(t)

        load(t, HEAD, 1 - q, vb.at[0, 0, at, :], at).wait()

        @pl.when((r == 0) & (q == 0) & (t >= 3))
        def _():
            factor_across(t - 3).wait_send()

        @pl.when(mine)
        def _():
            vf[at, lanes(q)] = eb[l]

        @pl.when(jnp.logical_not(mine))
        def _():
            load(t, HEAD, q, vb.at[0, 0, at, :], at).wait()

        def above(j, _):
            pieces(slot, pl.ds(pl.multiple_of(l * CH + j * NB, NB), NB), jnp.zeros((NB, PW), F32))
            return 0

        lax.fori_loop(0, chip_of(t), above, 0)

        i0 = lax.broadcasted_iota(jnp.int32, (NB, NB), 0)
        i1 = lax.broadcasted_iota(jnp.int32, (NB, NB), 1)
        one = jnp.where(i0 == i1, 1.0, 0.0).astype(F32)
        x0 = vf[at, 0:NB]
        x1 = vf[at, NB:PW]
        first = r == 0
        v0 = jnp.where(first, jnp.where(i0 > i1, x0, one), x0)
        v1 = jnp.where(first, 0.0, jnp.where(i0 > i1, x1, one))
        tc[slot, 0] = jnp.where(i0 > i1, 0.0, x0)
        tc[slot, 1] = jnp.where(i0 > i1, 0.0, x1)
        pieces(slot, at, jnp.concatenate([v0, v1], axis=1))

        @pl.when(first & (q == 0))
        def _():
            factor_across(t).start()

        def rest(r0, n):
            a = pl.ds(r0, n)
            for side in range(2):
                load(t, l, side, vb.at[0, 0, a, :], a).wait()

            def sub(j, _):
                b = pl.ds(pl.multiple_of(r0 + j * NB, NB), NB)
                pieces(slot, b, vf[b, :])
                return 0

            lax.fori_loop(0, n // NB, sub, 0)

        partial(t, rest)

        def chunk(c, r0, n):
            a = pl.ds(r0, n)
            for side in range(2):
                load(t, c, side, vb.at[0, 0, a, :], a).wait()
            for j in range(0, n, NB):
                b = pl.ds(pl.multiple_of(r0 + j, NB), NB)
                pieces(slot, b, vf[b, :])

        full(t, chunk)

    def factor_across(t):
        return rcopy(tc.at[t % 3, 0], tb.at[t % 8], t_snd.at[0, t % 8], t_rcv.at[0, t % 8], across)

    def factor_over(t):
        return rcopy(tb.at[t % 8], tb.at[t % 8], t_snd.at[1, t % 8], t_rcv.at[1, t % 8], partner)

    def share_factor(t):
        @pl.when((r == 1) & (q == 0))
        def _():
            factor_across(t).wait_recv()

            @pl.when(t >= 2)
            def _():
                factor_over(t - 2).wait_send()

            factor_over(t).start()

    def late(t):
        return t > AHEAD + 1

    def part_copy(t):
        return rcopy(gs.at[t % 2], gp.at[t % 2], p_snd.at[t % 2], p_rcv.at[t % 2], partner)

    def plane_copy(t):
        return rcopy(gz.at[t % 2], gr.at[t % 2], g_snd.at[t % 2], g_rcv.at[t % 2], across)

    def total_copy(t):
        return rcopy(gf.at[t % 8], gf.at[t % 8], f_snd.at[t % 8], f_rcv.at[t % 8], partner)

    def gram_part(t):
        slot = t % 3
        s = t % 2

        @pl.when(t >= 2)
        def _():
            part_copy(t - 2).wait_send()

        gs[s] = jnp.zeros((NB, NB), F32)
        off = (sb_of(t) + t + q) % 2

        def one(j, _):
            at = chunk_at(sb_of(t) + off + 2 * j)
            a = [vn[slot, at, i * PW : i * PW + NB].T for i in range(3)]
            b = [vn[slot, at, i * PW + NB : (i + 1) * PW] for i in range(3)]
            x = mm(jnp.concatenate(a, axis=0), jnp.concatenate(b[0:2], axis=1))
            gs[s] += add_rows(add_rows(mm(a[0], b[2]), x[:, 0:NB], NB), x[0 : 2 * NB, NB:PW], NB)
            return 0

        lax.fori_loop(0, (height(t) - off + 1) // 2, one, 0)
        part_copy(t).start()

    def sends_plane(t):
        return late(t) | (t % 2 == q)

    def gram_plane(t):
        s = t % 2
        part_copy(t).wait_recv()

        @pl.when((t >= 2) & sends_plane(t - 2))
        def _():
            plane_copy(t - 2).wait_send()

        gz[s] = gs[s] + gp[s]

        @pl.when(sends_plane(t))
        def _():
            plane_copy(t).start()

    def gram_total(t):
        s = t % 2

        @pl.when(sends_plane(t))
        def _():
            plane_copy(t).wait_recv()

            @pl.when((t >= 8) & (t % 2 == q) & jnp.logical_not(late(t - 8)))
            def _():
                total_copy(t - 8).wait_send()

            gf[t % 8] = gz[s] + gr[s]

            @pl.when(jnp.logical_not(late(t)))
            def _():
                total_copy(t).start()

    def block_factor(t):
        slot = t % 3

        @pl.when(jnp.logical_not(sends_plane(t)))
        def _():
            total_copy(t).wait_recv()

        @pl.when((r == 1) & (q == 1))
        def _():
            factor_over(t).wait_recv()

        g = gf[t % 8]
        ta = jnp.where(r == 0, tc[slot, 0], tb[t % 8])
        tbb = tc[slot, 1]
        upper = -full_dot(mm, ta, full_dot(mm, g, tbb))
        for i, piece in enumerate(split3(ta)):
            tp[0:NB, i * PW : i * PW + NB] = piece
        for i, piece in enumerate(split3(upper)):
            tp[0:NB, i * PW + NB : (i + 1) * PW] = piece
        for i, piece in enumerate(split3(tbb)):
            tp[NB:PW, i * PW : i * PW + NB] = jnp.zeros((NB, NB), BF16)
            tp[NB:PW, i * PW + NB : (i + 1) * PW] = piece

    def w_copy(t, g):
        return rcopy(ws.at[t % 2, g], wr.at[t % 2, g], w_snd.at[t % 2, g], w_rcv.at[t % 2, g], across)

    def coefficients(t, g):
        with jax.named_scope("wwait"):
            w_copy(t, g).wait_recv()
        w = ws[t % 2, g] + wr[t % 2, g]
        y = stacked(mm_nt, jnp.concatenate(split3(w), axis=0), [tp[:, i * PW : (i + 1) * PW] for i in range(3)])
        for i, piece in enumerate(split3(y)):
            yp[i * NB : (i + 1) * NB] = piece

    def piece_of(t, i, at):
        return vn[t % 3, at, i * PW : (i + 1) * PW]

    def chunk_at(c):
        return pl.ds(pl.multiple_of(c * CH, CH), CH)

    def passes(m, i, g, n, finish):
        units = m * CH // UNIT
        base = rows - m * CH
        w = None
        for c in range(units + (0 if n is None else LAG)):
            at = pl.ds(base + c * UNIT, UNIT)
            an = pl.ds(max(0, base + (c - LAG) * UNIT), UNIT)
            u = None
            for j in range(3):
                k3 = (3 - j) * NB
                if n is not None and c >= LAG:
                    w = add_rows(w, mm(xp[g, 0:k3, an], piece_of(n, j, an)), NB)
                if c < units:
                    u = add_rows(u, mm_nt(yp[0:k3], piece_of(i, j, at)), NB)
            if c < units:
                finish(at, xt[g, :, at] - u)
        if n is not None:
            ws[n % 2, g] += w

    def product(n, g, at):
        w = None
        for j in range(3):
            w = add_rows(w, mm(xp[g, 0 : (3 - j) * NB, at], piece_of(n, j, at)), NB)
        ws[n % 2, g] += w

    def both(i, g):
        n = i + 1

        @pl.when(sb_of(n) < sb_of(i))
        def _():
            product(n, g, chunk_at(sb_of(n)))

        for m in range(1, nsb + 1):

            @pl.when(height(i) == m)
            def _(m=m):
                passes(m, i, g, n, lambda at, x: put_x(g, x, at))

    def out_copy(g, c):
        return pltpu.make_async_copy(zl.at[g, chunk_at(c), :], out_ref.at[chunk_at(c), lanes(g)], o_sem.at[g, c])

    def last(i, g):
        def finish(at, x):
            zl[g, at, :] = x.T

        passes(nsb, i, g, None, finish)

        def out(c, _):
            out_copy(g, c).start()
            return 0

        lax.fori_loop(0, nsb, out, 0)

    def step(i, _):
        n = i + 1
        early = i < AHEAD
        b = jnp.where(early, i + 2, n)
        brings = (i != AHEAD) & (b < npair)

        @pl.when(i < npair - 1)
        def _():
            with jax.named_scope("svc"):
                service(i)

        @pl.when(brings)
        def _():
            with jax.named_scope("loads"):
                start_loads(b)

        @pl.when(i >= 0)
        def _():
            with jax.named_scope("bfac"):
                block_factor(i)

        @pl.when((n >= 0) & (n < npair) & (n % RING == 0))
        def _():
            with jax.named_scope("admit"):
                admit(sb_of(n))

        def group(g, _):
            @pl.when((g == jnp.where(early, 1, 0)) & brings)
            def _():
                with jax.named_scope("prep"):
                    prep(b)
                with jax.named_scope("gram"):
                    gram_part(b)

            @pl.when(i >= 0)
            def _():
                with jax.named_scope("coef"):
                    coefficients(i, g)

            @pl.when((n >= 0) & (n < npair))
            def _():
                @pl.when(n >= 2)
                def _():
                    w_copy(n - 2, g).wait_send()

                ws[n % 2, g] = jnp.zeros((NB, PW), F32)

            @pl.when(i == -1)
            def _():
                product(n, g, chunk_at(nsb - 1))

            @pl.when((i >= 0) & (n < npair))
            def _():
                with jax.named_scope("both"):
                    both(i, g)

            @pl.when((g == 0) & brings & jnp.logical_not(early))
            def _():
                with jax.named_scope("gplane"):
                    gram_plane(b)

            @pl.when((n >= 0) & (n < npair))
            def _():
                w_copy(n, g).start()

                @pl.when(g == jnp.where(i <= AHEAD, 0, 1))
                def _():
                    with jax.named_scope("fshare"):
                        share_factor(n)
                    with jax.named_scope("gtot"):
                        gram_total(n)

            @pl.when((g == 1) & brings & early)
            def _():
                with jax.named_scope("gplane"):
                    gram_plane(b)

            @pl.when(n == npair)
            def _():
                with jax.named_scope("last"):
                    last(i, g)

            return 0

        lax.fori_loop(0, 2, group, 0)

        @pl.when((n >= RING - 1) & (n + RING + 1 < npair))
        def _():
            z_piece(n + RING + 1).start()

        @pl.when((n >= 0) & (n % RING == 2) & (n + RING < npair))
        def _():
            z_local(sb_of(n) - 1).start()

        return 0

    barrier = pltpu.get_barrier_semaphore()
    for dev in (at_ring(rho + 1), at_ring(rho + RING - 1), partner, across):
        pl.semaphore_signal(barrier, inc=1, device_id=dev, device_id_type=MESH_ID)
    pl.semaphore_wait(barrier, 4)

    for j in range(min(2 * RING, npair)):
        z_piece(j).start()
    z_local(nsb - 1).start()
    with jax.named_scope("heads"):
        make_heads()
    lax.fori_loop(-2, npair, step, 0)

    for t in (npair - 2, npair - 1):
        for g in range(2):
            w_copy(t, g).wait_send()
    for t in (npair - 2, npair - 1):
        part_copy(t).wait_send()

        @pl.when(sends_plane(t))
        def _(t=t):
            plane_copy(t).wait_send()

    newest = min(npair - 1, AHEAD + 1)
    for t in range(max(0, npair - 8), newest + 1):

        @pl.when(t % 2 == q)
        def _(t=t):
            total_copy(t).wait_send()

    for t in range(npair - 3, npair):

        @pl.when((r == 0) & (q == 0))
        def _(t=t):
            factor_across(t).wait_send()

    for t in range(npair - 2, npair):

        @pl.when((r == 1) & (q == 0))
        def _(t=t):
            factor_over(t).wait_send()

    def drain(t, _):
        all_sent(t)
        return 0

    lax.fori_loop(max(0, npair - 8), npair, drain, 0)

    def out_done(c, _):
        for g in range(2):
            out_copy(g, c).wait()
        return 0

    lax.fori_loop(0, nsb, out_done, 0)


def solution(mesh):
    def local(v, t, z):
        rows, cols = v.shape
        nsb = cols // NB
        npair = nsb * RING
        hbm = pl.BlockSpec(memory_space=pltpu.MemorySpace.HBM)
        out, _ = pl.pallas_call(
            functools.partial(body, nsb),
            out_shape=(
                jax.ShapeDtypeStruct((rows, PW), F32),
                jax.ShapeDtypeStruct((2, npair, rows, NB), F32),
            ),
            in_specs=[hbm] * 3,
            out_specs=(hbm, hbm),
            scratch_shapes=[
                pltpu.VMEM((2, rows, NB), F32),
                pltpu.VMEM((2, NB, rows), F32),
                pltpu.VMEM((2, 3 * NB, rows), BF16),
                pltpu.VMEM((rows, PW), F32),
                pltpu.VMEM((3, rows, 3 * PW), BF16),
                pltpu.VMEM((8, NB, NB), F32),
                pltpu.VMEM((3, 2, NB, NB), F32),
                pltpu.VMEM((PW, 3 * PW), BF16),
                pltpu.VMEM((2, 2, NB, PW), F32),
                pltpu.VMEM((2, 2, NB, PW), F32),
                pltpu.VMEM((2, NB, NB), F32),
                pltpu.VMEM((2, NB, NB), F32),
                pltpu.VMEM((2, NB, NB), F32),
                pltpu.VMEM((2, NB, NB), F32),
                pltpu.VMEM((8, NB, NB), F32),
                pltpu.VMEM((3 * NB, PW), BF16),
                pltpu.VMEM((nsb, NB, NB), F32),
                pltpu.VMEM((nsb, NB, NB), F32),
            ],
            compiler_params=pltpu.CompilerParams(
                collective_id=0, has_side_effects=True, vmem_limit_bytes=60 * 2**20),
            name="backtransform",
        )(v, t, z)
        return out

    return jax.shard_map(local, mesh=mesh,
                         in_specs=(P("row", "col"), P("col", None, None), P(None, ("col", "row"))),
                         out_specs=P("row", "col"), check_vma=False)
```

```python
import functools

import jax
import jax.numpy as jnp
from jax import lax
from jax.experimental import pallas as pl
from jax.experimental.pallas import tpu as pltpu
from jax.sharding import PartitionSpec as P

F32 = jnp.float32
BF16 = jnp.bfloat16
MESH_ID = pl.DeviceIdType.MESH

NB = 128
PW = 2 * NB
CH = 4 * NB
UNIT = PW
LAG = 2
RING = 4
OWN_LEAD = 10
AHEAD = 20


def split3(x):
    hi = x.astype(BF16)
    rest = x - hi.astype(F32)
    mid = rest.astype(BF16)
    low = (rest - mid.astype(F32)).astype(BF16)
    return hi, mid, low


def mm(a, b):
    return lax.dot_general(a, b, (((1,), (0,)), ((), ())), preferred_element_type=F32)


def mm_nt(a, b):
    return lax.dot_general(a, b, (((1,), (1,)), ((), ())), preferred_element_type=F32)


def add_rows(total, x, n):
    for i in range(0, x.shape[0], n):
        part = x[i : i + n]
        total = part if total is None else total + part
    return total


def stacked(dot, a3, b):
    m = a3.shape[0] // 3
    s = None
    for i in range(3):
        s = add_rows(s, dot(a3[0 : (3 - i) * m], b[i]), m)
    return s


def full_dot(a, b):
    ah, am, al = split3(a)
    bh, bm, bl = split3(b)
    n = a.shape[0]
    x = mm(jnp.concatenate([ah, am], axis=1), jnp.concatenate([jnp.concatenate([bh, bm], axis=1)] * 2, axis=0))
    y = mm(jnp.concatenate([al, ah], axis=1), jnp.concatenate([bh, bl], axis=0))
    return x[:, 0:n] + x[:, n:] + y


def body(nsb, v_ref, t_ref, z_ref, out_ref, vb, *scratch):
    rows = nsb * CH
    dma = pltpu.SemaphoreType.DMA
    npair = nsb * RING
    nc = nsb + 1
    pl.run_scoped(
        functools.partial(run, nsb, rows, npair, v_ref, t_ref, z_ref, out_ref, vb, scratch),
        dma((nsb,)),
        dma((npair,)),
        dma((npair,)),
        dma((npair, nc)),
        dma((npair, nc)),
        dma((2, 2)),
        dma((2, 2)),
        dma((2,)),
        dma((2,)),
        dma((8,)),
        dma((8,)),
        dma((2, nc)),
        dma((2, nsb)),
        dma((2, 8, nc)),
        dma((8, nc)),
        dma((2, nsb)),
        dma((2,)),
        dma((2,)),
        dma((2, 8)),
        dma((2, 8)),
    )


def run(nsb, rows, npair, v_ref, t_ref, z_ref, out_ref, vb, scratch, *sems):
    (zl, xt, xp, vf, vn, tb, tc, tp, ws, wr, gs, gp, gz, gr, gf, yp, eb, et) = scratch
    (z_loc, z_snd, z_rcv, i_rcv, d_rcv, w_snd, w_rcv, g_snd, g_rcv, f_snd, f_rcv, ld, o_sem, i_snd, d_snd, h_sem, p_snd, p_rcv, t_snd, t_rcv) = sems
    HEAD = nsb
    r = lax.axis_index("row")
    col = lax.axis_index("col")
    q = col % 2
    k = col // 2
    ky, kx = k // 2, k % 2
    rho = 2 * ky + (kx + ky) % 2

    def at_ring(i):
        i = i % RING
        y = i // 2
        x = (i % 2 + y) % 2
        return (r, (y * 2 + x) * 2 + q)

    partner = (r, k * 2 + 1 - q)
    across = (1 - r, col)

    def pair_of(t):
        return npair - 1 - t

    def sb_of(t):
        return pair_of(t) // RING

    def chip_of(t):
        return pair_of(t) % RING

    def owner_dist(t):
        kk = chip_of(t)
        y = kk // 2
        ro = 2 * y + (kk % 2 + y) % 2
        return (rho - ro + RING) % RING

    def height(t):
        return nsb - sb_of(t)

    def half_of(t, c):
        return (c - sb_of(t) + (height(t) - 1) // 2) % 2

    def head_half(t):
        return height(t) % 2

    def partial(t, fn):
        kk = chip_of(t)
        for j in range(RING - 1):

            @pl.when(kk == j)
            def _(j=j):
                fn(pl.multiple_of(sb_of(t) * CH + (j + 1) * NB, NB), CH - (j + 1) * NB)

    def full(t, fn):
        def one(c, _):
            fn(c, pl.multiple_of(c * CH, CH), CH)
            return 0

        lax.fori_loop(sb_of(t) + 1, nsb, one, 0)

    def head_rows(t):
        return pl.ds(pl.multiple_of(pair_of(t) * NB, NB), NB)

    def lanes(l):
        return pl.ds(pl.multiple_of(l * NB, NB), NB)

    def rcopy(src, dst, ssem, rsem, dev):
        return pltpu.make_async_remote_copy(src, dst, ssem, rsem, device_id=dev, device_id_type=MESH_ID)

    def panel(t, r0, n, own):
        if own:
            return v_ref.at[pl.ds(r0, n), lanes(sb_of(t))]
        return vb.at[q, pair_of(t), pl.ds(r0, n), :]

    def side_copy(src, dst, t, c, d):
        return rcopy(src, dst, i_snd.at[d, t % 8, c], i_rcv.at[t, c], at_ring(rho + 1 - 2 * d + RING))

    def core_copy(src, dst, t, c):
        return rcopy(src, dst, d_snd.at[t % 8, c], d_rcv.at[t, c], partner)

    def ends(t, c, own, r0=None, n=None):
        if c is HEAD:
            dst = vb.at[q, pair_of(t), head_rows(t), :]
            return (eb.at[sb_of(t)] if own else dst), dst
        return panel(t, r0, n, own), panel(t, r0, n, False)

    def wait_sent(t, c, half, r0=None, n=None):
        src, dst = ends(t, c, False, r0, n)
        d = owner_dist(t)

        @pl.when((d == 0) | ((d == 1) & (half == 0)))
        def _():
            side_copy(src, dst, t, c, 0).wait_send()

        @pl.when((d == 0) | ((d == 3) & (half == 1)))
        def _():
            side_copy(src, dst, t, c, 1).wait_send()

        core_copy(src, dst, t, c).wait_send()

    def all_sent(t):
        wait_sent(t, HEAD, head_half(t))

        partial(t, lambda r0, n: wait_sent(t, sb_of(t), half_of(t, sb_of(t)), r0, n))
        full(t, lambda c, r0, n: wait_sent(t, c, half_of(t, c), r0, n))

    def free_slot(t):
        @pl.when(t >= 8)
        def _():
            all_sent(t - 8)

    def send_own(u):
        first = RING - 1 - k
        part = (u - first + 2 * RING) % RING
        t = u - part
        quarter = RING

        @pl.when((t >= 0) & (t < npair))
        def _():
            def out(c, r0=None, n=None):
                src, dst = ends(t, c, True, r0, n)
                for d in range(2):
                    side_copy(src, dst, t, c, d).start()
                core_copy(src, dst, t, c).start()

            @pl.when(part == 0)
            def _():
                free_slot(t)
                out(HEAD)

                partial(t, lambda r0, n: out(sb_of(t), r0, n))

            m = height(t)
            lo = (part * m + quarter - 1) // quarter
            hi = ((part + 1) * m + quarter - 1) // quarter

            def one(i, _):
                c = sb_of(t) + i
                out(c, pl.multiple_of(c * CH, CH), CH)
                return 0

            lax.fori_loop(jnp.maximum(lo, 1), hi, one, 0)

    def pass_on(t, near):
        d = owner_dist(t)
        free_slot(t)

        def got(c, half, r0=None, n=None):
            src, dst = ends(t, c, False, r0, n)
            side_copy(src, dst, t, c, 0).wait_recv()
            core_copy(src, dst, t, c).start()
            if near:

                @pl.when((d == 1) & (half == 0))
                def _():
                    side_copy(src, dst, t, c, 0).start()

                @pl.when((d == 3) & (half == 1))
                def _():
                    side_copy(src, dst, t, c, 1).start()

        got(HEAD, head_half(t))

        partial(t, lambda r0, n: got(sb_of(t), half_of(t, sb_of(t)), r0, n))
        full(t, lambda c, r0, n: got(c, half_of(t, c), r0, n))

    def brought(i):
        return jnp.minimum(npair - 1, jnp.minimum(i + 2, jnp.maximum(AHEAD + 1, i + 1)))

    def near_lead(i):
        return jnp.minimum(npair - 1, brought(i) + jnp.minimum(3, i + 3))

    def far_lead(i):
        return brought(i)

    def own_lead(i):
        return jnp.minimum(npair + RING - 2, brought(i) + jnp.minimum(OWN_LEAD, 3 + 5 * (i + 2)))

    def span(lead, i):
        return jnp.where(i < -1, 0, lead(i - 1) + 1), lead(i) + 1

    def service(i):
        def one(j, _):
            kind = jnp.where(i < -1, j, 2 - j)

            @pl.when(kind == 0)
            def _():
                lo, hi = span(own_lead, i)
                lax.fori_loop(lo, hi, lambda u, _: (send_own(u), 0)[1], 0)

            @pl.when(kind == 1)
            def _():
                def near(t, _):
                    @pl.when(owner_dist(t) % 2 == 1)
                    def _():
                        pass_on(t, True)

                    return 0

                lo, hi = span(near_lead, i)
                lax.fori_loop(lo, hi, near, 0)

            @pl.when(kind == 2)
            def _():
                def far(t, _):
                    @pl.when(owner_dist(t) == 2)
                    def _():
                        pass_on(t, False)

                    return 0

                lo, hi = span(far_lead, i)
                lax.fori_loop(lo, hi, far, 0)

            return 0

        lax.fori_loop(0, 3, one, 0)

    def make_heads():
        def copies(l):
            rr = pl.ds(pl.multiple_of((l * RING + k) * NB, NB), NB)
            return (pltpu.make_async_copy(v_ref.at[rr, lanes(l)], eb.at[l], h_sem.at[0, l]),
                    pltpu.make_async_copy(t_ref.at[l], et.at[l], h_sem.at[1, l]))

        def begin(l, _):
            for c in copies(l):
                c.start()
            return 0

        lax.fori_loop(0, nsb, begin, 0)

        def one(l, _):
            for c in copies(l):
                c.wait()
            x = eb[l]
            tt = et[l]
            below = lax.broadcasted_iota(jnp.int32, (NB, NB), 0) > lax.broadcasted_iota(jnp.int32, (NB, NB), 1)
            both_in = jnp.where(below, x, tt)
            eb[l] = jnp.where(r == q, both_in, jnp.where(r == 0, tt, x))
            return 0

        lax.fori_loop(0, nsb, one, 0)

    def z_local(c):
        mine = pl.multiple_of(r * rows + c * CH, CH)
        return pltpu.make_async_copy(z_ref.at[pl.ds(mine, CH), :], zl.at[r, chunk_at(c), :], z_loc.at[c])

    def z_piece(w):
        c = nsb - 1 - w // RING
        r0 = c * CH + w % RING * NB
        theirs = pl.multiple_of((1 - r) * rows + r0, NB)
        return rcopy(z_ref.at[pl.ds(theirs, NB), :], zl.at[r, pl.ds(pl.multiple_of(r0, NB), NB), :],
                     z_snd.at[w], z_rcv.at[w], across)

    def put_x(g, x, at):
        xt[g, :, at] = x
        for i, piece in enumerate(split3(x)):
            xp[g, i * NB : (i + 1) * NB, at] = piece

    def admit(c):
        for j in range(RING):
            z_piece((nsb - 1 - c) * RING + j).wait()
        z_local(c).wait()

        def one(g, _):
            put_x(g, zl[g, chunk_at(c), :].T, chunk_at(c))
            return 0

        lax.fori_loop(0, 2, one, 0)

    def load(t, c, side, src, at):
        return pltpu.make_async_copy(src, vf.at[at, lanes(side)], ld.at[side, c])

    def start_loads(t):
        mine = owner_dist(t) == 0
        p = pair_of(t)

        def one(c, r0, n):
            at = pl.ds(r0, n)

            @pl.when(mine)
            def _():
                load(t, c, q, panel(t, r0, n, True), at).start()

            @pl.when(jnp.logical_not(mine))
            def _():
                load(t, c, q, panel(t, r0, n, False), at).start()

            src, dst = ends(t, c, False, r0, n)
            core_copy(src, dst, t, c).wait_recv()
            load(t, c, 1 - q, vb.at[1 - q, p, at, :], at).start()

        at = head_rows(t)

        @pl.when(jnp.logical_not(mine))
        def _():
            load(t, HEAD, q, vb.at[q, p, at, :], at).start()

        core_copy(*ends(t, HEAD, False), t, HEAD).wait_recv()
        load(t, HEAD, 1 - q, vb.at[1 - q, p, at, :], at).start()

        partial(t, lambda r0, n: one(sb_of(t), r0, n))
        full(t, one)

    def pieces(slot, at, x):
        for i, piece in enumerate(split3(x)):
            vn[slot, at, i * PW : (i + 1) * PW] = piece

    def prep(t):
        slot = t % 3
        mine = owner_dist(t) == 0
        at = head_rows(t)
        l = sb_of(t)

        load(t, HEAD, 1 - q, vb.at[0, 0, at, :], at).wait()

        @pl.when((r == 0) & (q == 0) & (t >= 3))
        def _():
            factor_across(t - 3).wait_send()

        @pl.when(mine)
        def _():
            vf[at, lanes(q)] = eb[l]

        @pl.when(jnp.logical_not(mine))
        def _():
            load(t, HEAD, q, vb.at[0, 0, at, :], at).wait()

        def above(j, _):
            pieces(slot, pl.ds(pl.multiple_of(l * CH + j * NB, NB), NB), jnp.zeros((NB, PW), F32))
            return 0

        lax.fori_loop(0, chip_of(t), above, 0)

        i0 = lax.broadcasted_iota(jnp.int32, (NB, NB), 0)
        i1 = lax.broadcasted_iota(jnp.int32, (NB, NB), 1)
        one = jnp.where(i0 == i1, 1.0, 0.0).astype(F32)
        x0 = vf[at, 0:NB]
        x1 = vf[at, NB:PW]
        first = r == 0
        v0 = jnp.where(first, jnp.where(i0 > i1, x0, one), x0)
        v1 = jnp.where(first, 0.0, jnp.where(i0 > i1, x1, one))
        tc[slot, 0] = jnp.where(i0 > i1, 0.0, x0)
        tc[slot, 1] = jnp.where(i0 > i1, 0.0, x1)
        pieces(slot, at, jnp.concatenate([v0, v1], axis=1))

        @pl.when(first & (q == 0))
        def _():
            factor_across(t).start()

        def rest(r0, n):
            a = pl.ds(r0, n)
            for side in range(2):
                load(t, l, side, vb.at[0, 0, a, :], a).wait()

            def sub(j, _):
                b = pl.ds(pl.multiple_of(r0 + j * NB, NB), NB)
                pieces(slot, b, vf[b, :])
                return 0

            lax.fori_loop(0, n // NB, sub, 0)

        partial(t, rest)

        def chunk(c, r0, n):
            a = pl.ds(r0, n)
            for side in range(2):
                load(t, c, side, vb.at[0, 0, a, :], a).wait()
            for j in range(0, n, NB):
                b = pl.ds(pl.multiple_of(r0 + j, NB), NB)
                pieces(slot, b, vf[b, :])

        full(t, chunk)

    def factor_across(t):
        return rcopy(tc.at[t % 3, 0], tb.at[t % 8], t_snd.at[0, t % 8], t_rcv.at[0, t % 8], across)

    def factor_over(t):
        return rcopy(tb.at[t % 8], tb.at[t % 8], t_snd.at[1, t % 8], t_rcv.at[1, t % 8], partner)

    def share_factor(t):
        @pl.when((r == 1) & (q == 0))
        def _():
            factor_across(t).wait_recv()

            @pl.when(t >= 2)
            def _():
                factor_over(t - 2).wait_send()

            factor_over(t).start()

    def late(t):
        return t > AHEAD + 1

    def part_copy(t):
        return rcopy(gs.at[t % 2], gp.at[t % 2], p_snd.at[t % 2], p_rcv.at[t % 2], partner)

    def plane_copy(t):
        return rcopy(gz.at[t % 2], gr.at[t % 2], g_snd.at[t % 2], g_rcv.at[t % 2], across)

    def total_copy(t):
        return rcopy(gf.at[t % 8], gf.at[t % 8], f_snd.at[t % 8], f_rcv.at[t % 8], partner)

    def gram_part(t):
        slot = t % 3
        s = t % 2

        @pl.when(t >= 2)
        def _():
            part_copy(t - 2).wait_send()

        gs[s] = jnp.zeros((NB, NB), F32)
        off = (sb_of(t) + t + q) % 2

        def one(j, _):
            at = chunk_at(sb_of(t) + off + 2 * j)
            a = [vn[slot, at, i * PW : i * PW + NB].T for i in range(3)]
            b = [vn[slot, at, i * PW + NB : (i + 1) * PW] for i in range(3)]
            x = mm(jnp.concatenate(a, axis=0), jnp.concatenate(b[0:2], axis=1))
            gs[s] += add_rows(add_rows(mm(a[0], b[2]), x[:, 0:NB], NB), x[0 : 2 * NB, NB:PW], NB)
            return 0

        lax.fori_loop(0, (height(t) - off + 1) // 2, one, 0)
        part_copy(t).start()

    def sends_plane(t):
        return late(t) | (t % 2 == q)

    def gram_plane(t):
        s = t % 2
        part_copy(t).wait_recv()

        @pl.when((t >= 2) & sends_plane(t - 2))
        def _():
            plane_copy(t - 2).wait_send()

        gz[s] = gs[s] + gp[s]

        @pl.when(sends_plane(t))
        def _():
            plane_copy(t).start()

    def gram_total(t):
        s = t % 2

        @pl.when(sends_plane(t))
        def _():
            plane_copy(t).wait_recv()

            @pl.when((t >= 8) & (t % 2 == q) & jnp.logical_not(late(t - 8)))
            def _():
                total_copy(t - 8).wait_send()

            gf[t % 8] = gz[s] + gr[s]

            @pl.when(jnp.logical_not(late(t)))
            def _():
                total_copy(t).start()

    def block_factor(t):
        slot = t % 3

        @pl.when(jnp.logical_not(sends_plane(t)))
        def _():
            total_copy(t).wait_recv()

        @pl.when((r == 1) & (q == 1))
        def _():
            factor_over(t).wait_recv()

        g = gf[t % 8]
        ta = jnp.where(r == 0, tc[slot, 0], tb[t % 8])
        tbb = tc[slot, 1]
        upper = -full_dot(ta, full_dot(g, tbb))
        for i, piece in enumerate(split3(ta)):
            tp[0:NB, i * PW : i * PW + NB] = piece
        for i, piece in enumerate(split3(upper)):
            tp[0:NB, i * PW + NB : (i + 1) * PW] = piece
        for i, piece in enumerate(split3(tbb)):
            tp[NB:PW, i * PW : i * PW + NB] = jnp.zeros((NB, NB), BF16)
            tp[NB:PW, i * PW + NB : (i + 1) * PW] = piece

    def w_copy(t, g):
        return rcopy(ws.at[t % 2, g], wr.at[t % 2, g], w_snd.at[t % 2, g], w_rcv.at[t % 2, g], across)

    def coefficients(t, g):
        with jax.named_scope("wwait"):
            w_copy(t, g).wait_recv()
        w = ws[t % 2, g] + wr[t % 2, g]
        y = stacked(mm_nt, jnp.concatenate(split3(w), axis=0), [tp[:, i * PW : (i + 1) * PW] for i in range(3)])
        for i, piece in enumerate(split3(y)):
            yp[i * NB : (i + 1) * NB] = piece

    def piece_of(t, i, at):
        return vn[t % 3, at, i * PW : (i + 1) * PW]

    def chunk_at(c):
        return pl.ds(pl.multiple_of(c * CH, CH), CH)

    def passes(m, i, g, n, finish):
        units = m * CH // UNIT
        base = rows - m * CH
        w = None
        for c in range(units + (0 if n is None else LAG)):
            at = pl.ds(base + c * UNIT, UNIT)
            an = pl.ds(max(0, base + (c - LAG) * UNIT), UNIT)
            u = None
            for j in range(3):
                k3 = (3 - j) * NB
                if n is not None and c >= LAG:
                    w = add_rows(w, mm(xp[g, 0:k3, an], piece_of(n, j, an)), NB)
                if c < units:
                    u = add_rows(u, mm_nt(yp[0:k3], piece_of(i, j, at)), NB)
            if c < units:
                finish(at, xt[g, :, at] - u)
        if n is not None:
            ws[n % 2, g] += w

    def product(n, g, at):
        w = None
        for j in range(3):
            w = add_rows(w, mm(xp[g, 0 : (3 - j) * NB, at], piece_of(n, j, at)), NB)
        ws[n % 2, g] += w

    def both(i, g):
        n = i + 1

        @pl.when(sb_of(n) < sb_of(i))
        def _():
            product(n, g, chunk_at(sb_of(n)))

        for m in range(1, nsb + 1):

            @pl.when(height(i) == m)
            def _(m=m):
                passes(m, i, g, n, lambda at, x: put_x(g, x, at))

    def out_copy(g, c):
        return pltpu.make_async_copy(zl.at[g, chunk_at(c), :], out_ref.at[chunk_at(c), lanes(g)], o_sem.at[g, c])

    def last(i, g):
        def finish(at, x):
            zl[g, at, :] = x.T

        passes(nsb, i, g, None, finish)

        def out(c, _):
            out_copy(g, c).start()
            return 0

        lax.fori_loop(0, nsb, out, 0)

    def step(i, _):
        n = i + 1
        early = i < AHEAD
        b = jnp.where(early, i + 2, n)
        brings = (i != AHEAD) & (b < npair)

        @pl.when(i < npair - 1)
        def _():
            with jax.named_scope("svc"):
                service(i)

        @pl.when(brings)
        def _():
            with jax.named_scope("loads"):
                start_loads(b)

        @pl.when(i >= 0)
        def _():
            with jax.named_scope("bfac"):
                block_factor(i)

        @pl.when((n >= 0) & (n < npair) & (n % RING == 0))
        def _():
            with jax.named_scope("admit"):
                admit(sb_of(n))

        def group(g, _):
            @pl.when(i >= 0)
            def _():
                with jax.named_scope("coef"):
                    coefficients(i, g)

            @pl.when((g == 0) & brings)
            def _():
                with jax.named_scope("prep"):
                    prep(b)
                with jax.named_scope("gram"):
                    gram_part(b)

            @pl.when((n >= 0) & (n < npair))
            def _():
                @pl.when(n >= 2)
                def _():
                    w_copy(n - 2, g).wait_send()

                ws[n % 2, g] = jnp.zeros((NB, PW), F32)

            @pl.when(i == -1)
            def _():
                product(n, g, chunk_at(nsb - 1))

            @pl.when((i >= 0) & (n < npair))
            def _():
                with jax.named_scope("both"):
                    both(i, g)

            @pl.when((n >= 0) & (n < npair) & (g == jnp.where(i <= AHEAD, 0, 1)))
            def _():
                with jax.named_scope("fshare"):
                    share_factor(n)
                with jax.named_scope("gtot"):
                    gram_total(n)

            @pl.when((g == 0) & brings)
            def _():
                with jax.named_scope("gplane"):
                    gram_plane(b)

            @pl.when((n >= 0) & (n < npair))
            def _():
                w_copy(n, g).start()

            @pl.when(n == npair)
            def _():
                with jax.named_scope("last"):
                    last(i, g)

            return 0

        lax.fori_loop(0, 2, group, 0)

        @pl.when((n >= RING - 1) & (n + RING + 1 < npair))
        def _():
            z_piece(n + RING + 1).start()

        @pl.when((n >= 0) & (n % RING == 2) & (n + RING < npair))
        def _():
            z_local(sb_of(n) - 1).start()

        return 0

    barrier = pltpu.get_barrier_semaphore()
    for dev in (at_ring(rho + 1), at_ring(rho + RING - 1), partner, across):
        pl.semaphore_signal(barrier, inc=1, device_id=dev, device_id_type=MESH_ID)
    pl.semaphore_wait(barrier, 4)

    for j in range(min(2 * RING, npair)):
        z_piece(j).start()
    z_local(nsb - 1).start()
    with jax.named_scope("heads"):
        make_heads()
    lax.fori_loop(-2, npair, step, 0)

    for t in (npair - 2, npair - 1):
        for g in range(2):
            w_copy(t, g).wait_send()
    for t in (npair - 2, npair - 1):
        part_copy(t).wait_send()

        @pl.when(sends_plane(t))
        def _(t=t):
            plane_copy(t).wait_send()

    newest = min(npair - 1, AHEAD + 1)
    for t in range(max(0, npair - 8), newest + 1):

        @pl.when(t % 2 == q)
        def _(t=t):
            total_copy(t).wait_send()

    for t in range(npair - 3, npair):

        @pl.when((r == 0) & (q == 0))
        def _(t=t):
            factor_across(t).wait_send()

    for t in range(npair - 2, npair):

        @pl.when((r == 1) & (q == 0))
        def _(t=t):
            factor_over(t).wait_send()

    def drain(t, _):
        all_sent(t)
        return 0

    lax.fori_loop(max(0, npair - 8), npair, drain, 0)

    def out_done(c, _):
        for g in range(2):
            out_copy(g, c).wait()
        return 0

    lax.fori_loop(0, nsb, out_done, 0)


def solution(mesh):
    def local(v, t, z):
        rows, cols = v.shape
        nsb = cols // NB
        npair = nsb * RING
        hbm = pl.BlockSpec(memory_space=pltpu.MemorySpace.HBM)
        out, _ = pl.pallas_call(
            functools.partial(body, nsb),
            out_shape=(
                jax.ShapeDtypeStruct((rows, PW), F32),
                jax.ShapeDtypeStruct((2, npair, rows, NB), F32),
            ),
            in_specs=[hbm] * 3,
            out_specs=(hbm, hbm),
            scratch_shapes=[
                pltpu.VMEM((2, rows, NB), F32),
                pltpu.VMEM((2, NB, rows), F32),
                pltpu.VMEM((2, 3 * NB, rows), BF16),
                pltpu.VMEM((rows, PW), F32),
                pltpu.VMEM((3, rows, 3 * PW), BF16),
                pltpu.VMEM((8, NB, NB), F32),
                pltpu.VMEM((3, 2, NB, NB), F32),
                pltpu.VMEM((PW, 3 * PW), BF16),
                pltpu.VMEM((2, 2, NB, PW), F32),
                pltpu.VMEM((2, 2, NB, PW), F32),
                pltpu.VMEM((2, NB, NB), F32),
                pltpu.VMEM((2, NB, NB), F32),
                pltpu.VMEM((2, NB, NB), F32),
                pltpu.VMEM((2, NB, NB), F32),
                pltpu.VMEM((8, NB, NB), F32),
                pltpu.VMEM((3 * NB, PW), BF16),
                pltpu.VMEM((nsb, NB, NB), F32),
                pltpu.VMEM((nsb, NB, NB), F32),
            ],
            compiler_params=pltpu.CompilerParams(
                collective_id=0, has_side_effects=True, vmem_limit_bytes=60 * 2**20),
            name="backtransform",
        )(v, t, z)
        return out

    return jax.shard_map(local, mesh=mesh,
                         in_specs=(P("row", "col"), P("col", None, None), P(None, ("col", "row"))),
                         out_specs=P("row", "col"), check_vma=False)
```

```python
import functools

import jax
import jax.numpy as jnp
from jax import lax
from jax.experimental import pallas as pl
from jax.experimental.pallas import tpu as pltpu
from jax.sharding import PartitionSpec as P

F32 = jnp.float32
BF16 = jnp.bfloat16
MESH_ID = pl.DeviceIdType.MESH

NB = 128
PW = 2 * NB
CH = 4 * NB
UNIT = PW
LAG = 2
RING = 4
OWN_LEAD = 10
AHEAD = 20


def split3(x):
    hi = x.astype(BF16)
    rest = x - hi.astype(F32)
    mid = rest.astype(BF16)
    low = (rest - mid.astype(F32)).astype(BF16)
    return hi, mid, low


def mm(a, b):
    return lax.dot_general(a, b, (((1,), (0,)), ((), ())), preferred_element_type=F32)


def mm_nt(a, b):
    return lax.dot_general(a, b, (((1,), (1,)), ((), ())), preferred_element_type=F32)


def add_rows(total, x, n):
    for i in range(0, x.shape[0], n):
        part = x[i : i + n]
        total = part if total is None else total + part
    return total


def stacked(dot, a3, b):
    m = a3.shape[0] // 3
    s = None
    for i in range(3):
        s = add_rows(s, dot(a3[0 : (3 - i) * m], b[i]), m)
    return s


def full_dot(a, b):
    ah, am, al = split3(a)
    bh, bm, bl = split3(b)
    n = a.shape[0]
    x = mm(jnp.concatenate([ah, am], axis=1), jnp.concatenate([jnp.concatenate([bh, bm], axis=1)] * 2, axis=0))
    y = mm(jnp.concatenate([al, ah], axis=1), jnp.concatenate([bh, bl], axis=0))
    return x[:, 0:n] + x[:, n:] + y


def body(nsb, v_ref, t_ref, z_ref, out_ref, vb, *scratch):
    rows = nsb * CH
    dma = pltpu.SemaphoreType.DMA
    npair = nsb * RING
    nc = nsb + 1
    pl.run_scoped(
        functools.partial(run, nsb, rows, npair, v_ref, t_ref, z_ref, out_ref, vb, scratch),
        dma((nsb,)),
        dma((npair,)),
        dma((npair,)),
        dma((npair, nc)),
        dma((npair, nc)),
        dma((2, 2)),
        dma((2, 2)),
        dma((2,)),
        dma((2,)),
        dma((8,)),
        dma((8,)),
        dma((2, nc)),
        dma((2, nsb)),
        dma((2, 8, nc)),
        dma((8, nc)),
        dma((2, nsb)),
        dma((2,)),
        dma((2,)),
        dma((2, 8)),
        dma((2, 8)),
    )


def run(nsb, rows, npair, v_ref, t_ref, z_ref, out_ref, vb, scratch, *sems):
    (zl, xt, xp, vf, vn, tb, tc, tp, ws, wr, gs, gp, gz, gr, gf, yp, eb, et) = scratch
    (z_loc, z_snd, z_rcv, i_rcv, d_rcv, w_snd, w_rcv, g_snd, g_rcv, f_snd, f_rcv, ld, o_sem, i_snd, d_snd, h_sem, p_snd, p_rcv, t_snd, t_rcv) = sems
    HEAD = nsb
    r = lax.axis_index("row")
    col = lax.axis_index("col")
    q = col % 2
    k = col // 2
    ky, kx = k // 2, k % 2
    rho = 2 * ky + (kx + ky) % 2

    def at_ring(i):
        i = i % RING
        y = i // 2
        x = (i % 2 + y) % 2
        return (r, (y * 2 + x) * 2 + q)

    partner = (r, k * 2 + 1 - q)
    across = (1 - r, col)

    def pair_of(t):
        return npair - 1 - t

    def sb_of(t):
        return pair_of(t) // RING

    def chip_of(t):
        return pair_of(t) % RING

    def owner_dist(t):
        kk = chip_of(t)
        y = kk // 2
        ro = 2 * y + (kk % 2 + y) % 2
        return (rho - ro + RING) % RING

    def height(t):
        return nsb - sb_of(t)

    def half_of(t, c):
        return (c - sb_of(t) + (height(t) - 1) // 2) % 2

    def head_half(t):
        return height(t) % 2

    def partial(t, fn):
        kk = chip_of(t)
        for j in range(RING - 1):

            @pl.when(kk == j)
            def _(j=j):
                fn(pl.multiple_of(sb_of(t) * CH + (j + 1) * NB, NB), CH - (j + 1) * NB)

    def full(t, fn):
        def one(c, _):
            fn(c, pl.multiple_of(c * CH, CH), CH)
            return 0

        lax.fori_loop(sb_of(t) + 1, nsb, one, 0)

    def head_rows(t):
        return pl.ds(pl.multiple_of(pair_of(t) * NB, NB), NB)

    def lanes(l):
        return pl.ds(pl.multiple_of(l * NB, NB), NB)

    def rcopy(src, dst, ssem, rsem, dev):
        return pltpu.make_async_remote_copy(src, dst, ssem, rsem, device_id=dev, device_id_type=MESH_ID)

    def panel(t, r0, n, own):
        if own:
            return v_ref.at[pl.ds(r0, n), lanes(sb_of(t))]
        return vb.at[q, pair_of(t), pl.ds(r0, n), :]

    def side_copy(src, dst, t, c, d):
        return rcopy(src, dst, i_snd.at[d, t % 8, c], i_rcv.at[t, c], at_ring(rho + 1 - 2 * d + RING))

    def core_copy(src, dst, t, c):
        return rcopy(src, dst, d_snd.at[t % 8, c], d_rcv.at[t, c], partner)

    def ends(t, c, own, r0=None, n=None):
        if c is HEAD:
            dst = vb.at[q, pair_of(t), head_rows(t), :]
            return (eb.at[sb_of(t)] if own else dst), dst
        return panel(t, r0, n, own), panel(t, r0, n, False)

    def wait_sent(t, c, half, r0=None, n=None):
        src, dst = ends(t, c, False, r0, n)
        d = owner_dist(t)

        @pl.when((d == 0) | ((d == 1) & (half == 0)))
        def _():
            side_copy(src, dst, t, c, 0).wait_send()

        @pl.when((d == 0) | ((d == 3) & (half == 1)))
        def _():
            side_copy(src, dst, t, c, 1).wait_send()

        core_copy(src, dst, t, c).wait_send()

    def all_sent(t):
        wait_sent(t, HEAD, head_half(t))

        partial(t, lambda r0, n: wait_sent(t, sb_of(t), half_of(t, sb_of(t)), r0, n))
        full(t, lambda c, r0, n: wait_sent(t, c, half_of(t, c), r0, n))

    def free_slot(t):
        @pl.when(t >= 8)
        def _():
            all_sent(t - 8)

    def send_own(u):
        first = RING - 1 - k
        part = (u - first + 2 * RING) % RING
        t = u - part
        quarter = RING

        @pl.when((t >= 0) & (t < npair))
        def _():
            def out(c, r0=None, n=None):
                src, dst = ends(t, c, True, r0, n)
                for d in range(2):
                    side_copy(src, dst, t, c, d).start()
                core_copy(src, dst, t, c).start()

            @pl.when(part == 0)
            def _():
                free_slot(t)
                out(HEAD)

                partial(t, lambda r0, n: out(sb_of(t), r0, n))

            m = height(t)
            lo = (part * m + quarter - 1) // quarter
            hi = ((part + 1) * m + quarter - 1) // quarter

            def one(i, _):
                c = sb_of(t) + i
                out(c, pl.multiple_of(c * CH, CH), CH)
                return 0

            lax.fori_loop(jnp.maximum(lo, 1), hi, one, 0)

    def pass_on(t, near):
        d = owner_dist(t)
        free_slot(t)

        def got(c, half, r0=None, n=None):
            src, dst = ends(t, c, False, r0, n)
            side_copy(src, dst, t, c, 0).wait_recv()
            core_copy(src, dst, t, c).start()
            if near:

                @pl.when((d == 1) & (half == 0))
                def _():
                    side_copy(src, dst, t, c, 0).start()

                @pl.when((d == 3) & (half == 1))
                def _():
                    side_copy(src, dst, t, c, 1).start()

        got(HEAD, head_half(t))

        partial(t, lambda r0, n: got(sb_of(t), half_of(t, sb_of(t)), r0, n))
        full(t, lambda c, r0, n: got(c, half_of(t, c), r0, n))

    def brought(i):
        return jnp.minimum(npair - 1, jnp.minimum(i + 2, jnp.maximum(AHEAD + 1, i + 1)))

    def near_lead(i):
        return jnp.minimum(npair - 1, brought(i) + jnp.minimum(3, i + 3))

    def far_lead(i):
        return brought(i)

    def own_lead(i):
        return jnp.minimum(npair + RING - 2, brought(i) + jnp.minimum(OWN_LEAD, 3 + 5 * (i + 2)))

    def span(lead, i):
        return jnp.where(i < -1, 0, lead(i - 1) + 1), lead(i) + 1

    def service(i):
        def one(j, _):
            kind = jnp.where(i < -1, j, 2 - j)

            @pl.when(kind == 0)
            def _():
                lo, hi = span(own_lead, i)
                lax.fori_loop(lo, hi, lambda u, _: (send_own(u), 0)[1], 0)

            @pl.when(kind == 1)
            def _():
                def near(t, _):
                    @pl.when(owner_dist(t) % 2 == 1)
                    def _():
                        pass_on(t, True)

                    return 0

                lo, hi = span(near_lead, i)
                lax.fori_loop(lo, hi, near, 0)

            @pl.when(kind == 2)
            def _():
                def far(t, _):
                    @pl.when(owner_dist(t) == 2)
                    def _():
                        pass_on(t, False)

                    return 0

                lo, hi = span(far_lead, i)
                lax.fori_loop(lo, hi, far, 0)

            return 0

        lax.fori_loop(0, 3, one, 0)

    def make_heads():
        def copies(l):
            rr = pl.ds(pl.multiple_of((l * RING + k) * NB, NB), NB)
            return (pltpu.make_async_copy(v_ref.at[rr, lanes(l)], eb.at[l], h_sem.at[0, l]),
                    pltpu.make_async_copy(t_ref.at[l], et.at[l], h_sem.at[1, l]))

        def begin(l, _):
            for c in copies(l):
                c.start()
            return 0

        lax.fori_loop(0, nsb, begin, 0)

        def one(l, _):
            for c in copies(l):
                c.wait()
            x = eb[l]
            tt = et[l]
            below = lax.broadcasted_iota(jnp.int32, (NB, NB), 0) > lax.broadcasted_iota(jnp.int32, (NB, NB), 1)
            both_in = jnp.where(below, x, tt)
            eb[l] = jnp.where(r == q, both_in, jnp.where(r == 0, tt, x))
            return 0

        lax.fori_loop(0, nsb, one, 0)

    def z_local(c):
        mine = pl.multiple_of(r * rows + c * CH, CH)
        return pltpu.make_async_copy(z_ref.at[pl.ds(mine, CH), :], zl.at[r, chunk_at(c), :], z_loc.at[c])

    def z_piece(w):
        c = nsb - 1 - w // RING
        r0 = c * CH + w % RING * NB
        theirs = pl.multiple_of((1 - r) * rows + r0, NB)
        return rcopy(z_ref.at[pl.ds(theirs, NB), :], zl.at[r, pl.ds(pl.multiple_of(r0, NB), NB), :],
                     z_snd.at[w], z_rcv.at[w], across)

    def put_x(g, x, at):
        xt[g, :, at] = x
        for i, piece in enumerate(split3(x)):
            xp[g, i * NB : (i + 1) * NB, at] = piece

    def admit(c):
        for j in range(RING):
            z_piece((nsb - 1 - c) * RING + j).wait()
        z_local(c).wait()

        def one(g, _):
            put_x(g, zl[g, chunk_at(c), :].T, chunk_at(c))
            return 0

        lax.fori_loop(0, 2, one, 0)

    def load(t, c, side, src, at):
        return pltpu.make_async_copy(src, vf.at[at, lanes(side)], ld.at[side, c])

    def start_loads(t):
        mine = owner_dist(t) == 0
        p = pair_of(t)

        def one(c, r0, n):
            at = pl.ds(r0, n)

            @pl.when(mine)
            def _():
                load(t, c, q, panel(t, r0, n, True), at).start()

            @pl.when(jnp.logical_not(mine))
            def _():
                load(t, c, q, panel(t, r0, n, False), at).start()

            src, dst = ends(t, c, False, r0, n)
            core_copy(src, dst, t, c).wait_recv()
            load(t, c, 1 - q, vb.at[1 - q, p, at, :], at).start()

        at = head_rows(t)

        @pl.when(jnp.logical_not(mine))
        def _():
            load(t, HEAD, q, vb.at[q, p, at, :], at).start()

        core_copy(*ends(t, HEAD, False), t, HEAD).wait_recv()
        load(t, HEAD, 1 - q, vb.at[1 - q, p, at, :], at).start()

        partial(t, lambda r0, n: one(sb_of(t), r0, n))
        full(t, one)

    def pieces(slot, at, x):
        for i, piece in enumerate(split3(x)):
            vn[slot, at, i * PW : (i + 1) * PW] = piece

    def prep(t):
        slot = t % 3
        mine = owner_dist(t) == 0
        at = head_rows(t)
        l = sb_of(t)

        load(t, HEAD, 1 - q, vb.at[0, 0, at, :], at).wait()

        @pl.when((r == 0) & (q == 0) & (t >= 3))
        def _():
            factor_across(t - 3).wait_send()

        @pl.when(mine)
        def _():
            vf[at, lanes(q)] = eb[l]

        @pl.when(jnp.logical_not(mine))
        def _():
            load(t, HEAD, q, vb.at[0, 0, at, :], at).wait()

        def above(j, _):
            pieces(slot, pl.ds(pl.multiple_of(l * CH + j * NB, NB), NB), jnp.zeros((NB, PW), F32))
            return 0

        lax.fori_loop(0, chip_of(t), above, 0)

        i0 = lax.broadcasted_iota(jnp.int32, (NB, NB), 0)
        i1 = lax.broadcasted_iota(jnp.int32, (NB, NB), 1)
        one = jnp.where(i0 == i1, 1.0, 0.0).astype(F32)
        x0 = vf[at, 0:NB]
        x1 = vf[at, NB:PW]
        first = r == 0
        v0 = jnp.where(first, jnp.where(i0 > i1, x0, one), x0)
        v1 = jnp.where(first, 0.0, jnp.where(i0 > i1, x1, one))
        tc[slot, 0] = jnp.where(i0 > i1, 0.0, x0)
        tc[slot, 1] = jnp.where(i0 > i1, 0.0, x1)
        pieces(slot, at, jnp.concatenate([v0, v1], axis=1))

        @pl.when(first & (q == 0))
        def _():
            factor_across(t).start()

        def rest(r0, n):
            a = pl.ds(r0, n)
            for side in range(2):
                load(t, l, side, vb.at[0, 0, a, :], a).wait()

            def sub(j, _):
                b = pl.ds(pl.multiple_of(r0 + j * NB, NB), NB)
                pieces(slot, b, vf[b, :])
                return 0

            lax.fori_loop(0, n // NB, sub, 0)

        partial(t, rest)

        def chunk(c, r0, n):
            a = pl.ds(r0, n)
            for side in range(2):
                load(t, c, side, vb.at[0, 0, a, :], a).wait()
            for j in range(0, n, NB):
                b = pl.ds(pl.multiple_of(r0 + j, NB), NB)
                pieces(slot, b, vf[b, :])

        full(t, chunk)

    def factor_across(t):
        return rcopy(tc.at[t % 3, 0], tb.at[t % 8], t_snd.at[0, t % 8], t_rcv.at[0, t % 8], across)

    def factor_over(t):
        return rcopy(tb.at[t % 8], tb.at[t % 8], t_snd.at[1, t % 8], t_rcv.at[1, t % 8], partner)

    def share_factor(t):
        @pl.when((r == 1) & (q == 0))
        def _():
            factor_across(t).wait_recv()

            @pl.when(t >= 2)
            def _():
                factor_over(t - 2).wait_send()

            factor_over(t).start()

    def late(t):
        return t > AHEAD + 1

    def part_copy(t):
        return rcopy(gs.at[t % 2], gp.at[t % 2], p_snd.at[t % 2], p_rcv.at[t % 2], partner)

    def plane_copy(t):
        return rcopy(gz.at[t % 2], gr.at[t % 2], g_snd.at[t % 2], g_rcv.at[t % 2], across)

    def total_copy(t):
        return rcopy(gf.at[t % 8], gf.at[t % 8], f_snd.at[t % 8], f_rcv.at[t % 8], partner)

    def gram_part(t):
        slot = t % 3
        s = t % 2

        @pl.when(t >= 2)
        def _():
            part_copy(t - 2).wait_send()

        gs[s] = jnp.zeros((NB, NB), F32)
        off = (sb_of(t) + t + q) % 2

        def one(j, _):
            at = chunk_at(sb_of(t) + off + 2 * j)
            a = [vn[slot, at, i * PW : i * PW + NB].T for i in range(3)]
            b = [vn[slot, at, i * PW + NB : (i + 1) * PW] for i in range(3)]
            x = mm(jnp.concatenate(a, axis=0), jnp.concatenate(b[0:2], axis=1))
            gs[s] += add_rows(add_rows(mm(a[0], b[2]), x[:, 0:NB], NB), x[0 : 2 * NB, NB:PW], NB)
            return 0

        lax.fori_loop(0, (height(t) - off + 1) // 2, one, 0)
        part_copy(t).start()

    def sends_plane(t):
        return late(t) | (t % 2 == q)

    def gram_plane(t):
        s = t % 2
        part_copy(t).wait_recv()

        @pl.when((t >= 2) & sends_plane(t - 2))
        def _():
            plane_copy(t - 2).wait_send()

        gz[s] = gs[s] + gp[s]

        @pl.when(sends_plane(t))
        def _():
            plane_copy(t).start()

    def gram_total(t):
        s = t % 2

        @pl.when(sends_plane(t))
        def _():
            plane_copy(t).wait_recv()

            @pl.when((t >= 8) & (t % 2 == q) & jnp.logical_not(late(t - 8)))
            def _():
                total_copy(t - 8).wait_send()

            gf[t % 8] = gz[s] + gr[s]

            @pl.when(jnp.logical_not(late(t)))
            def _():
                total_copy(t).start()

    def block_factor(t):
        slot = t % 3

        @pl.when(jnp.logical_not(sends_plane(t)))
        def _():
            total_copy(t).wait_recv()

        @pl.when((r == 1) & (q == 1))
        def _():
            factor_over(t).wait_recv()

        g = gf[t % 8]
        ta = jnp.where(r == 0, tc[slot, 0], tb[t % 8])
        tbb = tc[slot, 1]
        upper = -full_dot(ta, full_dot(g, tbb))
        for i, piece in enumerate(split3(ta)):
            tp[0:NB, i * PW : i * PW + NB] = piece
        for i, piece in enumerate(split3(upper)):
            tp[0:NB, i * PW + NB : (i + 1) * PW] = piece
        for i, piece in enumerate(split3(tbb)):
            tp[NB:PW, i * PW : i * PW + NB] = jnp.zeros((NB, NB), BF16)
            tp[NB:PW, i * PW + NB : (i + 1) * PW] = piece

    def w_copy(t, g):
        return rcopy(ws.at[t % 2, g], wr.at[t % 2, g], w_snd.at[t % 2, g], w_rcv.at[t % 2, g], across)

    def coefficients(t, g):
        with jax.named_scope("wwait"):
            w_copy(t, g).wait_recv()
        w = ws[t % 2, g] + wr[t % 2, g]
        y = stacked(mm_nt, jnp.concatenate(split3(w), axis=0), [tp[:, i * PW : (i + 1) * PW] for i in range(3)])
        for i, piece in enumerate(split3(y)):
            yp[i * NB : (i + 1) * NB] = piece

    def piece_of(t, i, at):
        return vn[t % 3, at, i * PW : (i + 1) * PW]

    def chunk_at(c):
        return pl.ds(pl.multiple_of(c * CH, CH), CH)

    def passes(m, i, g, n, finish):
        units = m * CH // UNIT
        base = rows - m * CH
        w = None
        for c in range(units + (0 if n is None else LAG)):
            at = pl.ds(base + c * UNIT, UNIT)
            an = pl.ds(max(0, base + (c - LAG) * UNIT), UNIT)
            u = None
            for j in range(3):
                k3 = (3 - j) * NB
                if n is not None and c >= LAG:
                    w = add_rows(w, mm(xp[g, 0:k3, an], piece_of(n, j, an)), NB)
                if c < units:
                    u = add_rows(u, mm_nt(yp[0:k3], piece_of(i, j, at)), NB)
            if c < units:
                finish(at, xt[g, :, at] - u)
        if n is not None:
            ws[n % 2, g] += w

    def product(n, g, at):
        w = None
        for j in range(3):
            w = add_rows(w, mm(xp[g, 0 : (3 - j) * NB, at], piece_of(n, j, at)), NB)
        ws[n % 2, g] += w

    def both(i, g):
        n = i + 1

        @pl.when(sb_of(n) < sb_of(i))
        def _():
            product(n, g, chunk_at(sb_of(n)))

        for m in range(1, nsb + 1):

            @pl.when(height(i) == m)
            def _(m=m):
                passes(m, i, g, n, lambda at, x: put_x(g, x, at))

    def out_copy(g, c):
        return pltpu.make_async_copy(zl.at[g, chunk_at(c), :], out_ref.at[chunk_at(c), lanes(g)], o_sem.at[g, c])

    def last(i, g):
        def finish(at, x):
            zl[g, at, :] = x.T

        passes(nsb, i, g, None, finish)

        def out(c, _):
            out_copy(g, c).start()
            return 0

        lax.fori_loop(0, nsb, out, 0)

    def step(i, _):
        n = i + 1
        early = i < AHEAD
        b = jnp.where(early, i + 2, n)
        brings = (i != AHEAD) & (b < npair)

        @pl.when(i < npair - 1)
        def _():
            with jax.named_scope("svc"):
                service(i)

        @pl.when(brings)
        def _():
            with jax.named_scope("loads"):
                start_loads(b)

        @pl.when(i >= 0)
        def _():
            with jax.named_scope("bfac"):
                block_factor(i)

        @pl.when((n >= 0) & (n < npair) & (n % RING == 0))
        def _():
            with jax.named_scope("admit"):
                admit(sb_of(n))

        def group(g, _):
            @pl.when((g == jnp.where(early, 1, 0)) & brings)
            def _():
                with jax.named_scope("prep"):
                    prep(b)
                with jax.named_scope("gram"):
                    gram_part(b)

            @pl.when(i >= 0)
            def _():
                with jax.named_scope("coef"):
                    coefficients(i, g)

            @pl.when((n >= 0) & (n < npair))
            def _():
                @pl.when(n >= 2)
                def _():
                    w_copy(n - 2, g).wait_send()

                ws[n % 2, g] = jnp.zeros((NB, PW), F32)

            @pl.when(i == -1)
            def _():
                product(n, g, chunk_at(nsb - 1))

            @pl.when((i >= 0) & (n < npair))
            def _():
                with jax.named_scope("both"):
                    both(i, g)

            @pl.when((g == jnp.where(early, 1, 0)) & brings)
            def _():
                with jax.named_scope("gplane"):
                    gram_plane(b)

            @pl.when((n >= 0) & (n < npair))
            def _():
                w_copy(n, g).start()

                @pl.when(g == jnp.where(i <= AHEAD, 0, 1))
                def _():
                    with jax.named_scope("fshare"):
                        share_factor(n)
                    with jax.named_scope("gtot"):
                        gram_total(n)

            @pl.when(n == npair)
            def _():
                with jax.named_scope("last"):
                    last(i, g)

            return 0

        lax.fori_loop(0, 2, group, 0)

        @pl.when((n >= RING - 1) & (n + RING + 1 < npair))
        def _():
            z_piece(n + RING + 1).start()

        @pl.when((n >= 0) & (n % RING == 2) & (n + RING < npair))
        def _():
            z_local(sb_of(n) - 1).start()

        return 0

    barrier = pltpu.get_barrier_semaphore()
    for dev in (at_ring(rho + 1), at_ring(rho + RING - 1), partner, across):
        pl.semaphore_signal(barrier, inc=1, device_id=dev, device_id_type=MESH_ID)
    pl.semaphore_wait(barrier, 4)

    for j in range(min(2 * RING, npair)):
        z_piece(j).start()
    z_local(nsb - 1).start()
    with jax.named_scope("heads"):
        make_heads()
    lax.fori_loop(-2, npair, step, 0)

    for t in (npair - 2, npair - 1):
        for g in range(2):
            w_copy(t, g).wait_send()
    for t in (npair - 2, npair - 1):
        part_copy(t).wait_send()

        @pl.when(sends_plane(t))
        def _(t=t):
            plane_copy(t).wait_send()

    newest = min(npair - 1, AHEAD + 1)
    for t in range(max(0, npair - 8), newest + 1):

        @pl.when(t % 2 == q)
        def _(t=t):
            total_copy(t).wait_send()

    for t in range(npair - 3, npair):

        @pl.when((r == 0) & (q == 0))
        def _(t=t):
            factor_across(t).wait_send()

    for t in range(npair - 2, npair):

        @pl.when((r == 1) & (q == 0))
        def _(t=t):
            factor_over(t).wait_send()

    def drain(t, _):
        all_sent(t)
        return 0

    lax.fori_loop(max(0, npair - 8), npair, drain, 0)

    def out_done(c, _):
        for g in range(2):
            out_copy(g, c).wait()
        return 0

    lax.fori_loop(0, nsb, out_done, 0)


def solution(mesh):
    def local(v, t, z):
        rows, cols = v.shape
        nsb = cols // NB
        npair = nsb * RING
        hbm = pl.BlockSpec(memory_space=pltpu.MemorySpace.HBM)
        out, _ = pl.pallas_call(
            functools.partial(body, nsb),
            out_shape=(
                jax.ShapeDtypeStruct((rows, PW), F32),
                jax.ShapeDtypeStruct((2, npair, rows, NB), F32),
            ),
            in_specs=[hbm] * 3,
            out_specs=(hbm, hbm),
            scratch_shapes=[
                pltpu.VMEM((2, rows, NB), F32),
                pltpu.VMEM((2, NB, rows), F32),
                pltpu.VMEM((2, 3 * NB, rows), BF16),
                pltpu.VMEM((rows, PW), F32),
                pltpu.VMEM((3, rows, 3 * PW), BF16),
                pltpu.VMEM((8, NB, NB), F32),
                pltpu.VMEM((3, 2, NB, NB), F32),
                pltpu.VMEM((PW, 3 * PW), BF16),
                pltpu.VMEM((2, 2, NB, PW), F32),
                pltpu.VMEM((2, 2, NB, PW), F32),
                pltpu.VMEM((2, NB, NB), F32),
                pltpu.VMEM((2, NB, NB), F32),
                pltpu.VMEM((2, NB, NB), F32),
                pltpu.VMEM((2, NB, NB), F32),
                pltpu.VMEM((8, NB, NB), F32),
                pltpu.VMEM((3 * NB, PW), BF16),
                pltpu.VMEM((nsb, NB, NB), F32),
                pltpu.VMEM((nsb, NB, NB), F32),
            ],
            compiler_params=pltpu.CompilerParams(
                collective_id=0, has_side_effects=True, vmem_limit_bytes=60 * 2**20),
            name="backtransform",
        )(v, t, z)
        return out

    return jax.shard_map(local, mesh=mesh,
                         in_specs=(P("row", "col"), P("col", None, None), P(None, ("col", "row"))),
                         out_specs=P("row", "col"), check_vma=False)
```

```python
import functools

import jax
import jax.numpy as jnp
from jax import lax
from jax.experimental import pallas as pl
from jax.experimental.pallas import tpu as pltpu
from jax.sharding import PartitionSpec as P

F32 = jnp.float32
BF16 = jnp.bfloat16
MESH_ID = pl.DeviceIdType.MESH

NB = 128
PW = 2 * NB
CH = 4 * NB
UNIT = PW
LAG = 2
RING = 4
AHEAD = 20


def split3(x):
    hi = x.astype(BF16)
    rest = x - hi.astype(F32)
    mid = rest.astype(BF16)
    low = (rest - mid.astype(F32)).astype(BF16)
    return hi, mid, low


def mm(a, b):
    return lax.dot_general(a, b, (((1,), (0,)), ((), ())), preferred_element_type=F32)


def mm_nt(a, b):
    return lax.dot_general(a, b, (((1,), (1,)), ((), ())), preferred_element_type=F32)


def add_rows(total, x, n):
    for i in range(0, x.shape[0], n):
        part = x[i : i + n]
        total = part if total is None else total + part
    return total


def stacked(dot, a3, b):
    m = a3.shape[0] // 3
    s = None
    for i in range(3):
        s = add_rows(s, dot(a3[0 : (3 - i) * m], b[i]), m)
    return s


def full_dot(a, b):
    ah, am, al = split3(a)
    bh, bm, bl = split3(b)
    n = a.shape[0]
    x = mm(jnp.concatenate([ah, am], axis=1), jnp.concatenate([jnp.concatenate([bh, bm], axis=1)] * 2, axis=0))
    y = mm(jnp.concatenate([al, ah], axis=1), jnp.concatenate([bh, bl], axis=0))
    return x[:, 0:n] + x[:, n:] + y


def body(nsb, v_ref, t_ref, z_ref, out_ref, vb, *scratch):
    rows = nsb * CH
    dma = pltpu.SemaphoreType.DMA
    npair = nsb * RING
    nc = nsb + 1
    pl.run_scoped(
        functools.partial(run, nsb, rows, npair, v_ref, t_ref, z_ref, out_ref, vb, scratch),
        dma((nsb,)),
        dma((npair,)),
        dma((npair,)),
        dma((npair, nc)),
        dma((npair, nc)),
        dma((2, 2)),
        dma((2, 2)),
        dma((2,)),
        dma((2,)),
        dma((8,)),
        dma((8,)),
        dma((2, nc)),
        dma((2, nsb)),
        dma((2, 8, nc)),
        dma((8, nc)),
        dma((2, nsb)),
        dma((2,)),
        dma((2,)),
        dma((2, 8)),
        dma((2, 8)),
    )


def run(nsb, rows, npair, v_ref, t_ref, z_ref, out_ref, vb, scratch, *sems):
    (zl, xt, xp, vf, vn, tb, tc, tp, ws, wr, gs, gp, gz, gr, gf, yp, eb, et) = scratch
    (z_loc, z_snd, z_rcv, i_rcv, d_rcv, w_snd, w_rcv, g_snd, g_rcv, f_snd, f_rcv, ld, o_sem, i_snd, d_snd, h_sem, p_snd, p_rcv, t_snd, t_rcv) = sems
    HEAD = nsb
    r = lax.axis_index("row")
    col = lax.axis_index("col")
    q = col % 2
    k = col // 2
    ky, kx = k // 2, k % 2
    rho = 2 * ky + (kx + ky) % 2

    def at_ring(i):
        i = i % RING
        y = i // 2
        x = (i % 2 + y) % 2
        return (r, (y * 2 + x) * 2 + q)

    partner = (r, k * 2 + 1 - q)
    across = (1 - r, col)

    def pair_of(t):
        return npair - 1 - t

    def sb_of(t):
        return pair_of(t) // RING

    def chip_of(t):
        return pair_of(t) % RING

    def owner_dist(t):
        kk = chip_of(t)
        y = kk // 2
        ro = 2 * y + (kk % 2 + y) % 2
        return (rho - ro + RING) % RING

    def height(t):
        return nsb - sb_of(t)

    def half_of(t, c):
        return (c - sb_of(t) + (height(t) - 1) // 2) % 2

    def head_half(t):
        return height(t) % 2

    def partial(t, fn):
        kk = chip_of(t)
        for j in range(RING - 1):

            @pl.when(kk == j)
            def _(j=j):
                fn(pl.multiple_of(sb_of(t) * CH + (j + 1) * NB, NB), CH - (j + 1) * NB)

    def full(t, fn):
        def one(c, _):
            fn(c, pl.multiple_of(c * CH, CH), CH)
            return 0

        lax.fori_loop(sb_of(t) + 1, nsb, one, 0)

    def head_rows(t):
        return pl.ds(pl.multiple_of(pair_of(t) * NB, NB), NB)

    def lanes(l):
        return pl.ds(pl.multiple_of(l * NB, NB), NB)

    def rcopy(src, dst, ssem, rsem, dev):
        return pltpu.make_async_remote_copy(src, dst, ssem, rsem, device_id=dev, device_id_type=MESH_ID)

    def panel(t, r0, n, own):
        if own:
            return v_ref.at[pl.ds(r0, n), lanes(sb_of(t))]
        return vb.at[q, pair_of(t), pl.ds(r0, n), :]

    def side_copy(src, dst, t, c, d):
        return rcopy(src, dst, i_snd.at[d, t % 8, c], i_rcv.at[t, c], at_ring(rho + 1 - 2 * d + RING))

    def core_copy(src, dst, t, c):
        return rcopy(src, dst, d_snd.at[t % 8, c], d_rcv.at[t, c], partner)

    def ends(t, c, own, r0=None, n=None):
        if c is HEAD:
            dst = vb.at[q, pair_of(t), head_rows(t), :]
            return (eb.at[sb_of(t)] if own else dst), dst
        return panel(t, r0, n, own), panel(t, r0, n, False)

    def wait_sent(t, c, half, r0=None, n=None):
        src, dst = ends(t, c, False, r0, n)
        d = owner_dist(t)

        @pl.when((d == 0) | ((d == 1) & (half == 0)))
        def _():
            side_copy(src, dst, t, c, 0).wait_send()

        @pl.when((d == 0) | ((d == 3) & (half == 1)))
        def _():
            side_copy(src, dst, t, c, 1).wait_send()

        core_copy(src, dst, t, c).wait_send()

    def all_sent(t):
        wait_sent(t, HEAD, head_half(t))

        partial(t, lambda r0, n: wait_sent(t, sb_of(t), half_of(t, sb_of(t)), r0, n))
        full(t, lambda c, r0, n: wait_sent(t, c, half_of(t, c), r0, n))

    def free_slot(t):
        @pl.when(t >= 8)
        def _():
            all_sent(t - 8)

    def send_own(u):
        first = RING - 1 - k
        part = (u - first + 2 * RING) % RING
        t = u - part
        quarter = RING

        @pl.when((t >= 0) & (t < npair))
        def _():
            def out(c, r0=None, n=None):
                src, dst = ends(t, c, True, r0, n)
                for d in range(2):
                    side_copy(src, dst, t, c, d).start()
                core_copy(src, dst, t, c).start()

            @pl.when(part == 0)
            def _():
                free_slot(t)
                out(HEAD)

                partial(t, lambda r0, n: out(sb_of(t), r0, n))

            m = height(t)
            lo = (part * m + quarter - 1) // quarter
            hi = ((part + 1) * m + quarter - 1) // quarter

            def one(i, _):
                c = sb_of(t) + i
                out(c, pl.multiple_of(c * CH, CH), CH)
                return 0

            lax.fori_loop(jnp.maximum(lo, 1), hi, one, 0)

    def pass_on(t, near):
        d = owner_dist(t)
        free_slot(t)

        def got(c, half, r0=None, n=None):
            src, dst = ends(t, c, False, r0, n)
            side_copy(src, dst, t, c, 0).wait_recv()
            core_copy(src, dst, t, c).start()
            if near:

                @pl.when((d == 1) & (half == 0))
                def _():
                    side_copy(src, dst, t, c, 0).start()

                @pl.when((d == 3) & (half == 1))
                def _():
                    side_copy(src, dst, t, c, 1).start()

        got(HEAD, head_half(t))

        partial(t, lambda r0, n: got(sb_of(t), half_of(t, sb_of(t)), r0, n))
        full(t, lambda c, r0, n: got(c, half_of(t, c), r0, n))

    def brought(i):
        return jnp.minimum(npair - 1, jnp.minimum(i + 2, jnp.maximum(AHEAD + 1, i + 1)))

    def falling(i, high, low, i0, i1):
        return high - jnp.clip(((high - low) * (i - i0) + i1 - i0 - 1) // (i1 - i0), 0, high - low)

    def near_lead(i):
        return jnp.minimum(npair - 1, brought(i) + jnp.minimum(falling(i, 4, 2, 20, 31), i + 3))

    def far_lead(i):
        return brought(i)

    def own_lead(i):
        return jnp.minimum(npair + RING - 2, brought(i) + jnp.minimum(falling(i, 12, 7, 11, 26), 3 + 5 * (i + 2)))

    def span(lead, i):
        return jnp.where(i < -1, 0, lead(i - 1) + 1), lead(i) + 1

    def service(i):
        def one(j, _):
            kind = jnp.where(i < -1, j, 2 - j)

            @pl.when(kind == 0)
            def _():
                lo, hi = span(own_lead, i)
                lax.fori_loop(lo, hi, lambda u, _: (send_own(u), 0)[1], 0)

            @pl.when(kind == 1)
            def _():
                def near(t, _):
                    @pl.when(owner_dist(t) % 2 == 1)
                    def _():
                        pass_on(t, True)

                    return 0

                lo, hi = span(near_lead, i)
                lax.fori_loop(lo, hi, near, 0)

            @pl.when(kind == 2)
            def _():
                def far(t, _):
                    @pl.when(owner_dist(t) == 2)
                    def _():
                        pass_on(t, False)

                    return 0

                lo, hi = span(far_lead, i)
                lax.fori_loop(lo, hi, far, 0)

            return 0

        lax.fori_loop(0, 3, one, 0)

    def make_heads():
        def copies(l):
            rr = pl.ds(pl.multiple_of((l * RING + k) * NB, NB), NB)
            return (pltpu.make_async_copy(v_ref.at[rr, lanes(l)], eb.at[l], h_sem.at[0, l]),
                    pltpu.make_async_copy(t_ref.at[l], et.at[l], h_sem.at[1, l]))

        def begin(l, _):
            for c in copies(l):
                c.start()
            return 0

        lax.fori_loop(0, nsb, begin, 0)

        def one(l, _):
            for c in copies(l):
                c.wait()
            x = eb[l]
            tt = et[l]
            below = lax.broadcasted_iota(jnp.int32, (NB, NB), 0) > lax.broadcasted_iota(jnp.int32, (NB, NB), 1)
            both_in = jnp.where(below, x, tt)
            eb[l] = jnp.where(r == q, both_in, jnp.where(r == 0, tt, x))
            return 0

        lax.fori_loop(0, nsb, one, 0)

    def z_local(c):
        mine = pl.multiple_of(r * rows + c * CH, CH)
        return pltpu.make_async_copy(z_ref.at[pl.ds(mine, CH), :], zl.at[r, chunk_at(c), :], z_loc.at[c])

    def z_piece(w):
        c = nsb - 1 - w // RING
        r0 = c * CH + w % RING * NB
        theirs = pl.multiple_of((1 - r) * rows + r0, NB)
        return rcopy(z_ref.at[pl.ds(theirs, NB), :], zl.at[r, pl.ds(pl.multiple_of(r0, NB), NB), :],
                     z_snd.at[w], z_rcv.at[w], across)

    def put_x(g, x, at):
        xt[g, :, at] = x
        for i, piece in enumerate(split3(x)):
            xp[g, i * NB : (i + 1) * NB, at] = piece

    def admit(c):
        for j in range(RING):
            z_piece((nsb - 1 - c) * RING + j).wait()
        z_local(c).wait()

        def one(g, _):
            put_x(g, zl[g, chunk_at(c), :].T, chunk_at(c))
            return 0

        lax.fori_loop(0, 2, one, 0)

    def load(t, c, side, src, at):
        return pltpu.make_async_copy(src, vf.at[at, lanes(side)], ld.at[side, c])

    def start_loads(t):
        mine = owner_dist(t) == 0
        p = pair_of(t)

        def one(c, r0, n):
            at = pl.ds(r0, n)

            @pl.when(mine)
            def _():
                load(t, c, q, panel(t, r0, n, True), at).start()

            @pl.when(jnp.logical_not(mine))
            def _():
                load(t, c, q, panel(t, r0, n, False), at).start()

            src, dst = ends(t, c, False, r0, n)
            core_copy(src, dst, t, c).wait_recv()
            load(t, c, 1 - q, vb.at[1 - q, p, at, :], at).start()

        at = head_rows(t)

        @pl.when(jnp.logical_not(mine))
        def _():
            load(t, HEAD, q, vb.at[q, p, at, :], at).start()

        core_copy(*ends(t, HEAD, False), t, HEAD).wait_recv()
        load(t, HEAD, 1 - q, vb.at[1 - q, p, at, :], at).start()

        partial(t, lambda r0, n: one(sb_of(t), r0, n))
        full(t, one)

    def pieces(slot, at, x):
        for i, piece in enumerate(split3(x)):
            vn[slot, at, i * PW : (i + 1) * PW] = piece

    def prep(t):
        slot = t % 3
        mine = owner_dist(t) == 0
        at = head_rows(t)
        l = sb_of(t)

        load(t, HEAD, 1 - q, vb.at[0, 0, at, :], at).wait()

        @pl.when((r == 0) & (q == 0) & (t >= 3))
        def _():
            factor_across(t - 3).wait_send()

        @pl.when(mine)
        def _():
            vf[at, lanes(q)] = eb[l]

        @pl.when(jnp.logical_not(mine))
        def _():
            load(t, HEAD, q, vb.at[0, 0, at, :], at).wait()

        def above(j, _):
            pieces(slot, pl.ds(pl.multiple_of(l * CH + j * NB, NB), NB), jnp.zeros((NB, PW), F32))
            return 0

        lax.fori_loop(0, chip_of(t), above, 0)

        i0 = lax.broadcasted_iota(jnp.int32, (NB, NB), 0)
        i1 = lax.broadcasted_iota(jnp.int32, (NB, NB), 1)
        one = jnp.where(i0 == i1, 1.0, 0.0).astype(F32)
        x0 = vf[at, 0:NB]
        x1 = vf[at, NB:PW]
        first = r == 0
        v0 = jnp.where(first, jnp.where(i0 > i1, x0, one), x0)
        v1 = jnp.where(first, 0.0, jnp.where(i0 > i1, x1, one))
        tc[slot, 0] = jnp.where(i0 > i1, 0.0, x0)
        tc[slot, 1] = jnp.where(i0 > i1, 0.0, x1)
        pieces(slot, at, jnp.concatenate([v0, v1], axis=1))

        @pl.when(first & (q == 0))
        def _():
            factor_across(t).start()

        def rest(r0, n):
            a = pl.ds(r0, n)
            for side in range(2):
                load(t, l, side, vb.at[0, 0, a, :], a).wait()

            def sub(j, _):
                b = pl.ds(pl.multiple_of(r0 + j * NB, NB), NB)
                pieces(slot, b, vf[b, :])
                return 0

            lax.fori_loop(0, n // NB, sub, 0)

        partial(t, rest)

        def chunk(c, r0, n):
            a = pl.ds(r0, n)
            for side in range(2):
                load(t, c, side, vb.at[0, 0, a, :], a).wait()
            for j in range(0, n, NB):
                b = pl.ds(pl.multiple_of(r0 + j, NB), NB)
                pieces(slot, b, vf[b, :])

        full(t, chunk)

    def factor_across(t):
        return rcopy(tc.at[t % 3, 0], tb.at[t % 8], t_snd.at[0, t % 8], t_rcv.at[0, t % 8], across)

    def factor_over(t):
        return rcopy(tb.at[t % 8], tb.at[t % 8], t_snd.at[1, t % 8], t_rcv.at[1, t % 8], partner)

    def share_factor(t):
        @pl.when((r == 1) & (q == 0))
        def _():
            factor_across(t).wait_recv()

            @pl.when(t >= 2)
            def _():
                factor_over(t - 2).wait_send()

            factor_over(t).start()

    def late(t):
        return t > AHEAD + 1

    def part_copy(t):
        return rcopy(gs.at[t % 2], gp.at[t % 2], p_snd.at[t % 2], p_rcv.at[t % 2], partner)

    def plane_copy(t):
        return rcopy(gz.at[t % 2], gr.at[t % 2], g_snd.at[t % 2], g_rcv.at[t % 2], across)

    def total_copy(t):
        return rcopy(gf.at[t % 8], gf.at[t % 8], f_snd.at[t % 8], f_rcv.at[t % 8], partner)

    def gram_part(t):
        slot = t % 3
        s = t % 2

        @pl.when(t >= 2)
        def _():
            part_copy(t - 2).wait_send()

        gs[s] = jnp.zeros((NB, NB), F32)
        first = (height(t) + t % 2) // 2
        lo = sb_of(t) + q * first
        cnt = jnp.where(q == 0, first, height(t) - first)

        def block(c, n):
            at = pl.ds(pl.multiple_of(c * CH, CH), n * CH)
            a = [vn[slot, at, i * PW : i * PW + NB].T for i in range(3)]
            b = [vn[slot, at, i * PW + NB : (i + 1) * PW] for i in range(3)]
            x = mm(jnp.concatenate(a, axis=0), jnp.concatenate(b[0:2], axis=1))
            gs[s] += add_rows(add_rows(mm(a[0], b[2]), x[:, 0:NB], NB), x[0 : 2 * NB, NB:PW], NB)

        if nsb >= 8:

            @pl.when(cnt >= 4)
            def _():
                block(lo, 4)

        if nsb >= 3:

            @pl.when(cnt % 4 >= 2)
            def _():
                block(lo + cnt // 4 * 4, 2)

        @pl.when(cnt % 2 == 1)
        def _():
            block(lo + cnt - 1, 1)

        part_copy(t).start()

    def sends_plane(t):
        return late(t) | (t % 2 == q)

    def gram_plane(t):
        s = t % 2
        part_copy(t).wait_recv()

        @pl.when((t >= 2) & sends_plane(t - 2))
        def _():
            plane_copy(t - 2).wait_send()

        gz[s] = gs[s] + gp[s]

        @pl.when(sends_plane(t))
        def _():
            plane_copy(t).start()

    def gram_total(t):
        s = t % 2

        @pl.when(sends_plane(t))
        def _():
            plane_copy(t).wait_recv()

            @pl.when((t >= 8) & (t % 2 == q) & jnp.logical_not(late(t - 8)))
            def _():
                total_copy(t - 8).wait_send()

            gf[t % 8] = gz[s] + gr[s]

            @pl.when(jnp.logical_not(late(t)))
            def _():
                total_copy(t).start()

    def block_factor(t):
        slot = t % 3

        @pl.when(jnp.logical_not(sends_plane(t)))
        def _():
            total_copy(t).wait_recv()

        @pl.when((r == 1) & (q == 1))
        def _():
            factor_over(t).wait_recv()

        g = gf[t % 8]
        ta = jnp.where(r == 0, tc[slot, 0], tb[t % 8])
        tbb = tc[slot, 1]
        upper = -full_dot(ta, full_dot(g, tbb))
        for i, piece in enumerate(split3(ta)):
            tp[0:NB, i * PW : i * PW + NB] = piece
        for i, piece in enumerate(split3(upper)):
            tp[0:NB, i * PW + NB : (i + 1) * PW] = piece
        for i, piece in enumerate(split3(tbb)):
            tp[NB:PW, i * PW : i * PW + NB] = jnp.zeros((NB, NB), BF16)
            tp[NB:PW, i * PW + NB : (i + 1) * PW] = piece

    def w_copy(t, g):
        return rcopy(ws.at[t % 2, g], wr.at[t % 2, g], w_snd.at[t % 2, g], w_rcv.at[t % 2, g], across)

    def coefficients(t, g):
        with jax.named_scope("wwait"):
            w_copy(t, g).wait_recv()
        w = ws[t % 2, g] + wr[t % 2, g]
        y = stacked(mm_nt, jnp.concatenate(split3(w), axis=0), [tp[:, i * PW : (i + 1) * PW] for i in range(3)])
        for i, piece in enumerate(split3(y)):
            yp[i * NB : (i + 1) * NB] = piece

    def piece_of(t, i, at):
        return vn[t % 3, at, i * PW : (i + 1) * PW]

    def chunk_at(c):
        return pl.ds(pl.multiple_of(c * CH, CH), CH)

    def passes(m, i, g, n, finish):
        units = m * CH // UNIT
        base = rows - m * CH
        w = None
        for c in range(units + (0 if n is None else LAG)):
            at = pl.ds(base + c * UNIT, UNIT)
            an = pl.ds(max(0, base + (c - LAG) * UNIT), UNIT)
            u = None
            for j in range(3):
                k3 = (3 - j) * NB
                if n is not None and c >= LAG:
                    w = add_rows(w, mm(xp[g, 0:k3, an], piece_of(n, j, an)), NB)
                if c < units:
                    u = add_rows(u, mm_nt(yp[0:k3], piece_of(i, j, at)), NB)
            if c < units:
                finish(at, xt[g, :, at] - u)
        if n is not None:
            ws[n % 2, g] += w

    def product(n, g, at):
        w = None
        for j in range(3):
            w = add_rows(w, mm(xp[g, 0 : (3 - j) * NB, at], piece_of(n, j, at)), NB)
        ws[n % 2, g] += w

    def both(i, g):
        n = i + 1

        @pl.when(sb_of(n) < sb_of(i))
        def _():
            product(n, g, chunk_at(sb_of(n)))

        for m in range(1, nsb + 1):

            @pl.when(height(i) == m)
            def _(m=m):
                passes(m, i, g, n, lambda at, x: put_x(g, x, at))

    def out_copy(g, c):
        return pltpu.make_async_copy(zl.at[g, chunk_at(c), :], out_ref.at[chunk_at(c), lanes(g)], o_sem.at[g, c])

    def last(i, g):
        def finish(at, x):
            zl[g, at, :] = x.T

        passes(nsb, i, g, None, finish)

        def out(c, _):
            out_copy(g, c).start()
            return 0

        lax.fori_loop(0, nsb, out, 0)

    def step(i, _):
        n = i + 1
        early = i < AHEAD
        b = jnp.where(early, i + 2, n)
        brings = (i != AHEAD) & (b < npair)

        @pl.when(i < npair - 1)
        def _():
            with jax.named_scope("svc"):
                service(i)

        @pl.when(brings)
        def _():
            with jax.named_scope("loads"):
                start_loads(b)

        @pl.when(i >= 0)
        def _():
            with jax.named_scope("bfac"):
                block_factor(i)

        @pl.when((n >= 0) & (n < npair) & (n % RING == 0))
        def _():
            with jax.named_scope("admit"):
                admit(sb_of(n))

        def group(g, _):
            @pl.when((g == jnp.where(early, 1, 0)) & brings)
            def _():
                with jax.named_scope("prep"):
                    prep(b)
                with jax.named_scope("gram"):
                    gram_part(b)

            @pl.when(i >= 0)
            def _():
                with jax.named_scope("coef"):
                    coefficients(i, g)

            @pl.when((n >= 0) & (n < npair))
            def _():
                @pl.when(n >= 2)
                def _():
                    w_copy(n - 2, g).wait_send()

                ws[n % 2, g] = jnp.zeros((NB, PW), F32)

            @pl.when(i == -1)
            def _():
                product(n, g, chunk_at(nsb - 1))

            @pl.when((i >= 0) & (n < npair))
            def _():
                with jax.named_scope("both"):
                    both(i, g)

            @pl.when((g == jnp.where(early, 1, 0)) & brings)
            def _():
                with jax.named_scope("gplane"):
                    gram_plane(b)

            @pl.when((n >= 0) & (n < npair))
            def _():
                w_copy(n, g).start()

                @pl.when(g == jnp.where(i <= AHEAD, 0, 1))
                def _():
                    with jax.named_scope("fshare"):
                        share_factor(n)
                    with jax.named_scope("gtot"):
                        gram_total(n)

            @pl.when(n == npair)
            def _():
                with jax.named_scope("last"):
                    last(i, g)

            return 0

        lax.fori_loop(0, 2, group, 0)

        @pl.when((n >= RING + 1) & (n + RING + 1 < npair))
        def _():
            z_piece(n + RING + 1).start()

        @pl.when((n >= 0) & (n % RING == 2) & (n + RING < npair))
        def _():
            z_local(sb_of(n) - 1).start()

        return 0

    barrier = pltpu.get_barrier_semaphore()
    for dev in (at_ring(rho + 1), at_ring(rho + RING - 1), partner, across):
        pl.semaphore_signal(barrier, inc=1, device_id=dev, device_id_type=MESH_ID)
    pl.semaphore_wait(barrier, 4)

    for j in range(min(2 * RING + 2, npair)):
        z_piece(j).start()
    z_local(nsb - 1).start()
    with jax.named_scope("heads"):
        make_heads()
    lax.fori_loop(-2, npair, step, 0)

    for t in (npair - 2, npair - 1):
        for g in range(2):
            w_copy(t, g).wait_send()
    for t in (npair - 2, npair - 1):
        part_copy(t).wait_send()

        @pl.when(sends_plane(t))
        def _(t=t):
            plane_copy(t).wait_send()

    newest = min(npair - 1, AHEAD + 1)
    for t in range(max(0, npair - 8), newest + 1):

        @pl.when(t % 2 == q)
        def _(t=t):
            total_copy(t).wait_send()

    for t in range(npair - 3, npair):

        @pl.when((r == 0) & (q == 0))
        def _(t=t):
            factor_across(t).wait_send()

    for t in range(npair - 2, npair):

        @pl.when((r == 1) & (q == 0))
        def _(t=t):
            factor_over(t).wait_send()

    def drain(t, _):
        all_sent(t)
        return 0

    lax.fori_loop(max(0, npair - 8), npair, drain, 0)

    def out_done(c, _):
        for g in range(2):
            out_copy(g, c).wait()
        return 0

    lax.fori_loop(0, nsb, out_done, 0)


def solution(mesh):
    def local(v, t, z):
        rows, cols = v.shape
        nsb = cols // NB
        npair = nsb * RING
        hbm = pl.BlockSpec(memory_space=pltpu.MemorySpace.HBM)
        out, _ = pl.pallas_call(
            functools.partial(body, nsb),
            out_shape=(
                jax.ShapeDtypeStruct((rows, PW), F32),
                jax.ShapeDtypeStruct((2, npair, rows, NB), F32),
            ),
            in_specs=[hbm] * 3,
            out_specs=(hbm, hbm),
            scratch_shapes=[
                pltpu.VMEM((2, rows, NB), F32),
                pltpu.VMEM((2, NB, rows), F32),
                pltpu.VMEM((2, 3 * NB, rows), BF16),
                pltpu.VMEM((rows, PW), F32),
                pltpu.VMEM((3, rows, 3 * PW), BF16),
                pltpu.VMEM((8, NB, NB), F32),
                pltpu.VMEM((3, 2, NB, NB), F32),
                pltpu.VMEM((PW, 3 * PW), BF16),
                pltpu.VMEM((2, 2, NB, PW), F32),
                pltpu.VMEM((2, 2, NB, PW), F32),
                pltpu.VMEM((2, NB, NB), F32),
                pltpu.VMEM((2, NB, NB), F32),
                pltpu.VMEM((2, NB, NB), F32),
                pltpu.VMEM((2, NB, NB), F32),
                pltpu.VMEM((8, NB, NB), F32),
                pltpu.VMEM((3 * NB, PW), BF16),
                pltpu.VMEM((nsb, NB, NB), F32),
                pltpu.VMEM((nsb, NB, NB), F32),
            ],
            compiler_params=pltpu.CompilerParams(
                collective_id=0, has_side_effects=True, vmem_limit_bytes=60 * 2**20),
            name="backtransform",
        )(v, t, z)
        return out

    return jax.shard_map(local, mesh=mesh,
                         in_specs=(P("row", "col"), P("col", None, None), P(None, ("col", "row"))),
                         out_specs=P("row", "col"), check_vma=False)
```

```python
import functools

import jax
import jax.numpy as jnp
from jax import lax
from jax.experimental import pallas as pl
from jax.experimental.pallas import tpu as pltpu
from jax.sharding import PartitionSpec as P

F32 = jnp.float32
BF16 = jnp.bfloat16
MESH_ID = pl.DeviceIdType.MESH

NB = 128
PW = 2 * NB
CH = 4 * NB
UNIT = PW
LAG = 2
RING = 4
SLOTS = 16
AHEAD = 20


def split3(x):
    hi = x.astype(BF16)
    rest = x - hi.astype(F32)
    mid = rest.astype(BF16)
    low = (rest - mid.astype(F32)).astype(BF16)
    return hi, mid, low


def mm(a, b):
    return lax.dot_general(a, b, (((1,), (0,)), ((), ())), preferred_element_type=F32)


def mm_nt(a, b):
    return lax.dot_general(a, b, (((1,), (1,)), ((), ())), preferred_element_type=F32)


def add_rows(total, x, n):
    for i in range(0, x.shape[0], n):
        part = x[i : i + n]
        total = part if total is None else total + part
    return total


def stacked(dot, a3, b):
    m = a3.shape[0] // 3
    s = None
    for i in range(3):
        s = add_rows(s, dot(a3[0 : (3 - i) * m], b[i]), m)
    return s


def full_dot(a, b):
    ah, am, al = split3(a)
    bh, bm, bl = split3(b)
    n = a.shape[0]
    x = mm(jnp.concatenate([ah, am], axis=1), jnp.concatenate([jnp.concatenate([bh, bm], axis=1)] * 2, axis=0))
    y = mm(jnp.concatenate([al, ah], axis=1), jnp.concatenate([bh, bl], axis=0))
    return x[:, 0:n] + x[:, n:] + y


def body(nsb, v_ref, t_ref, z_ref, out_ref, vb, *scratch):
    rows = nsb * CH
    dma = pltpu.SemaphoreType.DMA
    npair = nsb * RING
    nc = nsb + 1
    pl.run_scoped(
        functools.partial(run, nsb, rows, npair, v_ref, t_ref, z_ref, out_ref, vb, scratch),
        dma((nsb,)),
        dma((npair,)),
        dma((npair,)),
        dma((npair, nc)),
        dma((npair, nc)),
        dma((2, 2)),
        dma((2, 2)),
        dma((2,)),
        dma((2,)),
        dma((8,)),
        dma((8,)),
        dma((2, nc)),
        dma((2, nsb)),
        dma((2, SLOTS, nc)),
        dma((SLOTS, nc)),
        dma((2, nsb)),
        dma((2,)),
        dma((2,)),
        dma((2, 8)),
        dma((2, 8)),
    )


def run(nsb, rows, npair, v_ref, t_ref, z_ref, out_ref, vb, scratch, *sems):
    (zl, xt, xp, vf, vn, tb, tc, tp, ws, wr, gs, gp, gz, gr, gf, yp, eb, et) = scratch
    (z_loc, z_snd, z_rcv, i_rcv, d_rcv, w_snd, w_rcv, g_snd, g_rcv, f_snd, f_rcv, ld, o_sem, i_snd, d_snd, h_sem, p_snd, p_rcv, t_snd, t_rcv) = sems
    HEAD = nsb
    r = lax.axis_index("row")
    col = lax.axis_index("col")
    q = col % 2
    k = col // 2
    ky, kx = k // 2, k % 2
    rho = 2 * ky + (kx + ky) % 2

    def at_ring(i):
        i = i % RING
        y = i // 2
        x = (i % 2 + y) % 2
        return (r, (y * 2 + x) * 2 + q)

    partner = (r, k * 2 + 1 - q)
    across = (1 - r, col)

    def pair_of(t):
        return npair - 1 - t

    def sb_of(t):
        return pair_of(t) // RING

    def chip_of(t):
        return pair_of(t) % RING

    def owner_dist(t):
        kk = chip_of(t)
        y = kk // 2
        ro = 2 * y + (kk % 2 + y) % 2
        return (rho - ro + RING) % RING

    def height(t):
        return nsb - sb_of(t)

    def half_of(t, c):
        return (c - sb_of(t) + (height(t) - 1) // 2) % 2

    def head_half(t):
        return height(t) % 2

    def partial(t, fn):
        kk = chip_of(t)
        for j in range(RING - 1):

            @pl.when(kk == j)
            def _(j=j):
                fn(pl.multiple_of(sb_of(t) * CH + (j + 1) * NB, NB), CH - (j + 1) * NB)

    def full(t, fn):
        def one(c, _):
            fn(c, pl.multiple_of(c * CH, CH), CH)
            return 0

        lax.fori_loop(sb_of(t) + 1, nsb, one, 0)

    def in_half(t, half, fn):
        flip = (height(t) - 1) // 2

        @pl.when(head_half(t) == half)
        def _():
            fn(HEAD, None, None)

        @pl.when(flip % 2 == half)
        def _():
            partial(t, lambda r0, n: fn(sb_of(t), r0, n))

        full_half(t, half, fn, 0, nsb)

    def count_half(t, half):
        first = 2 - (half + (height(t) - 1) // 2) % 2
        return (height(t) - first + 1) // 2, sb_of(t) + first

    def full_half(t, half, fn, lo, hi):
        cnt, first = count_half(t, half)

        def one(j, _):
            c = first + 2 * j
            fn(c, pl.multiple_of(c * CH, CH), CH)
            return 0

        lax.fori_loop(lo, jnp.minimum(cnt, hi), one, 0)

    def head_rows(t):
        return pl.ds(pl.multiple_of(pair_of(t) * NB, NB), NB)

    def lanes(l):
        return pl.ds(pl.multiple_of(l * NB, NB), NB)

    def rcopy(src, dst, ssem, rsem, dev):
        return pltpu.make_async_remote_copy(src, dst, ssem, rsem, device_id=dev, device_id_type=MESH_ID)

    def panel(t, r0, n, own):
        if own:
            return v_ref.at[pl.ds(r0, n), lanes(sb_of(t))]
        return vb.at[q, pair_of(t), pl.ds(r0, n), :]

    def side_copy(src, dst, t, c, d):
        return rcopy(src, dst, i_snd.at[d, t % SLOTS, c], i_rcv.at[t, c], at_ring(rho + 1 - 2 * d + RING))

    def core_copy(src, dst, t, c):
        return rcopy(src, dst, d_snd.at[t % SLOTS, c], d_rcv.at[t, c], partner)

    def ends(t, c, own, r0=None, n=None):
        if c is HEAD:
            dst = vb.at[q, pair_of(t), head_rows(t), :]
            return (eb.at[sb_of(t)] if own else dst), dst
        return panel(t, r0, n, own), panel(t, r0, n, False)

    def wait_sent(t, c, half, r0=None, n=None):
        src, dst = ends(t, c, False, r0, n)
        d = owner_dist(t)

        @pl.when((d == 0) | ((d == 1) & (half == 0)))
        def _():
            side_copy(src, dst, t, c, 0).wait_send()

        @pl.when((d == 0) | ((d == 3) & (half == 1)))
        def _():
            side_copy(src, dst, t, c, 1).wait_send()

        core_copy(src, dst, t, c).wait_send()

    def all_sent(t):
        wait_sent(t, HEAD, head_half(t))

        partial(t, lambda r0, n: wait_sent(t, sb_of(t), half_of(t, sb_of(t)), r0, n))
        full(t, lambda c, r0, n: wait_sent(t, c, half_of(t, c), r0, n))

    def free_slot(t):
        @pl.when(t >= SLOTS)
        def _():
            all_sent(t - SLOTS)

    def send_own(u):
        first = RING - 1 - k
        part = (u - first + 2 * RING) % RING
        t = u - part

        @pl.when((t >= 0) & (t < npair))
        def _():
            @pl.when(part == 0)
            def _():
                free_slot(t)

                def over(c, r0, n):
                    src, dst = ends(t, c, True, r0, n)
                    core_copy(src, dst, t, c).start()

                over(HEAD, None, None)
                partial(t, lambda r0, n: over(sb_of(t), r0, n))
                full(t, over)

            def side(d, _):
                half = (d + part // 2) % 2

                def out(c, r0, n):
                    src, dst = ends(t, c, True, r0, n)
                    rcopy(src, dst, i_snd.at[d, t % SLOTS, c], i_rcv.at[t, c], at_ring(rho + 1 - 2 * d + RING)).start()

                cnt, _ = count_half(t, half)
                mid = (cnt + 1) // 2

                @pl.when(part % 2 == 0)
                def _():
                    @pl.when(head_half(t) == half)
                    def _():
                        out(HEAD, None, None)

                    @pl.when((height(t) - 1) // 2 % 2 == half)
                    def _():
                        partial(t, lambda r0, n: out(sb_of(t), r0, n))

                full_half(t, half, out, jnp.where(part % 2 == 0, 0, mid), jnp.where(part % 2 == 0, mid, cnt))
                return 0

            lax.fori_loop(0, 2, side, 0)

    def pass_on(t, half, forward):
        def got(c, r0, n):
            src, dst = ends(t, c, False, r0, n)
            side_copy(src, dst, t, c, 0).wait_recv()
            core_copy(src, dst, t, c).start()

            @pl.when(forward)
            def _():
                rcopy(src, dst, i_snd.at[half, t % SLOTS, c], i_rcv.at[t, c], at_ring(rho + 1 - 2 * half + RING)).start()

        in_half(t, half, got)

    def brought(i):
        return jnp.minimum(npair - 1, jnp.minimum(i + 2, jnp.maximum(AHEAD + 1, i + 1)))

    def falling(i, high, low, i0, i1):
        return high - jnp.clip(((high - low) * (i - i0) + i1 - i0 - 1) // (i1 - i0), 0, high - low)

    def hand_lead(i):
        return jnp.minimum(npair - 1, brought(i) + jnp.minimum(falling(i, 5, 3, 15, 26), i + 3))

    def rest_lead(i):
        return jnp.minimum(npair - 1, brought(i) + jnp.where(i < 27, jnp.minimum(1, i + 3), 0))

    def far_lead(i):
        return jnp.minimum(npair - 1, brought(i) + jnp.where((i >= 4) & (i < 15), 1, 0))

    def own_lead(i):
        return jnp.minimum(npair + RING - 2, brought(i) + jnp.minimum(falling(i, 10, 6, 13, 28), 4 + 3 * (i + 2)))

    def span(lead, i):
        return jnp.where(i < -1, 0, lead(i - 1) + 1), lead(i) + 1

    def service(i):
        def one(j, _):
            kind = jnp.where(i < -1, j, 3 - j)

            @pl.when(kind == 0)
            def _():
                lo, hi = span(own_lead, i)
                lax.fori_loop(lo, hi, lambda u, _: (send_own(u), 0)[1], 0)

            @pl.when(kind > 0)
            def _():
                h = span(hand_lead, i)
                e = span(rest_lead, i)
                f = span(far_lead, i)
                lo, hi = (jnp.where(kind == 1, x, jnp.where(kind == 2, y, z)) for x, y, z in zip(h, e, f))

                def take(x, _):
                    t = lo + x // 2
                    d = owner_dist(t)
                    half = x % 2
                    mine = jnp.where(d == 1, 0, 1)
                    afar = (kind == 3) & (d == 2)
                    hand = (kind == 1) & (d % 2 == 1) & (half == mine)
                    rest = (kind == 2) & (d % 2 == 1) & (half != mine)

                    @pl.when(hand | (afar & (half == 0)))
                    def _():
                        free_slot(t)

                    @pl.when(afar | hand | rest)
                    def _():
                        pass_on(t, half, hand)

                    return 0

                lax.fori_loop(0, 2 * jnp.maximum(hi - lo, 0), take, 0)

            return 0

        lax.fori_loop(0, 4, one, 0)

    def make_heads():
        def copies(l):
            rr = pl.ds(pl.multiple_of((l * RING + k) * NB, NB), NB)
            return (pltpu.make_async_copy(v_ref.at[rr, lanes(l)], eb.at[l], h_sem.at[0, l]),
                    pltpu.make_async_copy(t_ref.at[l], et.at[l], h_sem.at[1, l]))

        def begin(l, _):
            for c in copies(l):
                c.start()
            return 0

        lax.fori_loop(0, nsb, begin, 0)

        def one(l, _):
            for c in copies(l):
                c.wait()
            x = eb[l]
            tt = et[l]
            below = lax.broadcasted_iota(jnp.int32, (NB, NB), 0) > lax.broadcasted_iota(jnp.int32, (NB, NB), 1)
            both_in = jnp.where(below, x, tt)
            eb[l] = jnp.where(r == q, both_in, jnp.where(r == 0, tt, x))
            return 0

        lax.fori_loop(0, nsb, one, 0)

    def z_local(c):
        mine = pl.multiple_of(r * rows + c * CH, CH)
        return pltpu.make_async_copy(z_ref.at[pl.ds(mine, CH), :], zl.at[r, chunk_at(c), :], z_loc.at[c])

    def z_piece(w):
        c = nsb - 1 - w // RING
        r0 = c * CH + w % RING * NB
        theirs = pl.multiple_of((1 - r) * rows + r0, NB)
        return rcopy(z_ref.at[pl.ds(theirs, NB), :], zl.at[r, pl.ds(pl.multiple_of(r0, NB), NB), :],
                     z_snd.at[w], z_rcv.at[w], across)

    def put_x(g, x, at):
        xt[g, :, at] = x
        for i, piece in enumerate(split3(x)):
            xp[g, i * NB : (i + 1) * NB, at] = piece

    def admit(c):
        for j in range(RING):
            z_piece((nsb - 1 - c) * RING + j).wait()
        z_local(c).wait()

        def one(g, _):
            put_x(g, zl[g, chunk_at(c), :].T, chunk_at(c))
            return 0

        lax.fori_loop(0, 2, one, 0)

    def load(t, c, side, src, at):
        return pltpu.make_async_copy(src, vf.at[at, lanes(side)], ld.at[side, c])

    def start_loads(t):
        mine = owner_dist(t) == 0
        p = pair_of(t)

        def one(c, r0, n):
            at = pl.ds(r0, n)

            @pl.when(mine)
            def _():
                load(t, c, q, panel(t, r0, n, True), at).start()

            @pl.when(jnp.logical_not(mine))
            def _():
                load(t, c, q, panel(t, r0, n, False), at).start()

            src, dst = ends(t, c, False, r0, n)
            core_copy(src, dst, t, c).wait_recv()
            load(t, c, 1 - q, vb.at[1 - q, p, at, :], at).start()

        at = head_rows(t)

        @pl.when(jnp.logical_not(mine))
        def _():
            load(t, HEAD, q, vb.at[q, p, at, :], at).start()

        core_copy(*ends(t, HEAD, False), t, HEAD).wait_recv()
        load(t, HEAD, 1 - q, vb.at[1 - q, p, at, :], at).start()

        partial(t, lambda r0, n: one(sb_of(t), r0, n))
        full(t, one)

    def pieces(slot, at, x):
        for i, piece in enumerate(split3(x)):
            vn[slot, at, i * PW : (i + 1) * PW] = piece

    def prep(t):
        slot = t % 3
        mine = owner_dist(t) == 0
        at = head_rows(t)
        l = sb_of(t)

        load(t, HEAD, 1 - q, vb.at[0, 0, at, :], at).wait()

        @pl.when((r == 0) & (q == 0) & (t >= 3))
        def _():
            factor_across(t - 3).wait_send()

        @pl.when(mine)
        def _():
            vf[at, lanes(q)] = eb[l]

        @pl.when(jnp.logical_not(mine))
        def _():
            load(t, HEAD, q, vb.at[0, 0, at, :], at).wait()

        def above(j, _):
            pieces(slot, pl.ds(pl.multiple_of(l * CH + j * NB, NB), NB), jnp.zeros((NB, PW), F32))
            return 0

        lax.fori_loop(0, chip_of(t), above, 0)

        i0 = lax.broadcasted_iota(jnp.int32, (NB, NB), 0)
        i1 = lax.broadcasted_iota(jnp.int32, (NB, NB), 1)
        one = jnp.where(i0 == i1, 1.0, 0.0).astype(F32)
        x0 = vf[at, 0:NB]
        x1 = vf[at, NB:PW]
        first = r == 0
        v0 = jnp.where(first, jnp.where(i0 > i1, x0, one), x0)
        v1 = jnp.where(first, 0.0, jnp.where(i0 > i1, x1, one))
        tc[slot, 0] = jnp.where(i0 > i1, 0.0, x0)
        tc[slot, 1] = jnp.where(i0 > i1, 0.0, x1)
        pieces(slot, at, jnp.concatenate([v0, v1], axis=1))

        @pl.when(first & (q == 0))
        def _():
            factor_across(t).start()

        def rest(r0, n):
            a = pl.ds(r0, n)
            for side in range(2):
                load(t, l, side, vb.at[0, 0, a, :], a).wait()

            def sub(j, _):
                b = pl.ds(pl.multiple_of(r0 + j * NB, NB), NB)
                pieces(slot, b, vf[b, :])
                return 0

            lax.fori_loop(0, n // NB, sub, 0)

        partial(t, rest)

        def chunk(c, r0, n):
            a = pl.ds(r0, n)
            for side in range(2):
                load(t, c, side, vb.at[0, 0, a, :], a).wait()
            for j in range(0, n, NB):
                b = pl.ds(pl.multiple_of(r0 + j, NB), NB)
                pieces(slot, b, vf[b, :])

        full(t, chunk)

    def factor_across(t):
        return rcopy(tc.at[t % 3, 0], tb.at[t % 8], t_snd.at[0, t % 8], t_rcv.at[0, t % 8], across)

    def factor_over(t):
        return rcopy(tb.at[t % 8], tb.at[t % 8], t_snd.at[1, t % 8], t_rcv.at[1, t % 8], partner)

    def share_factor(t):
        @pl.when((r == 1) & (q == 0))
        def _():
            factor_across(t).wait_recv()

            @pl.when(t >= 2)
            def _():
                factor_over(t - 2).wait_send()

            factor_over(t).start()

    def late(t):
        return t > AHEAD + 1

    def part_copy(t):
        return rcopy(gs.at[t % 2], gp.at[t % 2], p_snd.at[t % 2], p_rcv.at[t % 2], partner)

    def plane_copy(t):
        return rcopy(gz.at[t % 2], gr.at[t % 2], g_snd.at[t % 2], g_rcv.at[t % 2], across)

    def total_copy(t):
        return rcopy(gf.at[t % 8], gf.at[t % 8], f_snd.at[t % 8], f_rcv.at[t % 8], partner)

    def gram_part(t):
        slot = t % 3
        s = t % 2

        @pl.when(t >= 2)
        def _():
            part_copy(t - 2).wait_send()

        gs[s] = jnp.zeros((NB, NB), F32)
        first = (height(t) + t % 2) // 2
        lo = sb_of(t) + q * first
        cnt = jnp.where(q == 0, first, height(t) - first)

        def block(c, n):
            at = pl.ds(pl.multiple_of(c * CH, CH), n * CH)
            a = [vn[slot, at, i * PW : i * PW + NB].T for i in range(3)]
            b = [vn[slot, at, i * PW + NB : (i + 1) * PW] for i in range(3)]
            x = mm(jnp.concatenate(a, axis=0), jnp.concatenate(b[0:2], axis=1))
            gs[s] += add_rows(add_rows(mm(a[0], b[2]), x[:, 0:NB], NB), x[0 : 2 * NB, NB:PW], NB)

        if nsb >= 8:

            @pl.when(cnt >= 4)
            def _():
                block(lo, 4)

        if nsb >= 3:

            @pl.when(cnt % 4 >= 2)
            def _():
                block(lo + cnt // 4 * 4, 2)

        @pl.when(cnt % 2 == 1)
        def _():
            block(lo + cnt - 1, 1)

        part_copy(t).start()

    def sends_plane(t):
        return late(t) | (t % 2 == q)

    def gram_plane(t):
        s = t % 2
        part_copy(t).wait_recv()

        @pl.when((t >= 2) & sends_plane(t - 2))
        def _():
            plane_copy(t - 2).wait_send()

        gz[s] = gs[s] + gp[s]

        @pl.when(sends_plane(t))
        def _():
            plane_copy(t).start()

    def gram_total(t):
        s = t % 2

        @pl.when(sends_plane(t))
        def _():
            plane_copy(t).wait_recv()

            @pl.when((t >= 8) & (t % 2 == q) & jnp.logical_not(late(t - 8)))
            def _():
                total_copy(t - 8).wait_send()

            gf[t % 8] = gz[s] + gr[s]

            @pl.when(jnp.logical_not(late(t)))
            def _():
                total_copy(t).start()

    def block_factor(t):
        slot = t % 3

        @pl.when(jnp.logical_not(sends_plane(t)))
        def _():
            total_copy(t).wait_recv()

        @pl.when((r == 1) & (q == 1))
        def _():
            factor_over(t).wait_recv()

        g = gf[t % 8]
        ta = jnp.where(r == 0, tc[slot, 0], tb[t % 8])
        tbb = tc[slot, 1]
        upper = -full_dot(ta, full_dot(g, tbb))
        for i, piece in enumerate(split3(ta)):
            tp[0:NB, i * PW : i * PW + NB] = piece
        for i, piece in enumerate(split3(upper)):
            tp[0:NB, i * PW + NB : (i + 1) * PW] = piece
        for i, piece in enumerate(split3(tbb)):
            tp[NB:PW, i * PW : i * PW + NB] = jnp.zeros((NB, NB), BF16)
            tp[NB:PW, i * PW + NB : (i + 1) * PW] = piece

    def w_copy(t, g):
        return rcopy(ws.at[t % 2, g], wr.at[t % 2, g], w_snd.at[t % 2, g], w_rcv.at[t % 2, g], across)

    def coefficients(t, g):
        with jax.named_scope("wwait"):
            w_copy(t, g).wait_recv()
        w = ws[t % 2, g] + wr[t % 2, g]
        y = stacked(mm_nt, jnp.concatenate(split3(w), axis=0), [tp[:, i * PW : (i + 1) * PW] for i in range(3)])
        for i, piece in enumerate(split3(y)):
            yp[i * NB : (i + 1) * NB] = piece

    def piece_of(t, i, at):
        return vn[t % 3, at, i * PW : (i + 1) * PW]

    def chunk_at(c):
        return pl.ds(pl.multiple_of(c * CH, CH), CH)

    def passes(m, i, g, n, finish):
        units = m * CH // UNIT
        base = rows - m * CH
        w = None
        for c in range(units + (0 if n is None else LAG)):
            at = pl.ds(base + c * UNIT, UNIT)
            an = pl.ds(max(0, base + (c - LAG) * UNIT), UNIT)
            u = None
            for j in range(3):
                k3 = (3 - j) * NB
                if n is not None and c >= LAG:
                    w = add_rows(w, mm(xp[g, 0:k3, an], piece_of(n, j, an)), NB)
                if c < units:
                    u = add_rows(u, mm_nt(yp[0:k3], piece_of(i, j, at)), NB)
            if c < units:
                finish(at, xt[g, :, at] - u)
        if n is not None:
            ws[n % 2, g] += w

    def product(n, g, at):
        w = None
        for j in range(3):
            w = add_rows(w, mm(xp[g, 0 : (3 - j) * NB, at], piece_of(n, j, at)), NB)
        ws[n % 2, g] += w

    def both(i, g):
        n = i + 1

        @pl.when(sb_of(n) < sb_of(i))
        def _():
            product(n, g, chunk_at(sb_of(n)))

        for m in range(1, nsb + 1):

            @pl.when(height(i) == m)
            def _(m=m):
                passes(m, i, g, n, lambda at, x: put_x(g, x, at))

    def out_copy(g, c):
        return pltpu.make_async_copy(zl.at[g, chunk_at(c), :], out_ref.at[chunk_at(c), lanes(g)], o_sem.at[g, c])

    def last(i, g):
        def finish(at, x):
            zl[g, at, :] = x.T

        passes(nsb, i, g, None, finish)

        def out(c, _):
            out_copy(g, c).start()
            return 0

        lax.fori_loop(0, nsb, out, 0)

    def step(i, _):
        n = i + 1
        early = i < AHEAD
        b = jnp.where(early, i + 2, n)
        brings = (i != AHEAD) & (b < npair)

        @pl.when(i < npair - 1)
        def _():
            with jax.named_scope("svc"):
                service(i)

        @pl.when(brings)
        def _():
            with jax.named_scope("loads"):
                start_loads(b)

        @pl.when(i >= 0)
        def _():
            with jax.named_scope("bfac"):
                block_factor(i)

        @pl.when(n == npair)
        def _():
            lax.fori_loop(max(0, npair - SLOTS), npair, lambda t, _: (all_sent(t), 0)[1], 0)

        @pl.when((n >= 0) & (n < npair) & (n % RING == 0))
        def _():
            with jax.named_scope("admit"):
                admit(sb_of(n))

        def group(g, _):
            @pl.when((g == jnp.where(early, 1, 0)) & brings)
            def _():
                with jax.named_scope("prep"):
                    prep(b)
                with jax.named_scope("gram"):
                    gram_part(b)

            @pl.when(i >= 0)
            def _():
                with jax.named_scope("coef"):
                    coefficients(i, g)

            @pl.when((n >= 0) & (n < npair))
            def _():
                @pl.when(n >= 2)
                def _():
                    w_copy(n - 2, g).wait_send()

                ws[n % 2, g] = jnp.zeros((NB, PW), F32)

            @pl.when(i == -1)
            def _():
                product(n, g, chunk_at(nsb - 1))

            @pl.when((i >= 0) & (n < npair))
            def _():
                with jax.named_scope("both"):
                    both(i, g)

            @pl.when((g == jnp.where(early, 1, 0)) & brings)
            def _():
                with jax.named_scope("gplane"):
                    gram_plane(b)

            @pl.when((n >= 0) & (n < npair))
            def _():
                w_copy(n, g).start()

                @pl.when(g == jnp.where(i <= AHEAD, 0, 1))
                def _():
                    with jax.named_scope("fshare"):
                        share_factor(n)
                    with jax.named_scope("gtot"):
                        gram_total(n)

            @pl.when(n == npair)
            def _():
                with jax.named_scope("last"):
                    last(i, g)

            return 0

        lax.fori_loop(0, 2, group, 0)

        @pl.when((n >= RING + 1) & (n + RING + 1 < npair))
        def _():
            z_piece(n + RING + 1).start()

        @pl.when((n >= 0) & (n % RING == 2) & (n + RING < npair))
        def _():
            z_local(sb_of(n) - 1).start()

        return 0

    barrier = pltpu.get_barrier_semaphore()
    for dev in (at_ring(rho + 1), at_ring(rho + RING - 1), partner, across):
        pl.semaphore_signal(barrier, inc=1, device_id=dev, device_id_type=MESH_ID)
    pl.semaphore_wait(barrier, 4)

    for j in range(min(2 * RING + 2, npair)):
        z_piece(j).start()
    z_local(nsb - 1).start()
    with jax.named_scope("heads"):
        make_heads()
    lax.fori_loop(-2, npair, step, 0)

    for t in (npair - 2, npair - 1):
        for g in range(2):
            w_copy(t, g).wait_send()
    for t in (npair - 2, npair - 1):
        part_copy(t).wait_send()

        @pl.when(sends_plane(t))
        def _(t=t):
            plane_copy(t).wait_send()

    newest = min(npair - 1, AHEAD + 1)
    for t in range(max(0, npair - 8), newest + 1):

        @pl.when(t % 2 == q)
        def _(t=t):
            total_copy(t).wait_send()

    for t in range(npair - 3, npair):

        @pl.when((r == 0) & (q == 0))
        def _(t=t):
            factor_across(t).wait_send()

    for t in range(npair - 2, npair):

        @pl.when((r == 1) & (q == 0))
        def _(t=t):
            factor_over(t).wait_send()

    def out_done(c, _):
        for g in range(2):
            out_copy(g, c).wait()
        return 0

    lax.fori_loop(0, nsb, out_done, 0)


def solution(mesh):
    def local(v, t, z):
        rows, cols = v.shape
        nsb = cols // NB
        npair = nsb * RING
        hbm = pl.BlockSpec(memory_space=pltpu.MemorySpace.HBM)
        out, _ = pl.pallas_call(
            functools.partial(body, nsb),
            out_shape=(
                jax.ShapeDtypeStruct((rows, PW), F32),
                jax.ShapeDtypeStruct((2, npair, rows, NB), F32),
            ),
            in_specs=[hbm] * 3,
            out_specs=(hbm, hbm),
            scratch_shapes=[
                pltpu.VMEM((2, rows, NB), F32),
                pltpu.VMEM((2, NB, rows), F32),
                pltpu.VMEM((2, 3 * NB, rows), BF16),
                pltpu.VMEM((rows, PW), F32),
                pltpu.VMEM((3, rows, 3 * PW), BF16),
                pltpu.VMEM((8, NB, NB), F32),
                pltpu.VMEM((3, 2, NB, NB), F32),
                pltpu.VMEM((PW, 3 * PW), BF16),
                pltpu.VMEM((2, 2, NB, PW), F32),
                pltpu.VMEM((2, 2, NB, PW), F32),
                pltpu.VMEM((2, NB, NB), F32),
                pltpu.VMEM((2, NB, NB), F32),
                pltpu.VMEM((2, NB, NB), F32),
                pltpu.VMEM((2, NB, NB), F32),
                pltpu.VMEM((8, NB, NB), F32),
                pltpu.VMEM((3 * NB, PW), BF16),
                pltpu.VMEM((nsb, NB, NB), F32),
                pltpu.VMEM((nsb, NB, NB), F32),
            ],
            compiler_params=pltpu.CompilerParams(
                collective_id=0, has_side_effects=True, vmem_limit_bytes=60 * 2**20),
            name="backtransform",
        )(v, t, z)
        return out

    return jax.shard_map(local, mesh=mesh,
                         in_specs=(P("row", "col"), P("col", None, None), P(None, ("col", "row"))),
                         out_specs=P("row", "col"), check_vma=False)
```

```python
import functools

import jax
import jax.numpy as jnp
from jax import lax
from jax.experimental import pallas as pl
from jax.experimental.pallas import tpu as pltpu
from jax.sharding import PartitionSpec as P

F32 = jnp.float32
BF16 = jnp.bfloat16
MESH_ID = pl.DeviceIdType.MESH

NB = 128
PW = 2 * NB
CH = 4 * NB
UNIT = PW
LAG = 2
RING = 4
SLOTS = 16
AHEAD = 20


def split3(x):
    hi = x.astype(BF16)
    rest = x - hi.astype(F32)
    mid = rest.astype(BF16)
    low = (rest - mid.astype(F32)).astype(BF16)
    return hi, mid, low


def mm(a, b):
    return lax.dot_general(a, b, (((1,), (0,)), ((), ())), preferred_element_type=F32)


def mm_nt(a, b):
    return lax.dot_general(a, b, (((1,), (1,)), ((), ())), preferred_element_type=F32)


def add_rows(total, x, n):
    for i in range(0, x.shape[0], n):
        part = x[i : i + n]
        total = part if total is None else total + part
    return total


def stacked(dot, a3, b):
    m = a3.shape[0] // 3
    s = None
    for i in range(3):
        s = add_rows(s, dot(a3[0 : (3 - i) * m], b[i]), m)
    return s


def full_dot(a, b):
    ah, am, al = split3(a)
    bh, bm, bl = split3(b)
    n = a.shape[0]
    x = mm(jnp.concatenate([ah, am], axis=1), jnp.concatenate([jnp.concatenate([bh, bm], axis=1)] * 2, axis=0))
    y = mm(jnp.concatenate([al, ah], axis=1), jnp.concatenate([bh, bl], axis=0))
    return x[:, 0:n] + x[:, n:] + y


def body(nsb, v_ref, t_ref, z_ref, out_ref, vb, *scratch):
    rows = nsb * CH
    dma = pltpu.SemaphoreType.DMA
    npair = nsb * RING
    nc = nsb + RING
    pl.run_scoped(
        functools.partial(run, nsb, rows, npair, v_ref, t_ref, z_ref, out_ref, vb, scratch),
        dma((nsb,)),
        dma((npair,)),
        dma((npair,)),
        dma((npair, nc)),
        dma((npair, nc)),
        dma((2, 2)),
        dma((2, 2)),
        dma((2,)),
        dma((2,)),
        dma((8,)),
        dma((8,)),
        dma((2, nc)),
        dma((2, nsb)),
        dma((2, SLOTS, nc)),
        dma((SLOTS, nc)),
        dma((2, nsb)),
        dma((2,)),
        dma((2,)),
        dma((2, 8)),
        dma((2, 8)),
    )


def run(nsb, rows, npair, v_ref, t_ref, z_ref, out_ref, vb, scratch, *sems):
    (zl, xt, xp, vf, vn, tb, tc, tp, ws, wr, gs, gp, gz, gr, gf, yp, eb, et) = scratch
    (z_loc, z_snd, z_rcv, i_rcv, d_rcv, w_snd, w_rcv, g_snd, g_rcv, f_snd, f_rcv, ld, o_sem, i_snd, d_snd, h_sem, p_snd, p_rcv, t_snd, t_rcv) = sems
    r = lax.axis_index("row")
    col = lax.axis_index("col")
    q = col % 2
    k = col // 2
    ky, kx = k // 2, k % 2
    rho = 2 * ky + (kx + ky) % 2

    def at_ring(i):
        i = i % RING
        y = i // 2
        x = (i % 2 + y) % 2
        return (r, (y * 2 + x) * 2 + q)

    partner = (r, k * 2 + 1 - q)
    across = (1 - r, col)

    def pair_of(t):
        return npair - 1 - t

    def sb_of(t):
        return pair_of(t) // RING

    def chip_of(t):
        return pair_of(t) % RING

    def owner_dist(t):
        kk = chip_of(t)
        y = kk // 2
        ro = 2 * y + (kk % 2 + y) % 2
        return (rho - ro + RING) % RING

    def height(t):
        return nsb - sb_of(t)

    def half_of(t, c):
        return (c - sb_of(t) + (height(t) - 1) // 2) % 2

    def small_half(t):
        return (height(t) - 1) // 2 % 2

    def small(t, first, fn):
        def one(j, _):
            fn(nsb + j, pl.multiple_of((pair_of(t) + j) * NB, NB), NB)
            return 0

        lax.fori_loop(first, RING - chip_of(t), one, 0)

    def full(t, fn):
        def one(c, _):
            fn(c, pl.multiple_of(c * CH, CH), CH)
            return 0

        lax.fori_loop(sb_of(t) + 1, nsb, one, 0)

    def in_half(t, half, fn):
        @pl.when(small_half(t) == half)
        def _():
            small(t, 0, fn)

        full_half(t, half, fn, 0, nsb)

    def count_half(t, half):
        first = 2 - (half + (height(t) - 1) // 2) % 2
        return (height(t) - first + 1) // 2, sb_of(t) + first

    def full_half(t, half, fn, lo, hi):
        cnt, first = count_half(t, half)

        def one(j, _):
            c = first + 2 * j
            fn(c, pl.multiple_of(c * CH, CH), CH)
            return 0

        lax.fori_loop(lo, jnp.minimum(cnt, hi), one, 0)

    def head_row(t):
        return pl.multiple_of(pair_of(t) * NB, NB)

    def head_rows(t):
        return pl.ds(pl.multiple_of(pair_of(t) * NB, NB), NB)

    def lanes(l):
        return pl.ds(pl.multiple_of(l * NB, NB), NB)

    def rcopy(src, dst, ssem, rsem, dev):
        return pltpu.make_async_remote_copy(src, dst, ssem, rsem, device_id=dev, device_id_type=MESH_ID)

    def panel(t, r0, n, own):
        if own:
            return v_ref.at[pl.ds(r0, n), lanes(sb_of(t))]
        return vb.at[q, pair_of(t), pl.ds(r0, n), :]

    def side_copy(src, dst, t, c, d):
        return rcopy(src, dst, i_snd.at[d, t % SLOTS, c], i_rcv.at[t, c], at_ring(rho + 1 - 2 * d + RING))

    def core_copy(src, dst, t, c):
        return rcopy(src, dst, d_snd.at[t % SLOTS, c], d_rcv.at[t, c], partner)

    def wait_sent(t, c, half, r0, n):
        here = panel(t, r0, n, False)
        d = owner_dist(t)

        @pl.when((d == 0) | ((d == 1) & (half == 0)))
        def _():
            side_copy(here, here, t, c, 0).wait_send()

        @pl.when((d == 0) | ((d == 3) & (half == 1)))
        def _():
            side_copy(here, here, t, c, 1).wait_send()

        core_copy(here, here, t, c).wait_send()

    def all_sent(t):
        small(t, 0, lambda c, r0, n: wait_sent(t, c, small_half(t), r0, n))
        full(t, lambda c, r0, n: wait_sent(t, c, half_of(t, c), r0, n))

    def free_slot(t):
        @pl.when(t >= SLOTS)
        def _():
            all_sent(t - SLOTS)

    def send_own(u):
        first = RING - 1 - k
        part = (u - first + 2 * RING) % RING
        t = u - part

        @pl.when((t >= 0) & (t < npair))
        def _():
            @pl.when(part == 0)
            def _():
                free_slot(t)

                def over(c, r0, n):
                    core_copy(panel(t, r0, n, True), panel(t, r0, n, False), t, c).start()

                core_copy(eb.at[sb_of(t)], panel(t, head_row(t), NB, False), t, nsb).start()
                small(t, 1, over)
                full(t, over)

            def side(d, _):
                half = (d + part // 2) % 2

                def send(src, dst, c):
                    rcopy(src, dst, i_snd.at[d, t % SLOTS, c], i_rcv.at[t, c], at_ring(rho + 1 - 2 * d + RING)).start()

                def out(c, r0, n):
                    send(panel(t, r0, n, True), panel(t, r0, n, False), c)

                cnt, _ = count_half(t, half)
                mid = (cnt + 1) // 2

                @pl.when((part % 2 == 0) & (small_half(t) == half))
                def _():
                    send(eb.at[sb_of(t)], panel(t, head_row(t), NB, False), nsb)
                    small(t, 1, out)

                full_half(t, half, out, jnp.where(part % 2 == 0, 0, mid), jnp.where(part % 2 == 0, mid, cnt))
                return 0

            lax.fori_loop(0, 2, side, 0)

    def pass_on(t, half, forward):
        def got(c, r0, n):
            here = panel(t, r0, n, False)
            side_copy(here, here, t, c, 0).wait_recv()
            core_copy(here, here, t, c).start()

            @pl.when(forward)
            def _():
                rcopy(here, here, i_snd.at[half, t % SLOTS, c], i_rcv.at[t, c], at_ring(rho + 1 - 2 * half + RING)).start()

        in_half(t, half, got)

    def brought(i):
        return jnp.minimum(npair - 1, jnp.minimum(i + 2, jnp.maximum(AHEAD + 1, i + 1)))

    def falling(i, high, low, i0, i1):
        return high - jnp.clip(((high - low) * (i - i0) + i1 - i0 - 1) // (i1 - i0), 0, high - low)

    def hand_lead(i):
        return jnp.minimum(npair - 1, brought(i) + jnp.minimum(falling(i, 5, 3, 15, 26), i + 3))

    def rest_lead(i):
        return jnp.minimum(npair - 1, brought(i) + jnp.where(i < 27, jnp.minimum(1, i + 3), 0))

    def far_lead(i):
        return jnp.minimum(npair - 1, brought(i) + jnp.where((i >= 4) & (i < 15), 1, 0))

    def own_lead(i):
        return jnp.minimum(npair + RING - 2, brought(i) + jnp.minimum(falling(i, 10, 6, 13, 28), 4 + 3 * (i + 2)))

    def span(lead, i):
        return jnp.where(i < -1, 0, lead(i - 1) + 1), lead(i) + 1

    def service(i):
        def one(j, _):
            kind = jnp.where(i < -1, j, 3 - j)

            @pl.when(kind == 0)
            def _():
                lo, hi = span(own_lead, i)
                lax.fori_loop(lo, hi, lambda u, _: (send_own(u), 0)[1], 0)

            @pl.when(kind > 0)
            def _():
                h = span(hand_lead, i)
                e = span(rest_lead, i)
                f = span(far_lead, i)
                lo, hi = (jnp.where(kind == 1, x, jnp.where(kind == 2, y, z)) for x, y, z in zip(h, e, f))

                def take(x, _):
                    t = lo + x // 2
                    d = owner_dist(t)
                    half = x % 2
                    mine = jnp.where(d == 1, 0, 1)
                    afar = (kind == 3) & (d == 2)
                    hand = (kind == 1) & (d % 2 == 1) & (half == mine)
                    rest = (kind == 2) & (d % 2 == 1) & (half != mine)

                    @pl.when(hand | (afar & (half == 0)))
                    def _():
                        free_slot(t)

                    @pl.when(afar | hand | rest)
                    def _():
                        pass_on(t, half, hand)

                    return 0

                lax.fori_loop(0, 2 * jnp.maximum(hi - lo, 0), take, 0)

            return 0

        lax.fori_loop(0, 4, one, 0)

    def make_heads():
        def copies(l):
            rr = pl.ds(pl.multiple_of((l * RING + k) * NB, NB), NB)
            return (pltpu.make_async_copy(v_ref.at[rr, lanes(l)], eb.at[l], h_sem.at[0, l]),
                    pltpu.make_async_copy(t_ref.at[l], et.at[l], h_sem.at[1, l]))

        def begin(l, _):
            for c in copies(l):
                c.start()
            return 0

        lax.fori_loop(0, nsb, begin, 0)

        def one(l, _):
            for c in copies(l):
                c.wait()
            x = eb[l]
            tt = et[l]
            below = lax.broadcasted_iota(jnp.int32, (NB, NB), 0) > lax.broadcasted_iota(jnp.int32, (NB, NB), 1)
            both_in = jnp.where(below, x, tt)
            eb[l] = jnp.where(r == q, both_in, jnp.where(r == 0, tt, x))
            return 0

        lax.fori_loop(0, nsb, one, 0)

    def z_local(c):
        mine = pl.multiple_of(r * rows + c * CH, CH)
        return pltpu.make_async_copy(z_ref.at[pl.ds(mine, CH), :], zl.at[r, chunk_at(c), :], z_loc.at[c])

    def z_piece(w):
        c = nsb - 1 - w // RING
        r0 = c * CH + w % RING * NB
        theirs = pl.multiple_of((1 - r) * rows + r0, NB)
        return rcopy(z_ref.at[pl.ds(theirs, NB), :], zl.at[r, pl.ds(pl.multiple_of(r0, NB), NB), :],
                     z_snd.at[w], z_rcv.at[w], across)

    def put_x(g, x, at):
        xt[g, :, at] = x
        for i, piece in enumerate(split3(x)):
            xp[g, i * NB : (i + 1) * NB, at] = piece

    def admit(c):
        for j in range(RING):
            z_piece((nsb - 1 - c) * RING + j).wait()
        z_local(c).wait()

        def one(g, _):
            put_x(g, zl[g, chunk_at(c), :].T, chunk_at(c))
            return 0

        lax.fori_loop(0, 2, one, 0)

    def load(t, c, side, src, at):
        return pltpu.make_async_copy(src, vf.at[at, lanes(side)], ld.at[side, c])

    def start_loads(t):
        mine = owner_dist(t) == 0
        p = pair_of(t)

        def one(c, r0, n):
            at = pl.ds(r0, n)

            @pl.when(mine)
            def _():
                load(t, c, q, panel(t, r0, n, True), at).start()

            @pl.when(jnp.logical_not(mine))
            def _():
                load(t, c, q, panel(t, r0, n, False), at).start()

            here = panel(t, r0, n, False)
            core_copy(here, here, t, c).wait_recv()
            load(t, c, 1 - q, vb.at[1 - q, p, at, :], at).start()

        at = head_rows(t)

        @pl.when(jnp.logical_not(mine))
        def _():
            load(t, nsb, q, vb.at[q, p, at, :], at).start()

        here = panel(t, head_row(t), NB, False)
        core_copy(here, here, t, nsb).wait_recv()
        load(t, nsb, 1 - q, vb.at[1 - q, p, at, :], at).start()
        small(t, 1, one)
        full(t, one)

    def pieces(slot, at, x):
        for i, piece in enumerate(split3(x)):
            vn[slot, at, i * PW : (i + 1) * PW] = piece

    def prep(t):
        slot = t % 3
        mine = owner_dist(t) == 0
        at = head_rows(t)
        l = sb_of(t)

        load(t, nsb, 1 - q, vb.at[0, 0, at, :], at).wait()

        @pl.when((r == 0) & (q == 0) & (t >= 3))
        def _():
            factor_across(t - 3).wait_send()

        @pl.when(mine)
        def _():
            vf[at, lanes(q)] = eb[l]

        @pl.when(jnp.logical_not(mine))
        def _():
            load(t, nsb, q, vb.at[0, 0, at, :], at).wait()

        def above(j, _):
            pieces(slot, pl.ds(pl.multiple_of(l * CH + j * NB, NB), NB), jnp.zeros((NB, PW), F32))
            return 0

        lax.fori_loop(0, chip_of(t), above, 0)

        i0 = lax.broadcasted_iota(jnp.int32, (NB, NB), 0)
        i1 = lax.broadcasted_iota(jnp.int32, (NB, NB), 1)
        one = jnp.where(i0 == i1, 1.0, 0.0).astype(F32)
        x0 = vf[at, 0:NB]
        x1 = vf[at, NB:PW]
        first = r == 0
        v0 = jnp.where(first, jnp.where(i0 > i1, x0, one), x0)
        v1 = jnp.where(first, 0.0, jnp.where(i0 > i1, x1, one))
        tc[slot, 0] = jnp.where(i0 > i1, 0.0, x0)
        tc[slot, 1] = jnp.where(i0 > i1, 0.0, x1)
        pieces(slot, at, jnp.concatenate([v0, v1], axis=1))

        @pl.when(first & (q == 0))
        def _():
            factor_across(t).start()

        def chunk(c, r0, n):
            a = pl.ds(r0, n)
            for side in range(2):
                load(t, c, side, vb.at[0, 0, a, :], a).wait()
            for j in range(0, n, NB):
                b = pl.ds(pl.multiple_of(r0 + j, NB), NB)
                pieces(slot, b, vf[b, :])

        small(t, 1, chunk)
        full(t, chunk)

    def factor_across(t):
        return rcopy(tc.at[t % 3, 0], tb.at[t % 8], t_snd.at[0, t % 8], t_rcv.at[0, t % 8], across)

    def factor_over(t):
        return rcopy(tb.at[t % 8], tb.at[t % 8], t_snd.at[1, t % 8], t_rcv.at[1, t % 8], partner)

    def share_factor(t):
        @pl.when((r == 1) & (q == 0))
        def _():
            factor_across(t).wait_recv()

            @pl.when(t >= 2)
            def _():
                factor_over(t - 2).wait_send()

            factor_over(t).start()

    def late(t):
        return t > AHEAD + 1

    def part_copy(t):
        return rcopy(gs.at[t % 2], gp.at[t % 2], p_snd.at[t % 2], p_rcv.at[t % 2], partner)

    def plane_copy(t):
        return rcopy(gz.at[t % 2], gr.at[t % 2], g_snd.at[t % 2], g_rcv.at[t % 2], across)

    def total_copy(t):
        return rcopy(gf.at[t % 8], gf.at[t % 8], f_snd.at[t % 8], f_rcv.at[t % 8], partner)

    def gram_part(t):
        slot = t % 3
        s = t % 2

        @pl.when(t >= 2)
        def _():
            part_copy(t - 2).wait_send()

        gs[s] = jnp.zeros((NB, NB), F32)
        first = (height(t) + t % 2) // 2
        lo = sb_of(t) + q * first
        cnt = jnp.where(q == 0, first, height(t) - first)

        def block(c, n):
            at = pl.ds(pl.multiple_of(c * CH, CH), n * CH)
            a = [vn[slot, at, i * PW : i * PW + NB].T for i in range(3)]
            b = [vn[slot, at, i * PW + NB : (i + 1) * PW] for i in range(3)]
            x = mm(jnp.concatenate(a, axis=0), jnp.concatenate(b[0:2], axis=1))
            gs[s] += add_rows(add_rows(mm(a[0], b[2]), x[:, 0:NB], NB), x[0 : 2 * NB, NB:PW], NB)

        if nsb >= 8:

            @pl.when(cnt >= 4)
            def _():
                block(lo, 4)

        if nsb >= 3:

            @pl.when(cnt % 4 >= 2)
            def _():
                block(lo + cnt // 4 * 4, 2)

        @pl.when(cnt % 2 == 1)
        def _():
            block(lo + cnt - 1, 1)

        part_copy(t).start()

    def sends_plane(t):
        return late(t) | (t % 2 == q)

    def gram_plane(t):
        s = t % 2
        part_copy(t).wait_recv()

        @pl.when((t >= 2) & sends_plane(t - 2))
        def _():
            plane_copy(t - 2).wait_send()

        gz[s] = gs[s] + gp[s]

        @pl.when(sends_plane(t))
        def _():
            plane_copy(t).start()

    def gram_total(t):
        s = t % 2

        @pl.when(sends_plane(t))
        def _():
            plane_copy(t).wait_recv()

            @pl.when((t >= 8) & (t % 2 == q) & jnp.logical_not(late(t - 8)))
            def _():
                total_copy(t - 8).wait_send()

            gf[t % 8] = gz[s] + gr[s]

            @pl.when(jnp.logical_not(late(t)))
            def _():
                total_copy(t).start()

    def block_factor(t):
        slot = t % 3

        @pl.when(jnp.logical_not(sends_plane(t)))
        def _():
            total_copy(t).wait_recv()

        @pl.when((r == 1) & (q == 1))
        def _():
            factor_over(t).wait_recv()

        g = gf[t % 8]
        ta = jnp.where(r == 0, tc[slot, 0], tb[t % 8])
        tbb = tc[slot, 1]
        upper = -full_dot(ta, full_dot(g, tbb))
        for i, piece in enumerate(split3(ta)):
            tp[0:NB, i * PW : i * PW + NB] = piece
        for i, piece in enumerate(split3(upper)):
            tp[0:NB, i * PW + NB : (i + 1) * PW] = piece
        for i, piece in enumerate(split3(tbb)):
            tp[NB:PW, i * PW : i * PW + NB] = jnp.zeros((NB, NB), BF16)
            tp[NB:PW, i * PW + NB : (i + 1) * PW] = piece

    def w_copy(t, g):
        return rcopy(ws.at[t % 2, g], wr.at[t % 2, g], w_snd.at[t % 2, g], w_rcv.at[t % 2, g], across)

    def coefficients(t, g):
        with jax.named_scope("wwait"):
            w_copy(t, g).wait_recv()
        w = ws[t % 2, g] + wr[t % 2, g]
        y = stacked(mm_nt, jnp.concatenate(split3(w), axis=0), [tp[:, i * PW : (i + 1) * PW] for i in range(3)])
        for i, piece in enumerate(split3(y)):
            yp[i * NB : (i + 1) * NB] = piece

    def piece_of(t, i, at):
        return vn[t % 3, at, i * PW : (i + 1) * PW]

    def chunk_at(c):
        return pl.ds(pl.multiple_of(c * CH, CH), CH)

    def passes(m, i, g, n, finish):
        units = m * CH // UNIT
        base = rows - m * CH
        w = None
        for c in range(units + (0 if n is None else LAG)):
            at = pl.ds(base + c * UNIT, UNIT)
            an = pl.ds(max(0, base + (c - LAG) * UNIT), UNIT)
            u = None
            for j in range(3):
                k3 = (3 - j) * NB
                if n is not None and c >= LAG:
                    w = add_rows(w, mm(xp[g, 0:k3, an], piece_of(n, j, an)), NB)
                if c < units:
                    u = add_rows(u, mm_nt(yp[0:k3], piece_of(i, j, at)), NB)
            if c < units:
                finish(at, xt[g, :, at] - u)
        if n is not None:
            ws[n % 2, g] += w

    def product(n, g, at):
        w = None
        for j in range(3):
            w = add_rows(w, mm(xp[g, 0 : (3 - j) * NB, at], piece_of(n, j, at)), NB)
        ws[n % 2, g] += w

    def both(i, g):
        n = i + 1

        @pl.when(sb_of(n) < sb_of(i))
        def _():
            product(n, g, chunk_at(sb_of(n)))

        for m in range(1, nsb + 1):

            @pl.when(height(i) == m)
            def _(m=m):
                passes(m, i, g, n, lambda at, x: put_x(g, x, at))

    def out_copy(g, c):
        return pltpu.make_async_copy(zl.at[g, chunk_at(c), :], out_ref.at[chunk_at(c), lanes(g)], o_sem.at[g, c])

    def last(i, g):
        def finish(at, x):
            zl[g, at, :] = x.T

        passes(nsb, i, g, None, finish)

        def out(c, _):
            out_copy(g, c).start()
            return 0

        lax.fori_loop(0, nsb, out, 0)

    def step(i, _):
        n = i + 1
        early = i < AHEAD
        b = jnp.where(early, i + 2, n)
        brings = (i != AHEAD) & (b < npair)

        @pl.when(i < npair - 1)
        def _():
            with jax.named_scope("svc"):
                service(i)

        @pl.when(brings)
        def _():
            with jax.named_scope("loads"):
                start_loads(b)

        @pl.when(i >= 0)
        def _():
            with jax.named_scope("bfac"):
                block_factor(i)

        @pl.when(n == npair)
        def _():
            lax.fori_loop(max(0, npair - SLOTS), npair, lambda t, _: (all_sent(t), 0)[1], 0)

        @pl.when((n >= 0) & (n < npair) & (n % RING == 0))
        def _():
            with jax.named_scope("admit"):
                admit(sb_of(n))

        def group(g, _):
            @pl.when((g == jnp.where(early, 1, 0)) & brings)
            def _():
                with jax.named_scope("prep"):
                    prep(b)
                with jax.named_scope("gram"):
                    gram_part(b)

            @pl.when(i >= 0)
            def _():
                with jax.named_scope("coef"):
                    coefficients(i, g)

            @pl.when((n >= 0) & (n < npair))
            def _():
                @pl.when(n >= 2)
                def _():
                    w_copy(n - 2, g).wait_send()

                ws[n % 2, g] = jnp.zeros((NB, PW), F32)

            @pl.when(i == -1)
            def _():
                product(n, g, chunk_at(nsb - 1))

            @pl.when((i >= 0) & (n < npair))
            def _():
                with jax.named_scope("both"):
                    both(i, g)

            @pl.when((g == jnp.where(early, 1, 0)) & brings)
            def _():
                with jax.named_scope("gplane"):
                    gram_plane(b)

            @pl.when((n >= 0) & (n < npair))
            def _():
                w_copy(n, g).start()

                @pl.when(g == jnp.where(i <= AHEAD, 0, 1))
                def _():
                    with jax.named_scope("fshare"):
                        share_factor(n)
                    with jax.named_scope("gtot"):
                        gram_total(n)

            @pl.when(n == npair)
            def _():
                with jax.named_scope("last"):
                    last(i, g)

            return 0

        lax.fori_loop(0, 2, group, 0)

        @pl.when((n >= RING + 1) & (n + RING + 1 < npair))
        def _():
            z_piece(n + RING + 1).start()

        @pl.when((n >= 0) & (n % RING == 2) & (n + RING < npair))
        def _():
            z_local(sb_of(n) - 1).start()

        return 0

    barrier = pltpu.get_barrier_semaphore()
    for dev in (at_ring(rho + 1), at_ring(rho + RING - 1), partner, across):
        pl.semaphore_signal(barrier, inc=1, device_id=dev, device_id_type=MESH_ID)
    pl.semaphore_wait(barrier, 4)

    for j in range(min(2 * RING + 2, npair)):
        z_piece(j).start()
    z_local(nsb - 1).start()
    with jax.named_scope("heads"):
        make_heads()
    lax.fori_loop(-2, npair, step, 0)

    for t in (npair - 2, npair - 1):
        for g in range(2):
            w_copy(t, g).wait_send()
    for t in (npair - 2, npair - 1):
        part_copy(t).wait_send()

        @pl.when(sends_plane(t))
        def _(t=t):
            plane_copy(t).wait_send()

    newest = min(npair - 1, AHEAD + 1)
    for t in range(max(0, npair - 8), newest + 1):

        @pl.when(t % 2 == q)
        def _(t=t):
            total_copy(t).wait_send()

    for t in range(npair - 3, npair):

        @pl.when((r == 0) & (q == 0))
        def _(t=t):
            factor_across(t).wait_send()

    for t in range(npair - 2, npair):

        @pl.when((r == 1) & (q == 0))
        def _(t=t):
            factor_over(t).wait_send()

    def out_done(c, _):
        for g in range(2):
            out_copy(g, c).wait()
        return 0

    lax.fori_loop(0, nsb, out_done, 0)


def solution(mesh):
    def local(v, t, z):
        rows, cols = v.shape
        nsb = cols // NB
        npair = nsb * RING
        hbm = pl.BlockSpec(memory_space=pltpu.MemorySpace.HBM)
        out, _ = pl.pallas_call(
            functools.partial(body, nsb),
            out_shape=(
                jax.ShapeDtypeStruct((rows, PW), F32),
                jax.ShapeDtypeStruct((2, npair, rows, NB), F32),
            ),
            in_specs=[hbm] * 3,
            out_specs=(hbm, hbm),
            scratch_shapes=[
                pltpu.VMEM((2, rows, NB), F32),
                pltpu.VMEM((2, NB, rows), F32),
                pltpu.VMEM((2, 3 * NB, rows), BF16),
                pltpu.VMEM((rows, PW), F32),
                pltpu.VMEM((3, rows, 3 * PW), BF16),
                pltpu.VMEM((8, NB, NB), F32),
                pltpu.VMEM((3, 2, NB, NB), F32),
                pltpu.VMEM((PW, 3 * PW), BF16),
                pltpu.VMEM((2, 2, NB, PW), F32),
                pltpu.VMEM((2, 2, NB, PW), F32),
                pltpu.VMEM((2, NB, NB), F32),
                pltpu.VMEM((2, NB, NB), F32),
                pltpu.VMEM((2, NB, NB), F32),
                pltpu.VMEM((2, NB, NB), F32),
                pltpu.VMEM((8, NB, NB), F32),
                pltpu.VMEM((3 * NB, PW), BF16),
                pltpu.VMEM((nsb, NB, NB), F32),
                pltpu.VMEM((nsb, NB, NB), F32),
            ],
            compiler_params=pltpu.CompilerParams(
                collective_id=0, has_side_effects=True, vmem_limit_bytes=60 * 2**20),
            name="backtransform",
        )(v, t, z)
        return out

    return jax.shard_map(local, mesh=mesh,
                         in_specs=(P("row", "col"), P("col", None, None), P(None, ("col", "row"))),
                         out_specs=P("row", "col"), check_vma=False)
```

```python
import functools

import jax
import jax.numpy as jnp
from jax import lax
from jax.experimental import pallas as pl
from jax.experimental.pallas import tpu as pltpu
from jax.sharding import PartitionSpec as P

F32 = jnp.float32
BF16 = jnp.bfloat16
MESH_ID = pl.DeviceIdType.MESH

NB = 128
PW = 2 * NB
CH = 4 * NB
UNIT = PW
LAG = 2
RING = 4
SLOTS = 8
AHEAD = 20


def div(a, b):
    return lax.div(a, b)


def rem(a, b):
    return lax.rem(a, b)


def split3(x):
    hi = x.astype(BF16)
    rest = x - hi.astype(F32)
    mid = rest.astype(BF16)
    low = (rest - mid.astype(F32)).astype(BF16)
    return hi, mid, low


def mm(a, b):
    return lax.dot_general(a, b, (((1,), (0,)), ((), ())), preferred_element_type=F32)


def mm_nt(a, b):
    return lax.dot_general(a, b, (((1,), (1,)), ((), ())), preferred_element_type=F32)


def add_rows(total, x, n):
    for i in range(0, x.shape[0], n):
        part = x[i : i + n]
        total = part if total is None else total + part
    return total


def stacked(dot, a3, b):
    m = a3.shape[0] // 3
    s = None
    for i in range(3):
        s = add_rows(s, dot(a3[0 : (3 - i) * m], b[i]), m)
    return s


def full_dot(a, b):
    ah, am, al = split3(a)
    bh, bm, bl = split3(b)
    n = a.shape[0]
    x = mm(jnp.concatenate([ah, am], axis=1), jnp.concatenate([jnp.concatenate([bh, bm], axis=1)] * 2, axis=0))
    y = mm(jnp.concatenate([al, ah], axis=1), jnp.concatenate([bh, bl], axis=0))
    return x[:, 0:n] + x[:, n:] + y


def body(nsb, v_ref, t_ref, z_ref, out_ref, vb, *scratch):
    rows = nsb * CH
    dma = pltpu.SemaphoreType.DMA
    npair = nsb * RING
    nc = nsb + RING
    pl.run_scoped(
        functools.partial(run, nsb, rows, npair, v_ref, t_ref, z_ref, out_ref, vb, scratch),
        dma((nsb,)),
        dma((npair,)),
        dma((npair,)),
        dma((npair, nc)),
        dma((npair, nc)),
        dma((2, 2)),
        dma((2, 2)),
        dma((2,)),
        dma((2,)),
        dma((8,)),
        dma((8,)),
        dma((2, nc)),
        dma((2, nsb)),
        dma((2, SLOTS, nc)),
        dma((SLOTS, nc)),
        dma((2, nsb)),
        dma((2,)),
        dma((2,)),
        dma((2, 8)),
        dma((2, 8)),
    )


def run(nsb, rows, npair, v_ref, t_ref, z_ref, out_ref, vb, scratch, *sems):
    (zl, xt, xp, vf, vn, tb, tc, tp, ws, wr, gs, gp, gz, gr, gf, yp, eb, et) = scratch
    (z_loc, z_snd, z_rcv, i_rcv, d_rcv, w_snd, w_rcv, g_snd, g_rcv, f_snd, f_rcv, ld, o_sem, i_snd, d_snd, h_sem, p_snd, p_rcv, t_snd, t_rcv) = sems
    r = lax.axis_index("row")
    col = lax.axis_index("col")
    q = rem(col, 2)
    k = div(col, 2)
    ky, kx = div(k, 2), rem(k, 2)
    rho = 2 * ky + rem(kx + ky, 2)

    def at_ring(i):
        i = rem(i, RING)
        y = div(i, 2)
        x = rem(rem(i, 2) + y, 2)
        return (r, (y * 2 + x) * 2 + q)

    cw, ccw = at_ring(rho + 1), at_ring(rho + RING - 1)

    def side_of(d):
        return (r, jnp.where(d == 0, cw[1], ccw[1]))

    partner = (r, k * 2 + 1 - q)
    across = (1 - r, col)

    def pair_of(t):
        return npair - 1 - t

    def sb_of(t):
        return div(pair_of(t), RING)

    def chip_of(t):
        return rem(pair_of(t), RING)

    def owner_dist(t):
        kk = chip_of(t)
        y = div(kk, 2)
        ro = 2 * y + rem(rem(kk, 2) + y, 2)
        return rem(rho - ro + RING, RING)

    def height(t):
        return nsb - sb_of(t)

    def small_half(t):
        return rem(div(height(t) - 1, 2), 2)

    def small(t, first, fn):
        def one(j, _):
            fn(nsb + j, pl.multiple_of((pair_of(t) + j) * NB, NB), NB)
            return 0

        lax.fori_loop(first, RING - chip_of(t), one, 0)

    def full(t, fn):
        def one(c, _):
            fn(c, pl.multiple_of(c * CH, CH), CH)
            return 0

        lax.fori_loop(sb_of(t) + 1, nsb, one, 0)

    def in_half(t, half, fn):
        @pl.when(small_half(t) == half)
        def _():
            small(t, 0, fn)

        full_half(t, half, fn, 0, nsb)

    def count_half(t, half):
        first = 2 - rem(half + div(height(t) - 1, 2), 2)
        return div(height(t) - first + 1, 2), sb_of(t) + first

    def full_half(t, half, fn, lo, hi):
        cnt, first = count_half(t, half)

        def one(j, _):
            c = first + 2 * j
            fn(c, pl.multiple_of(c * CH, CH), CH)
            return 0

        lax.fori_loop(lo, jnp.minimum(cnt, hi), one, 0)

    def head_row(t):
        return pl.multiple_of(pair_of(t) * NB, NB)

    def head_rows(t):
        return pl.ds(pl.multiple_of(pair_of(t) * NB, NB), NB)

    def lanes(l):
        return pl.ds(pl.multiple_of(l * NB, NB), NB)

    def rcopy(src, dst, ssem, rsem, dev):
        return pltpu.make_async_remote_copy(src, dst, ssem, rsem, device_id=dev, device_id_type=MESH_ID)

    def panel(t, r0, n, own):
        if own:
            return v_ref.at[pl.ds(r0, n), lanes(sb_of(t))]
        return vb.at[q, pair_of(t), pl.ds(r0, n), :]

    def side_copy(src, dst, t, c, d):
        return rcopy(src, dst, i_snd.at[d, rem(t, SLOTS), c], i_rcv.at[t, c], side_of(d))

    def core_copy(src, dst, t, c):
        return rcopy(src, dst, d_snd.at[rem(t, SLOTS), c], d_rcv.at[t, c], partner)

    def all_sent(t):
        d = owner_dist(t)

        def over(c, r0, n):
            here = panel(t, r0, n, False)
            core_copy(here, here, t, c).wait_send()

        small(t, 0, over)
        full(t, over)

        def by_side(x):
            def fn(c, r0, n):
                here = panel(t, r0, n, False)
                side_copy(here, here, t, c, x).wait_send()

            return fn

        @pl.when(d == 0)
        def _():
            for x in range(2):
                small(t, 0, by_side(x))
                full(t, by_side(x))

        @pl.when(rem(d, 2) == 1)
        def _():
            half = jnp.where(d == 1, 0, 1)
            in_half(t, half, by_side(half))

    def free_slot(t):
        @pl.when(t >= SLOTS)
        def _():
            all_sent(t - SLOTS)

    def send_own(u):
        first = RING - 1 - k
        part = rem(u - first + 2 * RING, RING)
        t = u - part

        @pl.when((t >= 0) & (t < npair))
        def _():
            @pl.when(part == 0)
            def _():
                free_slot(t)

                def over(c, r0, n):
                    core_copy(panel(t, r0, n, True), panel(t, r0, n, False), t, c).start()

                core_copy(eb.at[sb_of(t)], panel(t, head_row(t), NB, False), t, nsb).start()
                small(t, 1, over)
                full(t, over)

            def side(d, _):
                half = rem(d + div(part, 2), 2)

                def send(src, dst, c):
                    side_copy(src, dst, t, c, d).start()

                def out(c, r0, n):
                    send(panel(t, r0, n, True), panel(t, r0, n, False), c)

                cnt, _ = count_half(t, half)
                mid = div(cnt + 1, 2)
                begins = rem(part, 2) == 0

                @pl.when(begins & (small_half(t) == half))
                def _():
                    send(eb.at[sb_of(t)], panel(t, head_row(t), NB, False), nsb)
                    small(t, 1, out)

                full_half(t, half, out, jnp.where(begins, 0, mid), jnp.where(begins, mid, cnt))
                return 0

            lax.fori_loop(0, 2, side, 0)

    def pass_on(t, half, forward):
        def got(send):
            def fn(c, r0, n):
                here = panel(t, r0, n, False)
                side_copy(here, here, t, c, half).wait_recv()
                core_copy(here, here, t, c).start()
                if send:
                    side_copy(here, here, t, c, half).start()

            return fn

        @pl.when(forward)
        def _():
            in_half(t, half, got(True))

        @pl.when(jnp.logical_not(forward))
        def _():
            in_half(t, half, got(False))

    def brought(i):
        return jnp.minimum(npair - 1, jnp.minimum(i + 2, jnp.maximum(AHEAD + 1, i + 1)))

    def falling(i, high, low, i0, i1):
        return high - jnp.clip(((high - low) * (i - i0) + i1 - i0 - 1) // (i1 - i0), 0, high - low)

    def hand_lead(i):
        return jnp.minimum(npair - 1, brought(i) + jnp.minimum(falling(i, 5, 3, 15, 26), i + 3))

    def rest_lead(i):
        return jnp.minimum(npair - 1, brought(i) + jnp.where(i < 27, jnp.minimum(1, i + 3), 0))

    def far_lead(i):
        return jnp.minimum(npair - 1, brought(i) + jnp.where((i >= 4) & (i < 15), 1, 0))

    def own_lead(i):
        return jnp.minimum(npair + RING - 2, brought(i) + jnp.minimum(falling(i, 10, 6, 13, 28), 4 + 3 * (i + 2)))

    def span(lead, i):
        return jnp.where(i < -1, 0, lead(i - 1) + 1), lead(i) + 1

    def service(i):
        def one(j, _):
            kind = jnp.where(i < -1, j, 3 - j)

            @pl.when(kind == 0)
            def _():
                lo, hi = span(own_lead, i)
                lax.fori_loop(lo, hi, lambda u, _: (send_own(u), 0)[1], 0)

            @pl.when(kind > 0)
            def _():
                h = span(hand_lead, i)
                e = span(rest_lead, i)
                f = span(far_lead, i)
                lo, hi = (jnp.where(kind == 1, x, jnp.where(kind == 2, y, z)) for x, y, z in zip(h, e, f))

                def take(x, _):
                    t = lo + div(x, 2)
                    d = owner_dist(t)
                    half = rem(x, 2)
                    mine = jnp.where(d == 1, 0, 1)
                    afar = (kind == 3) & (d == 2)
                    hand = (kind == 1) & (rem(d, 2) == 1) & (half == mine)
                    rest = (kind == 2) & (rem(d, 2) == 1) & (half != mine)

                    @pl.when(hand | (afar & (half == 0)))
                    def _():
                        free_slot(t)

                    @pl.when(afar | hand | rest)
                    def _():
                        pass_on(t, half, hand)

                    return 0

                lax.fori_loop(0, 2 * jnp.maximum(hi - lo, 0), take, 0)

            return 0

        lax.fori_loop(0, 4, one, 0)

    def make_heads():
        def copies(l):
            rr = pl.ds(pl.multiple_of((l * RING + k) * NB, NB), NB)
            return (pltpu.make_async_copy(v_ref.at[rr, lanes(l)], eb.at[l], h_sem.at[0, l]),
                    pltpu.make_async_copy(t_ref.at[l], et.at[l], h_sem.at[1, l]))

        def begin(l, _):
            for c in copies(l):
                c.start()
            return 0

        lax.fori_loop(0, nsb, begin, 0)

        def one(l, _):
            for c in copies(l):
                c.wait()
            x = eb[l]
            tt = et[l]
            below = lax.broadcasted_iota(jnp.int32, (NB, NB), 0) > lax.broadcasted_iota(jnp.int32, (NB, NB), 1)
            both_in = jnp.where(below, x, tt)
            eb[l] = jnp.where(r == q, both_in, jnp.where(r == 0, tt, x))
            return 0

        lax.fori_loop(0, nsb, one, 0)

    def z_local(c):
        mine = pl.multiple_of(r * rows + c * CH, CH)
        return pltpu.make_async_copy(z_ref.at[pl.ds(mine, CH), :], zl.at[r, chunk_at(c), :], z_loc.at[c])

    def z_piece(w):
        c = nsb - 1 - w // RING
        r0 = c * CH + w % RING * NB
        theirs = pl.multiple_of((1 - r) * rows + r0, NB)
        return rcopy(z_ref.at[pl.ds(theirs, NB), :], zl.at[r, pl.ds(pl.multiple_of(r0, NB), NB), :],
                     z_snd.at[w], z_rcv.at[w], across)

    def put_x(g, x, at):
        xt[g, :, at] = x
        for i, piece in enumerate(split3(x)):
            xp[g, i * NB : (i + 1) * NB, at] = piece

    def admit(c):
        for j in range(RING):
            z_piece((nsb - 1 - c) * RING + j).wait()
        z_local(c).wait()

        def one(g, _):
            put_x(g, zl[g, chunk_at(c), :].T, chunk_at(c))
            return 0

        lax.fori_loop(0, 2, one, 0)

    def load(t, c, side, src, at):
        return pltpu.make_async_copy(src, vf.at[at, lanes(side)], ld.at[side, c])

    def start_loads(t):
        mine = owner_dist(t) == 0
        p = pair_of(t)

        def one(c, r0, n):
            at = pl.ds(r0, n)

            @pl.when(mine)
            def _():
                load(t, c, q, panel(t, r0, n, True), at).start()

            @pl.when(jnp.logical_not(mine))
            def _():
                load(t, c, q, panel(t, r0, n, False), at).start()

            here = panel(t, r0, n, False)
            core_copy(here, here, t, c).wait_recv()
            load(t, c, 1 - q, vb.at[1 - q, p, at, :], at).start()

        at = head_rows(t)

        @pl.when(jnp.logical_not(mine))
        def _():
            load(t, nsb, q, vb.at[q, p, at, :], at).start()

        here = panel(t, head_row(t), NB, False)
        core_copy(here, here, t, nsb).wait_recv()
        load(t, nsb, 1 - q, vb.at[1 - q, p, at, :], at).start()
        small(t, 1, one)
        full(t, one)

    def pieces(slot, at, x):
        for i, piece in enumerate(split3(x)):
            vn[slot, at, i * PW : (i + 1) * PW] = piece

    def prep(t):
        slot = t % 3
        mine = owner_dist(t) == 0
        at = head_rows(t)
        l = sb_of(t)

        load(t, nsb, 1 - q, vb.at[0, 0, at, :], at).wait()

        @pl.when((r == 0) & (q == 0) & (t >= 3))
        def _():
            factor_across(t - 3).wait_send()

        @pl.when(mine)
        def _():
            vf[at, lanes(q)] = eb[l]

        @pl.when(jnp.logical_not(mine))
        def _():
            load(t, nsb, q, vb.at[0, 0, at, :], at).wait()

        def above(j, _):
            pieces(slot, pl.ds(pl.multiple_of(l * CH + j * NB, NB), NB), jnp.zeros((NB, PW), F32))
            return 0

        lax.fori_loop(0, chip_of(t), above, 0)

        i0 = lax.broadcasted_iota(jnp.int32, (NB, NB), 0)
        i1 = lax.broadcasted_iota(jnp.int32, (NB, NB), 1)
        one = jnp.where(i0 == i1, 1.0, 0.0).astype(F32)
        x0 = vf[at, 0:NB]
        x1 = vf[at, NB:PW]
        first = r == 0
        v0 = jnp.where(first, jnp.where(i0 > i1, x0, one), x0)
        v1 = jnp.where(first, 0.0, jnp.where(i0 > i1, x1, one))
        tc[slot, 0] = jnp.where(i0 > i1, 0.0, x0)
        tc[slot, 1] = jnp.where(i0 > i1, 0.0, x1)
        pieces(slot, at, jnp.concatenate([v0, v1], axis=1))

        @pl.when(first & (q == 0))
        def _():
            factor_across(t).start()

        def chunk(c, r0, n):
            a = pl.ds(r0, n)
            for side in range(2):
                load(t, c, side, vb.at[0, 0, a, :], a).wait()
            for j in range(0, n, NB):
                b = pl.ds(pl.multiple_of(r0 + j, NB), NB)
                pieces(slot, b, vf[b, :])

        small(t, 1, chunk)
        full(t, chunk)

    def factor_across(t):
        return rcopy(tc.at[t % 3, 0], tb.at[t % 8], t_snd.at[0, t % 8], t_rcv.at[0, t % 8], across)

    def factor_over(t):
        return rcopy(tb.at[t % 8], tb.at[t % 8], t_snd.at[1, t % 8], t_rcv.at[1, t % 8], partner)

    def share_factor(t):
        @pl.when((r == 1) & (q == 0))
        def _():
            factor_across(t).wait_recv()

            @pl.when(t >= 2)
            def _():
                factor_over(t - 2).wait_send()

            factor_over(t).start()

    def late(t):
        return t > AHEAD + 1

    def part_copy(t):
        return rcopy(gs.at[t % 2], gp.at[t % 2], p_snd.at[t % 2], p_rcv.at[t % 2], partner)

    def plane_copy(t):
        return rcopy(gz.at[t % 2], gr.at[t % 2], g_snd.at[t % 2], g_rcv.at[t % 2], across)

    def total_copy(t):
        return rcopy(gf.at[t % 8], gf.at[t % 8], f_snd.at[t % 8], f_rcv.at[t % 8], partner)

    def gram_part(t):
        slot = t % 3
        s = t % 2

        @pl.when(t >= 2)
        def _():
            part_copy(t - 2).wait_send()

        gs[s] = jnp.zeros((NB, NB), F32)
        first = (height(t) + t % 2) // 2
        lo = sb_of(t) + q * first
        cnt = jnp.where(q == 0, first, height(t) - first)

        def block(c, n):
            at = pl.ds(pl.multiple_of(c * CH, CH), n * CH)
            a = [vn[slot, at, i * PW : i * PW + NB].T for i in range(3)]
            b = [vn[slot, at, i * PW + NB : (i + 1) * PW] for i in range(3)]
            x = mm(jnp.concatenate(a, axis=0), jnp.concatenate(b[0:2], axis=1))
            gs[s] += add_rows(add_rows(mm(a[0], b[2]), x[:, 0:NB], NB), x[0 : 2 * NB, NB:PW], NB)

        if nsb >= 8:

            @pl.when(cnt >= 4)
            def _():
                block(lo, 4)

        if nsb >= 3:

            @pl.when(cnt % 4 >= 2)
            def _():
                block(lo + cnt // 4 * 4, 2)

        @pl.when(cnt % 2 == 1)
        def _():
            block(lo + cnt - 1, 1)

        part_copy(t).start()

    def sends_plane(t):
        return late(t) | (t % 2 == q)

    def gram_plane(t):
        s = t % 2
        part_copy(t).wait_recv()

        @pl.when((t >= 2) & sends_plane(t - 2))
        def _():
            plane_copy(t - 2).wait_send()

        gz[s] = gs[s] + gp[s]

        @pl.when(sends_plane(t))
        def _():
            plane_copy(t).start()

    def gram_total(t):
        s = t % 2

        @pl.when(sends_plane(t))
        def _():
            plane_copy(t).wait_recv()

            @pl.when((t >= 8) & (t % 2 == q) & jnp.logical_not(late(t - 8)))
            def _():
                total_copy(t - 8).wait_send()

            gf[t % 8] = gz[s] + gr[s]

            @pl.when(jnp.logical_not(late(t)))
            def _():
                total_copy(t).start()

    def block_factor(t):
        slot = t % 3

        @pl.when(jnp.logical_not(sends_plane(t)))
        def _():
            total_copy(t).wait_recv()

        @pl.when((r == 1) & (q == 1))
        def _():
            factor_over(t).wait_recv()

        g = gf[t % 8]
        ta = jnp.where(r == 0, tc[slot, 0], tb[t % 8])
        tbb = tc[slot, 1]
        upper = -full_dot(ta, full_dot(g, tbb))
        for i, piece in enumerate(split3(ta)):
            tp[0:NB, i * PW : i * PW + NB] = piece
        for i, piece in enumerate(split3(upper)):
            tp[0:NB, i * PW + NB : (i + 1) * PW] = piece
        for i, piece in enumerate(split3(tbb)):
            tp[NB:PW, i * PW : i * PW + NB] = jnp.zeros((NB, NB), BF16)
            tp[NB:PW, i * PW + NB : (i + 1) * PW] = piece

    def w_copy(t, g):
        return rcopy(ws.at[t % 2, g], wr.at[t % 2, g], w_snd.at[t % 2, g], w_rcv.at[t % 2, g], across)

    def coefficients(t, g):
        with jax.named_scope("wwait"):
            w_copy(t, g).wait_recv()
        w = ws[t % 2, g] + wr[t % 2, g]
        y = stacked(mm_nt, jnp.concatenate(split3(w), axis=0), [tp[:, i * PW : (i + 1) * PW] for i in range(3)])
        for i, piece in enumerate(split3(y)):
            yp[i * NB : (i + 1) * NB] = piece

    def piece_of(t, i, at):
        return vn[t % 3, at, i * PW : (i + 1) * PW]

    def chunk_at(c):
        return pl.ds(pl.multiple_of(c * CH, CH), CH)

    def passes(m, i, g, n, finish):
        units = m * CH // UNIT
        base = rows - m * CH
        w = None
        for c in range(units + (0 if n is None else LAG)):
            at = pl.ds(base + c * UNIT, UNIT)
            an = pl.ds(max(0, base + (c - LAG) * UNIT), UNIT)
            u = None
            for j in range(3):
                k3 = (3 - j) * NB
                if n is not None and c >= LAG:
                    w = add_rows(w, mm(xp[g, 0:k3, an], piece_of(n, j, an)), NB)
                if c < units:
                    u = add_rows(u, mm_nt(yp[0:k3], piece_of(i, j, at)), NB)
            if c < units:
                finish(at, xt[g, :, at] - u)
        if n is not None:
            ws[n % 2, g] += w

    def product(n, g, at):
        w = None
        for j in range(3):
            w = add_rows(w, mm(xp[g, 0 : (3 - j) * NB, at], piece_of(n, j, at)), NB)
        ws[n % 2, g] += w

    def both(i, g):
        n = i + 1

        @pl.when(sb_of(n) < sb_of(i))
        def _():
            product(n, g, chunk_at(sb_of(n)))

        for m in range(1, nsb + 1):

            @pl.when(height(i) == m)
            def _(m=m):
                passes(m, i, g, n, lambda at, x: put_x(g, x, at))

    def out_copy(g, c):
        return pltpu.make_async_copy(zl.at[g, chunk_at(c), :], out_ref.at[chunk_at(c), lanes(g)], o_sem.at[g, c])

    def last(i, g):
        def finish(at, x):
            zl[g, at, :] = x.T

        passes(nsb, i, g, None, finish)

        def out(c, _):
            out_copy(g, c).start()
            return 0

        lax.fori_loop(0, nsb, out, 0)

    def step(i, _):
        n = i + 1
        early = i < AHEAD
        b = jnp.where(early, i + 2, n)
        brings = (i != AHEAD) & (b < npair)

        @pl.when(i < npair - 1)
        def _():
            with jax.named_scope("svc"):
                service(i)

        @pl.when(brings)
        def _():
            with jax.named_scope("loads"):
                start_loads(b)

        @pl.when(i >= 0)
        def _():
            with jax.named_scope("bfac"):
                block_factor(i)

        @pl.when(n == npair)
        def _():
            lax.fori_loop(max(0, npair - SLOTS), npair, lambda t, _: (all_sent(t), 0)[1], 0)

        @pl.when((n >= 0) & (n < npair) & (n % RING == 0))
        def _():
            with jax.named_scope("admit"):
                admit(sb_of(n))

        def group(g, _):
            @pl.when((g == jnp.where(early, 1, 0)) & brings)
            def _():
                with jax.named_scope("prep"):
                    prep(b)
                with jax.named_scope("gram"):
                    gram_part(b)

            @pl.when(i >= 0)
            def _():
                with jax.named_scope("coef"):
                    coefficients(i, g)

            @pl.when((n >= 0) & (n < npair))
            def _():
                @pl.when(n >= 2)
                def _():
                    w_copy(n - 2, g).wait_send()

                ws[n % 2, g] = jnp.zeros((NB, PW), F32)

            @pl.when(i == -1)
            def _():
                product(n, g, chunk_at(nsb - 1))

            @pl.when((i >= 0) & (n < npair))
            def _():
                with jax.named_scope("both"):
                    both(i, g)

            @pl.when((g == jnp.where(early, 1, 0)) & brings)
            def _():
                with jax.named_scope("gplane"):
                    gram_plane(b)

            @pl.when((n >= 0) & (n < npair))
            def _():
                w_copy(n, g).start()

                @pl.when(g == jnp.where(i <= AHEAD, 0, 1))
                def _():
                    with jax.named_scope("fshare"):
                        share_factor(n)
                    with jax.named_scope("gtot"):
                        gram_total(n)

            @pl.when(n == npair)
            def _():
                with jax.named_scope("last"):
                    last(i, g)

            return 0

        lax.fori_loop(0, 2, group, 0)

        @pl.when((n >= RING + 1) & (n + RING + 1 < npair))
        def _():
            z_piece(n + RING + 1).start()

        @pl.when((n >= 0) & (n % RING == 2) & (n + RING < npair))
        def _():
            z_local(sb_of(n) - 1).start()

        return 0

    barrier = pltpu.get_barrier_semaphore()
    for dev in (at_ring(rho + 1), at_ring(rho + RING - 1), partner, across):
        pl.semaphore_signal(barrier, inc=1, device_id=dev, device_id_type=MESH_ID)
    pl.semaphore_wait(barrier, 4)

    for j in range(min(2 * RING + 2, npair)):
        z_piece(j).start()
    z_local(nsb - 1).start()
    with jax.named_scope("heads"):
        make_heads()
    lax.fori_loop(-2, npair, step, 0)

    for t in (npair - 2, npair - 1):
        for g in range(2):
            w_copy(t, g).wait_send()
    for t in (npair - 2, npair - 1):
        part_copy(t).wait_send()

        @pl.when(sends_plane(t))
        def _(t=t):
            plane_copy(t).wait_send()

    newest = min(npair - 1, AHEAD + 1)
    for t in range(max(0, npair - 8), newest + 1):

        @pl.when(t % 2 == q)
        def _(t=t):
            total_copy(t).wait_send()

    for t in range(npair - 3, npair):

        @pl.when((r == 0) & (q == 0))
        def _(t=t):
            factor_across(t).wait_send()

    for t in range(npair - 2, npair):

        @pl.when((r == 1) & (q == 0))
        def _(t=t):
            factor_over(t).wait_send()

    def out_done(c, _):
        for g in range(2):
            out_copy(g, c).wait()
        return 0

    lax.fori_loop(0, nsb, out_done, 0)


def solution(mesh):
    def local(v, t, z):
        rows, cols = v.shape
        nsb = cols // NB
        npair = nsb * RING
        hbm = pl.BlockSpec(memory_space=pltpu.MemorySpace.HBM)
        out, _ = pl.pallas_call(
            functools.partial(body, nsb),
            out_shape=(
                jax.ShapeDtypeStruct((rows, PW), F32),
                jax.ShapeDtypeStruct((2, npair, rows, NB), F32),
            ),
            in_specs=[hbm] * 3,
            out_specs=(hbm, hbm),
            scratch_shapes=[
                pltpu.VMEM((2, rows, NB), F32),
                pltpu.VMEM((2, NB, rows), F32),
                pltpu.VMEM((2, 3 * NB, rows), BF16),
                pltpu.VMEM((rows, PW), F32),
                pltpu.VMEM((3, rows, 3 * PW), BF16),
                pltpu.VMEM((8, NB, NB), F32),
                pltpu.VMEM((3, 2, NB, NB), F32),
                pltpu.VMEM((PW, 3 * PW), BF16),
                pltpu.VMEM((2, 2, NB, PW), F32),
                pltpu.VMEM((2, 2, NB, PW), F32),
                pltpu.VMEM((2, NB, NB), F32),
                pltpu.VMEM((2, NB, NB), F32),
                pltpu.VMEM((2, NB, NB), F32),
                pltpu.VMEM((2, NB, NB), F32),
                pltpu.VMEM((8, NB, NB), F32),
                pltpu.VMEM((3 * NB, PW), BF16),
                pltpu.VMEM((nsb, NB, NB), F32),
                pltpu.VMEM((nsb, NB, NB), F32),
            ],
            compiler_params=pltpu.CompilerParams(
                collective_id=0, has_side_effects=True, vmem_limit_bytes=60 * 2**20),
            name="backtransform",
        )(v, t, z)
        return out

    return jax.shard_map(local, mesh=mesh,
                         in_specs=(P("row", "col"), P("col", None, None), P(None, ("col", "row"))),
                         out_specs=P("row", "col"), check_vma=False)
```

```python
import functools

import jax
import jax.numpy as jnp
from jax import lax
from jax.experimental import pallas as pl
from jax.experimental.pallas import tpu as pltpu
from jax.sharding import PartitionSpec as P

F32 = jnp.float32
BF16 = jnp.bfloat16
MESH_ID = pl.DeviceIdType.MESH

NB = 128
PW = 2 * NB
CH = 4 * NB
UNIT = PW
LAG = 2
RING = 4
SLOTS = 8
AHEAD = 20


def div(a, b):
    return lax.div(a, b)


def rem(a, b):
    return lax.rem(a, b)


def split3(x):
    hi = x.astype(BF16)
    rest = x - hi.astype(F32)
    mid = rest.astype(BF16)
    low = (rest - mid.astype(F32)).astype(BF16)
    return hi, mid, low


def mm(a, b):
    return lax.dot_general(a, b, (((1,), (0,)), ((), ())), preferred_element_type=F32)


def mm_nt(a, b):
    return lax.dot_general(a, b, (((1,), (1,)), ((), ())), preferred_element_type=F32)


def add_rows(total, x, n):
    for i in range(0, x.shape[0], n):
        part = x[i : i + n]
        total = part if total is None else total + part
    return total


def stacked(dot, a3, b):
    m = a3.shape[0] // 3
    s = None
    for i in range(3):
        s = add_rows(s, dot(a3[0 : (3 - i) * m], b[i]), m)
    return s


def full_dot(a, b):
    ah, am, al = split3(a)
    bh, bm, bl = split3(b)
    n = a.shape[0]
    x = mm(jnp.concatenate([ah, am], axis=1), jnp.concatenate([jnp.concatenate([bh, bm], axis=1)] * 2, axis=0))
    y = mm(jnp.concatenate([al, ah], axis=1), jnp.concatenate([bh, bl], axis=0))
    return x[:, 0:n] + x[:, n:] + y


def body(nsb, v_ref, t_ref, z_ref, out_ref, vb, *scratch):
    rows = nsb * CH
    dma = pltpu.SemaphoreType.DMA
    npair = nsb * RING
    nc = nsb + RING
    pl.run_scoped(
        functools.partial(run, nsb, rows, npair, v_ref, t_ref, z_ref, out_ref, vb, scratch),
        dma((nsb,)),
        dma((npair,)),
        dma((npair,)),
        dma((npair, nc)),
        dma((npair, nc)),
        dma((2, 2)),
        dma((2, 2)),
        dma((2,)),
        dma((2,)),
        dma((8,)),
        dma((8,)),
        dma((2, nc)),
        dma((2, nsb)),
        dma((2, SLOTS, nc)),
        dma((SLOTS, nc)),
        dma((2, nsb)),
        dma((2,)),
        dma((2,)),
        dma((2, 8)),
        dma((2, 8)),
    )


def run(nsb, rows, npair, v_ref, t_ref, z_ref, out_ref, vb, scratch, *sems):
    (zl, xt, xp, vf, vn, tb, tc, tp, ws, wr, gs, gp, gz, gr, gf, yp, eb, et) = scratch
    (z_loc, z_snd, z_rcv, i_rcv, d_rcv, w_snd, w_rcv, g_snd, g_rcv, f_snd, f_rcv, ld, o_sem, i_snd, d_snd, h_sem, p_snd, p_rcv, t_snd, t_rcv) = sems
    r = lax.axis_index("row")
    col = lax.axis_index("col")
    q = rem(col, 2)
    k = div(col, 2)
    ky, kx = div(k, 2), rem(k, 2)
    rho = 2 * ky + rem(kx + ky, 2)

    def at_ring(i):
        i = rem(i, RING)
        y = div(i, 2)
        x = rem(rem(i, 2) + y, 2)
        return (r, (y * 2 + x) * 2 + q)

    cw, ccw = at_ring(rho + 1), at_ring(rho + RING - 1)

    def side_of(d):
        return (r, jnp.where(d == 0, cw[1], ccw[1]))

    partner = (r, k * 2 + 1 - q)
    across = (1 - r, col)

    def pair_of(t):
        return npair - 1 - t

    def sb_of(t):
        return div(pair_of(t), RING)

    def chip_of(t):
        return rem(pair_of(t), RING)

    def owner_dist(t):
        kk = chip_of(t)
        y = div(kk, 2)
        ro = 2 * y + rem(rem(kk, 2) + y, 2)
        return rem(rho - ro + RING, RING)

    def height(t):
        return nsb - sb_of(t)

    def small_half(t):
        return rem(div(height(t) - 1, 2), 2)

    def small(t, first, fn):
        def one(j, _):
            fn(nsb + j, pl.multiple_of((pair_of(t) + j) * NB, NB), NB)
            return 0

        lax.fori_loop(first, RING - chip_of(t), one, 0)

    def full(t, fn):
        def one(c, _):
            fn(c, pl.multiple_of(c * CH, CH), CH)
            return 0

        lax.fori_loop(sb_of(t) + 1, nsb, one, 0)

    def in_half(t, half, fn):
        @pl.when(small_half(t) == half)
        def _():
            small(t, 0, fn)

        full_half(t, half, fn, 0, nsb)

    def count_half(t, half):
        first = 2 - rem(half + div(height(t) - 1, 2), 2)
        return div(height(t) - first + 1, 2), sb_of(t) + first

    def full_half(t, half, fn, lo, hi):
        cnt, first = count_half(t, half)

        def one(j, _):
            c = first + 2 * j
            fn(c, pl.multiple_of(c * CH, CH), CH)
            return 0

        lax.fori_loop(lo, jnp.minimum(cnt, hi), one, 0)

    def head_row(t):
        return pl.multiple_of(pair_of(t) * NB, NB)

    def head_rows(t):
        return pl.ds(pl.multiple_of(pair_of(t) * NB, NB), NB)

    def lanes(l):
        return pl.ds(pl.multiple_of(l * NB, NB), NB)

    def rcopy(src, dst, ssem, rsem, dev):
        return pltpu.make_async_remote_copy(src, dst, ssem, rsem, device_id=dev, device_id_type=MESH_ID)

    def panel(t, r0, n, own):
        if own:
            return v_ref.at[pl.ds(r0, n), lanes(sb_of(t))]
        return vb.at[q, pair_of(t), pl.ds(r0, n), :]

    def side_copy(src, dst, t, c, d):
        return rcopy(src, dst, i_snd.at[d, rem(t, SLOTS), c], i_rcv.at[t, c], side_of(d))

    def core_copy(src, dst, t, c):
        return rcopy(src, dst, d_snd.at[rem(t, SLOTS), c], d_rcv.at[t, c], partner)

    def all_sent(t):
        d = owner_dist(t)

        def over(c, r0, n):
            here = panel(t, r0, n, False)
            core_copy(here, here, t, c).wait_send()

        small(t, 0, over)
        full(t, over)

        def by_side(x):
            def fn(c, r0, n):
                here = panel(t, r0, n, False)
                side_copy(here, here, t, c, x).wait_send()

            return fn

        @pl.when(d == 0)
        def _():
            for x in range(2):
                small(t, 0, by_side(x))
                full(t, by_side(x))

        @pl.when(rem(d, 2) == 1)
        def _():
            half = jnp.where(d == 1, 0, 1)
            in_half(t, half, by_side(half))

    def free_slot(t):
        @pl.when(t >= SLOTS)
        def _():
            all_sent(t - SLOTS)

    def send_own(u):
        first = RING - 1 - k
        part = rem(u - first + 2 * RING, RING)
        t = u - part

        @pl.when((t >= 0) & (t < npair))
        def _():
            @pl.when(part == 0)
            def _():
                free_slot(t)

                def over(c, r0, n):
                    core_copy(panel(t, r0, n, True), panel(t, r0, n, False), t, c).start()

                core_copy(eb.at[sb_of(t)], panel(t, head_row(t), NB, False), t, nsb).start()
                small(t, 1, over)
                full(t, over)

            def side(d, _):
                half = rem(d + div(part, 2), 2)

                def send(src, dst, c):
                    side_copy(src, dst, t, c, d).start()

                def out(c, r0, n):
                    send(panel(t, r0, n, True), panel(t, r0, n, False), c)

                cnt, _ = count_half(t, half)
                mid = div(cnt + 1, 2)
                begins = rem(part, 2) == 0

                @pl.when(begins & (small_half(t) == half))
                def _():
                    send(eb.at[sb_of(t)], panel(t, head_row(t), NB, False), nsb)
                    small(t, 1, out)

                full_half(t, half, out, jnp.where(begins, 0, mid), jnp.where(begins, mid, cnt))
                return 0

            lax.fori_loop(0, 2, side, 0)

    def pass_on(t, half, forward):
        def got(send):
            def fn(c, r0, n):
                here = panel(t, r0, n, False)
                side_copy(here, here, t, c, half).wait_recv()
                core_copy(here, here, t, c).start()
                if send:
                    side_copy(here, here, t, c, half).start()

            return fn

        @pl.when(forward)
        def _():
            in_half(t, half, got(True))

        @pl.when(jnp.logical_not(forward))
        def _():
            in_half(t, half, got(False))

    def brought(i):
        return jnp.minimum(npair - 1, jnp.minimum(i + 2, jnp.maximum(AHEAD + 1, i + 1)))

    def falling(i, high, low, i0, i1):
        return high - jnp.clip(((high - low) * (i - i0) + i1 - i0 - 1) // (i1 - i0), 0, high - low)

    def hand_lead(i):
        return jnp.minimum(npair - 1, brought(i) + jnp.minimum(falling(i, 5, 3, 1, 31), i + 3))

    def rest_lead(i):
        return jnp.minimum(npair - 1, brought(i) + jnp.where(i < 28, jnp.minimum(1, i + 3), 0))

    def far_lead(i):
        return jnp.minimum(npair - 1, brought(i) + jnp.where(((i >= 2) & (i < 24)) | ((i >= 26) & (i < 29)), 1, 0))

    def own_lead(i):
        return jnp.minimum(npair + RING - 2, brought(i) + jnp.minimum(falling(i, 9, 7, 12, 16), 4 + 2 * (i + 2)))

    def span(lead, i):
        return jnp.where(i < -1, 0, lead(i - 1) + 1), lead(i) + 1

    def service(i):
        def one(j, _):
            kind = jnp.where(i < -1, j, 3 - j)

            @pl.when(kind == 0)
            def _():
                lo, hi = span(own_lead, i)
                lax.fori_loop(lo, hi, lambda u, _: (send_own(u), 0)[1], 0)

            @pl.when(kind > 0)
            def _():
                h = span(hand_lead, i)
                e = span(rest_lead, i)
                f = span(far_lead, i)
                lo, hi = (jnp.where(kind == 1, x, jnp.where(kind == 2, y, z)) for x, y, z in zip(h, e, f))

                def take(x, _):
                    t = lo + div(x, 2)
                    d = owner_dist(t)
                    half = rem(x, 2)
                    mine = jnp.where(d == 1, 0, 1)
                    afar = (kind == 3) & (d == 2)
                    hand = (kind == 1) & (rem(d, 2) == 1) & (half == mine)
                    rest = (kind == 2) & (rem(d, 2) == 1) & (half != mine)

                    @pl.when(hand | (afar & (half == 0)))
                    def _():
                        free_slot(t)

                    @pl.when(afar | hand | rest)
                    def _():
                        pass_on(t, half, hand)

                    return 0

                lax.fori_loop(0, 2 * jnp.maximum(hi - lo, 0), take, 0)

            return 0

        lax.fori_loop(0, 4, one, 0)

    def make_heads():
        def copies(l):
            rr = pl.ds(pl.multiple_of((l * RING + k) * NB, NB), NB)
            return (pltpu.make_async_copy(v_ref.at[rr, lanes(l)], eb.at[l], h_sem.at[0, l]),
                    pltpu.make_async_copy(t_ref.at[l], et.at[l], h_sem.at[1, l]))

        def begin(l, _):
            for c in copies(l):
                c.start()
            return 0

        lax.fori_loop(0, nsb, begin, 0)

        def one(l, _):
            for c in copies(l):
                c.wait()
            x = eb[l]
            tt = et[l]
            below = lax.broadcasted_iota(jnp.int32, (NB, NB), 0) > lax.broadcasted_iota(jnp.int32, (NB, NB), 1)
            both_in = jnp.where(below, x, tt)
            eb[l] = jnp.where(r == q, both_in, jnp.where(r == 0, tt, x))
            return 0

        lax.fori_loop(0, nsb, one, 0)

    def z_local(c):
        mine = pl.multiple_of(r * rows + c * CH, CH)
        return pltpu.make_async_copy(z_ref.at[pl.ds(mine, CH), :], zl.at[r, chunk_at(c), :], z_loc.at[c])

    def z_piece(w):
        c = nsb - 1 - w // RING
        r0 = c * CH + w % RING * NB
        theirs = pl.multiple_of((1 - r) * rows + r0, NB)
        return rcopy(z_ref.at[pl.ds(theirs, NB), :], zl.at[r, pl.ds(pl.multiple_of(r0, NB), NB), :],
                     z_snd.at[w], z_rcv.at[w], across)

    def put_x(g, x, at):
        xt[g, :, at] = x
        for i, piece in enumerate(split3(x)):
            xp[g, i * NB : (i + 1) * NB, at] = piece

    def admit(c):
        for j in range(RING):
            z_piece((nsb - 1 - c) * RING + j).wait()
        z_local(c).wait()

        def one(g, _):
            put_x(g, zl[g, chunk_at(c), :].T, chunk_at(c))
            return 0

        lax.fori_loop(0, 2, one, 0)

    def load(t, c, side, src, at):
        return pltpu.make_async_copy(src, vf.at[at, lanes(side)], ld.at[side, c])

    def start_loads(t):
        mine = owner_dist(t) == 0
        p = pair_of(t)

        def one(c, r0, n):
            at = pl.ds(r0, n)

            @pl.when(mine)
            def _():
                load(t, c, q, panel(t, r0, n, True), at).start()

            @pl.when(jnp.logical_not(mine))
            def _():
                load(t, c, q, panel(t, r0, n, False), at).start()

            here = panel(t, r0, n, False)
            core_copy(here, here, t, c).wait_recv()
            load(t, c, 1 - q, vb.at[1 - q, p, at, :], at).start()

        at = head_rows(t)

        @pl.when(jnp.logical_not(mine))
        def _():
            load(t, nsb, q, vb.at[q, p, at, :], at).start()

        here = panel(t, head_row(t), NB, False)
        core_copy(here, here, t, nsb).wait_recv()
        load(t, nsb, 1 - q, vb.at[1 - q, p, at, :], at).start()
        small(t, 1, one)
        full(t, one)

    def pieces(slot, at, x):
        for i, piece in enumerate(split3(x)):
            vn[slot, at, i * PW : (i + 1) * PW] = piece

    def prep(t):
        slot = t % 3
        mine = owner_dist(t) == 0
        at = head_rows(t)
        l = sb_of(t)

        load(t, nsb, 1 - q, vb.at[0, 0, at, :], at).wait()

        @pl.when((r == 0) & (q == 0) & (t >= 3))
        def _():
            factor_across(t - 3).wait_send()

        @pl.when(mine)
        def _():
            vf[at, lanes(q)] = eb[l]

        @pl.when(jnp.logical_not(mine))
        def _():
            load(t, nsb, q, vb.at[0, 0, at, :], at).wait()

        def above(j, _):
            pieces(slot, pl.ds(pl.multiple_of(l * CH + j * NB, NB), NB), jnp.zeros((NB, PW), F32))
            return 0

        lax.fori_loop(0, chip_of(t), above, 0)

        i0 = lax.broadcasted_iota(jnp.int32, (NB, NB), 0)
        i1 = lax.broadcasted_iota(jnp.int32, (NB, NB), 1)
        one = jnp.where(i0 == i1, 1.0, 0.0).astype(F32)
        x0 = vf[at, 0:NB]
        x1 = vf[at, NB:PW]
        first = r == 0
        v0 = jnp.where(first, jnp.where(i0 > i1, x0, one), x0)
        v1 = jnp.where(first, 0.0, jnp.where(i0 > i1, x1, one))
        tc[slot, 0] = jnp.where(i0 > i1, 0.0, x0)
        tc[slot, 1] = jnp.where(i0 > i1, 0.0, x1)
        pieces(slot, at, jnp.concatenate([v0, v1], axis=1))

        @pl.when(first & (q == 0))
        def _():
            factor_across(t).start()

        def chunk(c, r0, n):
            a = pl.ds(r0, n)
            for side in range(2):
                load(t, c, side, vb.at[0, 0, a, :], a).wait()
            for j in range(0, n, NB):
                b = pl.ds(pl.multiple_of(r0 + j, NB), NB)
                pieces(slot, b, vf[b, :])

        small(t, 1, chunk)
        full(t, chunk)

    def factor_across(t):
        return rcopy(tc.at[t % 3, 0], tb.at[t % 8], t_snd.at[0, t % 8], t_rcv.at[0, t % 8], across)

    def factor_over(t):
        return rcopy(tb.at[t % 8], tb.at[t % 8], t_snd.at[1, t % 8], t_rcv.at[1, t % 8], partner)

    def share_factor(t):
        @pl.when((r == 1) & (q == 0))
        def _():
            factor_across(t).wait_recv()

            @pl.when(t >= 2)
            def _():
                factor_over(t - 2).wait_send()

            factor_over(t).start()

    def late(t):
        return t > AHEAD + 1

    def part_copy(t):
        return rcopy(gs.at[t % 2], gp.at[t % 2], p_snd.at[t % 2], p_rcv.at[t % 2], partner)

    def plane_copy(t):
        return rcopy(gz.at[t % 2], gr.at[t % 2], g_snd.at[t % 2], g_rcv.at[t % 2], across)

    def total_copy(t):
        return rcopy(gf.at[t % 8], gf.at[t % 8], f_snd.at[t % 8], f_rcv.at[t % 8], partner)

    def gram_part(t):
        slot = t % 3
        s = t % 2

        @pl.when(t >= 2)
        def _():
            part_copy(t - 2).wait_send()

        gs[s] = jnp.zeros((NB, NB), F32)
        first = (height(t) + t % 2) // 2
        lo = sb_of(t) + q * first
        cnt = jnp.where(q == 0, first, height(t) - first)

        def block(c, n):
            at = pl.ds(pl.multiple_of(c * CH, CH), n * CH)
            a = [vn[slot, at, i * PW : i * PW + NB].T for i in range(3)]
            b = [vn[slot, at, i * PW + NB : (i + 1) * PW] for i in range(3)]
            x = mm(jnp.concatenate(a, axis=0), jnp.concatenate(b[0:2], axis=1))
            gs[s] += add_rows(add_rows(mm(a[0], b[2]), x[:, 0:NB], NB), x[0 : 2 * NB, NB:PW], NB)

        if nsb >= 8:

            @pl.when(cnt >= 4)
            def _():
                block(lo, 4)

        if nsb >= 3:

            @pl.when(cnt % 4 >= 2)
            def _():
                block(lo + cnt // 4 * 4, 2)

        @pl.when(cnt % 2 == 1)
        def _():
            block(lo + cnt - 1, 1)

        part_copy(t).start()

    def sends_plane(t):
        return late(t) | (t % 2 == q)

    def gram_plane(t):
        s = t % 2
        part_copy(t).wait_recv()

        @pl.when((t >= 2) & sends_plane(t - 2))
        def _():
            plane_copy(t - 2).wait_send()

        gz[s] = gs[s] + gp[s]

        @pl.when(sends_plane(t))
        def _():
            plane_copy(t).start()

    def gram_total(t):
        s = t % 2

        @pl.when(sends_plane(t))
        def _():
            plane_copy(t).wait_recv()

            @pl.when((t >= 8) & (t % 2 == q) & jnp.logical_not(late(t - 8)))
            def _():
                total_copy(t - 8).wait_send()

            gf[t % 8] = gz[s] + gr[s]

            @pl.when(jnp.logical_not(late(t)))
            def _():
                total_copy(t).start()

    def block_factor(t):
        slot = t % 3

        @pl.when(jnp.logical_not(sends_plane(t)))
        def _():
            total_copy(t).wait_recv()

        @pl.when((r == 1) & (q == 1))
        def _():
            factor_over(t).wait_recv()

        g = gf[t % 8]
        ta = jnp.where(r == 0, tc[slot, 0], tb[t % 8])
        tbb = tc[slot, 1]
        upper = -full_dot(ta, full_dot(g, tbb))
        for i, piece in enumerate(split3(ta)):
            tp[0:NB, i * PW : i * PW + NB] = piece
        for i, piece in enumerate(split3(upper)):
            tp[0:NB, i * PW + NB : (i + 1) * PW] = piece
        for i, piece in enumerate(split3(tbb)):
            tp[NB:PW, i * PW : i * PW + NB] = jnp.zeros((NB, NB), BF16)
            tp[NB:PW, i * PW + NB : (i + 1) * PW] = piece

    def w_copy(t, g):
        return rcopy(ws.at[t % 2, g], wr.at[t % 2, g], w_snd.at[t % 2, g], w_rcv.at[t % 2, g], across)

    def coefficients(t, g):
        w_copy(t, g).wait_recv()
        w = ws[t % 2, g] + wr[t % 2, g]
        y = stacked(mm_nt, jnp.concatenate(split3(w), axis=0), [tp[:, i * PW : (i + 1) * PW] for i in range(3)])
        for i, piece in enumerate(split3(y)):
            yp[i * NB : (i + 1) * NB] = piece

    def piece_of(t, i, at):
        return vn[t % 3, at, i * PW : (i + 1) * PW]

    def chunk_at(c):
        return pl.ds(pl.multiple_of(c * CH, CH), CH)

    def passes(m, i, g, n, finish):
        units = m * CH // UNIT
        base = rows - m * CH
        w = None
        for c in range(units + (0 if n is None else LAG)):
            at = pl.ds(base + c * UNIT, UNIT)
            an = pl.ds(max(0, base + (c - LAG) * UNIT), UNIT)
            u = None
            for j in range(3):
                k3 = (3 - j) * NB
                if n is not None and c >= LAG:
                    w = add_rows(w, mm(xp[g, 0:k3, an], piece_of(n, j, an)), NB)
                if c < units:
                    u = add_rows(u, mm_nt(yp[0:k3], piece_of(i, j, at)), NB)
            if c < units:
                finish(at, xt[g, :, at] - u)
        if n is not None:
            ws[n % 2, g] += w

    def product(n, g, at):
        w = None
        for j in range(3):
            w = add_rows(w, mm(xp[g, 0 : (3 - j) * NB, at], piece_of(n, j, at)), NB)
        ws[n % 2, g] += w

    def both(i, g):
        n = i + 1

        @pl.when(sb_of(n) < sb_of(i))
        def _():
            product(n, g, chunk_at(sb_of(n)))

        for m in range(1, nsb + 1):

            @pl.when(height(i) == m)
            def _(m=m):
                passes(m, i, g, n, lambda at, x: put_x(g, x, at))

    def out_copy(g, c):
        return pltpu.make_async_copy(zl.at[g, chunk_at(c), :], out_ref.at[chunk_at(c), lanes(g)], o_sem.at[g, c])

    def last(i, g):
        def finish(at, x):
            zl[g, at, :] = x.T

        passes(nsb, i, g, None, finish)

        def out(c, _):
            out_copy(g, c).start()
            return 0

        lax.fori_loop(0, nsb, out, 0)

    def step(i, _):
        n = i + 1
        early = i < AHEAD
        b = jnp.where(early, i + 2, n)
        brings = (i != AHEAD) & (b < npair)

        @pl.when(i < npair - 1)
        def _():
            service(i)

        @pl.when(brings)
        def _():
            start_loads(b)

        @pl.when(i >= 0)
        def _():
            block_factor(i)

        @pl.when(n == npair)
        def _():
            lax.fori_loop(max(0, npair - SLOTS), npair, lambda t, _: (all_sent(t), 0)[1], 0)

        @pl.when((n >= 0) & (n < npair) & (n % RING == 0))
        def _():
            admit(sb_of(n))

        def group(g, _):
            @pl.when((g == jnp.where(early, 1, 0)) & brings)
            def _():
                prep(b)
                gram_part(b)

            @pl.when(i >= 0)
            def _():
                coefficients(i, g)

            @pl.when((n >= 0) & (n < npair))
            def _():
                @pl.when(n >= 2)
                def _():
                    w_copy(n - 2, g).wait_send()

                ws[n % 2, g] = jnp.zeros((NB, PW), F32)

            @pl.when(i == -1)
            def _():
                product(n, g, chunk_at(nsb - 1))

            @pl.when((i >= 0) & (n < npair))
            def _():
                both(i, g)

            @pl.when((g == jnp.where(early, 1, 0)) & brings)
            def _():
                gram_plane(b)

            @pl.when((n >= 0) & (n < npair))
            def _():
                w_copy(n, g).start()

                @pl.when(g == jnp.where(i <= AHEAD, 0, 1))
                def _():
                    share_factor(n)
                    gram_total(n)

            @pl.when(n == npair)
            def _():
                last(i, g)

            return 0

        lax.fori_loop(0, 2, group, 0)

        @pl.when((n >= RING + 1) & (n + RING + 1 < npair))
        def _():
            z_piece(n + RING + 1).start()

        @pl.when((n >= 0) & (n % RING == 2) & (n + RING < npair))
        def _():
            z_local(sb_of(n) - 1).start()

        return 0

    barrier = pltpu.get_barrier_semaphore()
    for dev in (at_ring(rho + 1), at_ring(rho + RING - 1), partner, across):
        pl.semaphore_signal(barrier, inc=1, device_id=dev, device_id_type=MESH_ID)
    pl.semaphore_wait(barrier, 4)

    for j in range(min(2 * RING + 2, npair)):
        z_piece(j).start()
    z_local(nsb - 1).start()
    make_heads()
    lax.fori_loop(-2, npair, step, 0)

    for t in (npair - 2, npair - 1):
        for g in range(2):
            w_copy(t, g).wait_send()
    for t in (npair - 2, npair - 1):
        part_copy(t).wait_send()

        @pl.when(sends_plane(t))
        def _(t=t):
            plane_copy(t).wait_send()

    newest = min(npair - 1, AHEAD + 1)
    for t in range(max(0, npair - 8), newest + 1):

        @pl.when(t % 2 == q)
        def _(t=t):
            total_copy(t).wait_send()

    for t in range(npair - 3, npair):

        @pl.when((r == 0) & (q == 0))
        def _(t=t):
            factor_across(t).wait_send()

    for t in range(npair - 2, npair):

        @pl.when((r == 1) & (q == 0))
        def _(t=t):
            factor_over(t).wait_send()

    def out_done(c, _):
        for g in range(2):
            out_copy(g, c).wait()
        return 0

    lax.fori_loop(0, nsb, out_done, 0)


def solution(mesh):
    def local(v, t, z):
        rows, cols = v.shape
        nsb = cols // NB
        npair = nsb * RING
        hbm = pl.BlockSpec(memory_space=pltpu.MemorySpace.HBM)
        out, _ = pl.pallas_call(
            functools.partial(body, nsb),
            out_shape=(
                jax.ShapeDtypeStruct((rows, PW), F32),
                jax.ShapeDtypeStruct((2, npair, rows, NB), F32),
            ),
            in_specs=[hbm] * 3,
            out_specs=(hbm, hbm),
            scratch_shapes=[
                pltpu.VMEM((2, rows, NB), F32),
                pltpu.VMEM((2, NB, rows), F32),
                pltpu.VMEM((2, 3 * NB, rows), BF16),
                pltpu.VMEM((rows, PW), F32),
                pltpu.VMEM((3, rows, 3 * PW), BF16),
                pltpu.VMEM((8, NB, NB), F32),
                pltpu.VMEM((3, 2, NB, NB), F32),
                pltpu.VMEM((PW, 3 * PW), BF16),
                pltpu.VMEM((2, 2, NB, PW), F32),
                pltpu.VMEM((2, 2, NB, PW), F32),
                pltpu.VMEM((2, NB, NB), F32),
                pltpu.VMEM((2, NB, NB), F32),
                pltpu.VMEM((2, NB, NB), F32),
                pltpu.VMEM((2, NB, NB), F32),
                pltpu.VMEM((8, NB, NB), F32),
                pltpu.VMEM((3 * NB, PW), BF16),
                pltpu.VMEM((nsb, NB, NB), F32),
                pltpu.VMEM((nsb, NB, NB), F32),
            ],
            compiler_params=pltpu.CompilerParams(
                collective_id=0, has_side_effects=True, vmem_limit_bytes=60 * 2**20),
            name="backtransform",
        )(v, t, z)
        return out

    return jax.shard_map(local, mesh=mesh,
                         in_specs=(P("row", "col"), P("col", None, None), P(None, ("col", "row"))),
                         out_specs=P("row", "col"), check_vma=False)
```

```python
import functools

import jax
import jax.numpy as jnp
from jax import lax
from jax.experimental import pallas as pl
from jax.experimental.pallas import tpu as pltpu
from jax.sharding import PartitionSpec as P

F32 = jnp.float32
BF16 = jnp.bfloat16
MESH_ID = pl.DeviceIdType.MESH

NB = 128
PW = 2 * NB
CH = 4 * NB
UNIT = PW
LAG = 2
RING = 4
SLOTS = 8
AHEAD = 20


def div(a, b):
    return lax.div(a, b)


def rem(a, b):
    return lax.rem(a, b)


def split3(x):
    hi = x.astype(BF16)
    rest = x - hi.astype(F32)
    mid = rest.astype(BF16)
    low = (rest - mid.astype(F32)).astype(BF16)
    return hi, mid, low


def mm(a, b):
    return lax.dot_general(a, b, (((1,), (0,)), ((), ())), preferred_element_type=F32)


def mm_nt(a, b):
    return lax.dot_general(a, b, (((1,), (1,)), ((), ())), preferred_element_type=F32)


def add_rows(total, x, n):
    for i in range(0, x.shape[0], n):
        part = x[i : i + n]
        total = part if total is None else total + part
    return total


def stacked(dot, a3, b):
    m = a3.shape[0] // 3
    s = None
    for i in range(3):
        s = add_rows(s, dot(a3[0 : (3 - i) * m], b[i]), m)
    return s


def full_dot(a, b):
    ah, am, al = split3(a)
    bh, bm, bl = split3(b)
    n = a.shape[0]
    x = mm(jnp.concatenate([ah, am], axis=1), jnp.concatenate([jnp.concatenate([bh, bm], axis=1)] * 2, axis=0))
    y = mm(jnp.concatenate([al, ah], axis=1), jnp.concatenate([bh, bl], axis=0))
    return x[:, 0:n] + x[:, n:] + y


def body(nsb, v_ref, t_ref, z_ref, out_ref, vb, *scratch):
    rows = nsb * CH
    dma = pltpu.SemaphoreType.DMA
    npair = nsb * RING
    nc = nsb + RING
    pl.run_scoped(
        functools.partial(run, nsb, rows, npair, v_ref, t_ref, z_ref, out_ref, vb, scratch),
        dma((nsb,)),
        dma((npair,)),
        dma((npair,)),
        dma((npair, nc)),
        dma((npair, nc)),
        dma((2, 2)),
        dma((2, 2)),
        dma((2,)),
        dma((2,)),
        dma((8,)),
        dma((8,)),
        dma((2, nc)),
        dma((2, nsb)),
        dma((2, SLOTS, nc)),
        dma((SLOTS, nc)),
        dma((2, nsb)),
        dma((2,)),
        dma((2,)),
        dma((2, 8)),
        dma((2, 8)),
    )


def run(nsb, rows, npair, v_ref, t_ref, z_ref, out_ref, vb, scratch, *sems):
    (zl, xt, xp, vf, vn, tb, tc, tp, ws, wr, gs, gp, gz, gr, gf, yp, eb, et) = scratch
    (z_loc, z_snd, z_rcv, i_rcv, d_rcv, w_snd, w_rcv, g_snd, g_rcv, f_snd, f_rcv, ld, o_sem, i_snd, d_snd, h_sem, p_snd, p_rcv, t_snd, t_rcv) = sems
    r = lax.axis_index("row")
    col = lax.axis_index("col")
    q = rem(col, 2)
    k = div(col, 2)
    ky, kx = div(k, 2), rem(k, 2)
    rho = 2 * ky + rem(kx + ky, 2)

    def at_ring(i):
        i = rem(i, RING)
        y = div(i, 2)
        x = rem(rem(i, 2) + y, 2)
        return (r, (y * 2 + x) * 2 + q)

    cw, ccw = at_ring(rho + 1), at_ring(rho + RING - 1)

    def side_of(d):
        return (r, jnp.where(d == 0, cw[1], ccw[1]))

    partner = (r, k * 2 + 1 - q)
    across = (1 - r, col)

    def pair_of(t):
        return npair - 1 - t

    def sb_of(t):
        return div(pair_of(t), RING)

    def chip_of(t):
        return rem(pair_of(t), RING)

    def owner_dist(t):
        kk = chip_of(t)
        y = div(kk, 2)
        ro = 2 * y + rem(rem(kk, 2) + y, 2)
        return rem(rho - ro + RING, RING)

    def height(t):
        return nsb - sb_of(t)

    def small_half(t):
        return rem(div(height(t) - 1, 2), 2)

    def small(t, first, fn):
        def one(j, _):
            fn(nsb + j, pl.multiple_of((pair_of(t) + j) * NB, NB), NB)
            return 0

        lax.fori_loop(first, RING - chip_of(t), one, 0)

    def full(t, fn):
        def one(c, _):
            fn(c, pl.multiple_of(c * CH, CH), CH)
            return 0

        lax.fori_loop(sb_of(t) + 1, nsb, one, 0)

    def in_half(t, half, fn):
        @pl.when(small_half(t) == half)
        def _():
            small(t, 0, fn)

        full_half(t, half, fn, 0, nsb)

    def count_half(t, half):
        first = 2 - rem(half + div(height(t) - 1, 2), 2)
        return div(height(t) - first + 1, 2), sb_of(t) + first

    def full_half(t, half, fn, lo, hi):
        cnt, first = count_half(t, half)

        def one(j, _):
            c = first + 2 * j
            fn(c, pl.multiple_of(c * CH, CH), CH)
            return 0

        lax.fori_loop(lo, jnp.minimum(cnt, hi), one, 0)

    def head_row(t):
        return pl.multiple_of(pair_of(t) * NB, NB)

    def head_rows(t):
        return pl.ds(pl.multiple_of(pair_of(t) * NB, NB), NB)

    def lanes(l):
        return pl.ds(pl.multiple_of(l * NB, NB), NB)

    def rcopy(src, dst, ssem, rsem, dev):
        return pltpu.make_async_remote_copy(src, dst, ssem, rsem, device_id=dev, device_id_type=MESH_ID)

    def panel(t, r0, n, own):
        if own:
            return v_ref.at[pl.ds(r0, n), lanes(sb_of(t))]
        return vb.at[q, pair_of(t), pl.ds(r0, n), :]

    def side_copy(src, dst, t, c, d):
        return rcopy(src, dst, i_snd.at[d, rem(t, SLOTS), c], i_rcv.at[t, c], side_of(d))

    def core_copy(src, dst, t, c):
        return rcopy(src, dst, d_snd.at[rem(t, SLOTS), c], d_rcv.at[t, c], partner)

    def all_sent(t):
        d = owner_dist(t)

        def over(c, r0, n):
            here = panel(t, r0, n, False)
            core_copy(here, here, t, c).wait_send()

        small(t, 0, over)
        full(t, over)

        def by_side(x):
            def fn(c, r0, n):
                here = panel(t, r0, n, False)
                side_copy(here, here, t, c, x).wait_send()

            return fn

        @pl.when(d == 0)
        def _():
            for x in range(2):
                small(t, 0, by_side(x))
                full(t, by_side(x))

        @pl.when(rem(d, 2) == 1)
        def _():
            half = jnp.where(d == 1, 0, 1)
            in_half(t, half, by_side(half))

    def free_slot(t):
        @pl.when(t >= SLOTS)
        def _():
            all_sent(t - SLOTS)

    def send_own(u):
        first = RING - 1 - k
        part = rem(u - first + 2 * RING, RING)
        t = u - part

        @pl.when((t >= 0) & (t < npair))
        def _():
            @pl.when(part == 0)
            def _():
                free_slot(t)

                def over(c, r0, n):
                    core_copy(panel(t, r0, n, True), panel(t, r0, n, False), t, c).start()

                core_copy(eb.at[sb_of(t)], panel(t, head_row(t), NB, False), t, nsb).start()
                small(t, 1, over)
                full(t, over)

            def side(d, _):
                half = rem(d + div(part, 2), 2)

                def send(src, dst, c):
                    side_copy(src, dst, t, c, d).start()

                def out(c, r0, n):
                    send(panel(t, r0, n, True), panel(t, r0, n, False), c)

                cnt, _ = count_half(t, half)
                mid = div(cnt + 1, 2)
                begins = rem(part, 2) == 0

                @pl.when(begins & (small_half(t) == half))
                def _():
                    send(eb.at[sb_of(t)], panel(t, head_row(t), NB, False), nsb)
                    small(t, 1, out)

                full_half(t, half, out, jnp.where(begins, 0, mid), jnp.where(begins, mid, cnt))
                return 0

            lax.fori_loop(0, 2, side, 0)

    def pass_on(t, half, forward):
        def got(send):
            def fn(c, r0, n):
                here = panel(t, r0, n, False)
                side_copy(here, here, t, c, half).wait_recv()
                core_copy(here, here, t, c).start()
                if send:
                    side_copy(here, here, t, c, half).start()

            return fn

        @pl.when(forward)
        def _():
            in_half(t, half, got(True))

        @pl.when(jnp.logical_not(forward))
        def _():
            in_half(t, half, got(False))

    def brought(i):
        return jnp.minimum(npair - 1, jnp.minimum(i + 2, jnp.maximum(AHEAD + 1, i + 1)))

    def falling(i, high, low, i0, i1):
        return high - jnp.clip(((high - low) * (i - i0) + i1 - i0 - 1) // (i1 - i0), 0, high - low)

    def hand_lead(i):
        return jnp.minimum(npair - 1, brought(i) + jnp.minimum(falling(i, 5, 3, 15, 26), i + 3))

    def rest_lead(i):
        return jnp.minimum(npair - 1, brought(i) + jnp.where(i < 27, jnp.minimum(1, i + 3), 0))

    def far_lead(i):
        return jnp.minimum(npair - 1, brought(i) + jnp.where((i >= 4) & (i < 21), 1, 0))

    def own_lead(i):
        return jnp.minimum(npair + RING - 2, brought(i) + jnp.minimum(falling(i, 10, 6, 13, 28), 4 + 3 * (i + 2)))

    def span(lead, i):
        return jnp.where(i < -1, 0, lead(i - 1) + 1), lead(i) + 1

    def service(i):
        def one(j, _):
            kind = jnp.where(i < -1, j, 3 - j)

            @pl.when(kind == 0)
            def _():
                lo, hi = span(own_lead, i)
                lax.fori_loop(lo, hi, lambda u, _: (send_own(u), 0)[1], 0)

            @pl.when(kind > 0)
            def _():
                h = span(hand_lead, i)
                e = span(rest_lead, i)
                f = span(far_lead, i)
                lo, hi = (jnp.where(kind == 1, x, jnp.where(kind == 2, y, z)) for x, y, z in zip(h, e, f))

                def take(x, _):
                    t = lo + div(x, 2)
                    d = owner_dist(t)
                    half = rem(x, 2)
                    mine = jnp.where(d == 1, 0, 1)
                    afar = (kind == 3) & (d == 2)
                    hand = (kind == 1) & (rem(d, 2) == 1) & (half == mine)
                    rest = (kind == 2) & (rem(d, 2) == 1) & (half != mine)

                    @pl.when(hand | (afar & (half == 0)))
                    def _():
                        free_slot(t)

                    @pl.when(afar | hand | rest)
                    def _():
                        pass_on(t, half, hand)

                    return 0

                lax.fori_loop(0, 2 * jnp.maximum(hi - lo, 0), take, 0)

            return 0

        lax.fori_loop(0, 4, one, 0)

    def make_heads():
        def copies(l):
            rr = pl.ds(pl.multiple_of((l * RING + k) * NB, NB), NB)
            return (pltpu.make_async_copy(v_ref.at[rr, lanes(l)], eb.at[l], h_sem.at[0, l]),
                    pltpu.make_async_copy(t_ref.at[l], et.at[l], h_sem.at[1, l]))

        def begin(l, _):
            for c in copies(l):
                c.start()
            return 0

        lax.fori_loop(0, nsb, begin, 0)

        def one(l, _):
            for c in copies(l):
                c.wait()
            x = eb[l]
            tt = et[l]
            below = lax.broadcasted_iota(jnp.int32, (NB, NB), 0) > lax.broadcasted_iota(jnp.int32, (NB, NB), 1)
            both_in = jnp.where(below, x, tt)
            eb[l] = jnp.where(r == q, both_in, jnp.where(r == 0, tt, x))
            return 0

        lax.fori_loop(0, nsb, one, 0)

    def z_local(c):
        mine = pl.multiple_of(r * rows + c * CH, CH)
        return pltpu.make_async_copy(z_ref.at[pl.ds(mine, CH), :], zl.at[r, chunk_at(c), :], z_loc.at[c])

    def z_piece(w):
        c = nsb - 1 - w // RING
        r0 = c * CH + w % RING * NB
        theirs = pl.multiple_of((1 - r) * rows + r0, NB)
        return rcopy(z_ref.at[pl.ds(theirs, NB), :], zl.at[r, pl.ds(pl.multiple_of(r0, NB), NB), :],
                     z_snd.at[w], z_rcv.at[w], across)

    def put_x(g, x, at):
        xt[g, :, at] = x
        for i, piece in enumerate(split3(x)):
            xp[g, i * NB : (i + 1) * NB, at] = piece

    def admit(c):
        for j in range(RING):
            z_piece((nsb - 1 - c) * RING + j).wait()
        z_local(c).wait()

        def one(g, _):
            put_x(g, zl[g, chunk_at(c), :].T, chunk_at(c))
            return 0

        lax.fori_loop(0, 2, one, 0)

    def load(t, c, side, src, at):
        return pltpu.make_async_copy(src, vf.at[at, lanes(side)], ld.at[side, c])

    def start_loads(t):
        mine = owner_dist(t) == 0
        p = pair_of(t)

        def one(c, r0, n):
            at = pl.ds(r0, n)

            @pl.when(mine)
            def _():
                load(t, c, q, panel(t, r0, n, True), at).start()

            @pl.when(jnp.logical_not(mine))
            def _():
                load(t, c, q, panel(t, r0, n, False), at).start()

            here = panel(t, r0, n, False)
            core_copy(here, here, t, c).wait_recv()
            load(t, c, 1 - q, vb.at[1 - q, p, at, :], at).start()

        at = head_rows(t)

        @pl.when(jnp.logical_not(mine))
        def _():
            load(t, nsb, q, vb.at[q, p, at, :], at).start()

        here = panel(t, head_row(t), NB, False)
        core_copy(here, here, t, nsb).wait_recv()
        load(t, nsb, 1 - q, vb.at[1 - q, p, at, :], at).start()
        small(t, 1, one)
        full(t, one)

    def pieces(slot, at, x):
        for i, piece in enumerate(split3(x)):
            vn[slot, at, i * PW : (i + 1) * PW] = piece

    def prep(t):
        slot = t % 3
        mine = owner_dist(t) == 0
        at = head_rows(t)
        l = sb_of(t)

        load(t, nsb, 1 - q, vb.at[0, 0, at, :], at).wait()

        @pl.when((r == 0) & (q == 0) & (t >= 3))
        def _():
            factor_across(t - 3).wait_send()

        @pl.when(mine)
        def _():
            vf[at, lanes(q)] = eb[l]

        @pl.when(jnp.logical_not(mine))
        def _():
            load(t, nsb, q, vb.at[0, 0, at, :], at).wait()

        def above(j, _):
            pieces(slot, pl.ds(pl.multiple_of(l * CH + j * NB, NB), NB), jnp.zeros((NB, PW), F32))
            return 0

        lax.fori_loop(0, chip_of(t), above, 0)

        i0 = lax.broadcasted_iota(jnp.int32, (NB, NB), 0)
        i1 = lax.broadcasted_iota(jnp.int32, (NB, NB), 1)
        one = jnp.where(i0 == i1, 1.0, 0.0).astype(F32)
        x0 = vf[at, 0:NB]
        x1 = vf[at, NB:PW]
        first = r == 0
        v0 = jnp.where(first, jnp.where(i0 > i1, x0, one), x0)
        v1 = jnp.where(first, 0.0, jnp.where(i0 > i1, x1, one))
        tc[slot, 0] = jnp.where(i0 > i1, 0.0, x0)
        tc[slot, 1] = jnp.where(i0 > i1, 0.0, x1)
        pieces(slot, at, jnp.concatenate([v0, v1], axis=1))

        @pl.when(first & (q == 0))
        def _():
            factor_across(t).start()

        def chunk(c, r0, n):
            a = pl.ds(r0, n)
            for side in range(2):
                load(t, c, side, vb.at[0, 0, a, :], a).wait()
            for j in range(0, n, NB):
                b = pl.ds(pl.multiple_of(r0 + j, NB), NB)
                pieces(slot, b, vf[b, :])

        small(t, 1, chunk)
        full(t, chunk)

    def factor_across(t):
        return rcopy(tc.at[t % 3, 0], tb.at[t % 8], t_snd.at[0, t % 8], t_rcv.at[0, t % 8], across)

    def factor_over(t):
        return rcopy(tb.at[t % 8], tb.at[t % 8], t_snd.at[1, t % 8], t_rcv.at[1, t % 8], partner)

    def share_factor(t):
        @pl.when((r == 1) & (q == 0))
        def _():
            factor_across(t).wait_recv()

            @pl.when(t >= 2)
            def _():
                factor_over(t - 2).wait_send()

            factor_over(t).start()

    def late(t):
        return t > AHEAD + 1

    def part_copy(t):
        return rcopy(gs.at[t % 2], gp.at[t % 2], p_snd.at[t % 2], p_rcv.at[t % 2], partner)

    def plane_copy(t):
        return rcopy(gz.at[t % 2], gr.at[t % 2], g_snd.at[t % 2], g_rcv.at[t % 2], across)

    def total_copy(t):
        return rcopy(gf.at[t % 8], gf.at[t % 8], f_snd.at[t % 8], f_rcv.at[t % 8], partner)

    def gram_part(t):
        slot = t % 3
        s = t % 2

        @pl.when(t >= 2)
        def _():
            part_copy(t - 2).wait_send()

        gs[s] = jnp.zeros((NB, NB), F32)
        first = (height(t) + t % 2) // 2
        lo = sb_of(t) + q * first
        cnt = jnp.where(q == 0, first, height(t) - first)

        def block(c, n):
            at = pl.ds(pl.multiple_of(c * CH, CH), n * CH)
            a = [vn[slot, at, i * PW : i * PW + NB].T for i in range(3)]
            b = [vn[slot, at, i * PW + NB : (i + 1) * PW] for i in range(3)]
            x = mm(jnp.concatenate(a, axis=0), jnp.concatenate(b[0:2], axis=1))
            gs[s] += add_rows(add_rows(mm(a[0], b[2]), x[:, 0:NB], NB), x[0 : 2 * NB, NB:PW], NB)

        if nsb >= 8:

            @pl.when(cnt >= 4)
            def _():
                block(lo, 4)

        if nsb >= 3:

            @pl.when(cnt % 4 >= 2)
            def _():
                block(lo + cnt // 4 * 4, 2)

        @pl.when(cnt % 2 == 1)
        def _():
            block(lo + cnt - 1, 1)

        part_copy(t).start()

    def sends_plane(t):
        return late(t) | (t % 2 == q)

    def gram_plane(t):
        s = t % 2
        part_copy(t).wait_recv()

        @pl.when((t >= 2) & sends_plane(t - 2))
        def _():
            plane_copy(t - 2).wait_send()

        gz[s] = gs[s] + gp[s]

        @pl.when(sends_plane(t))
        def _():
            plane_copy(t).start()

    def gram_total(t):
        s = t % 2

        @pl.when(sends_plane(t))
        def _():
            plane_copy(t).wait_recv()

            @pl.when((t >= 8) & (t % 2 == q) & jnp.logical_not(late(t - 8)))
            def _():
                total_copy(t - 8).wait_send()

            gf[t % 8] = gz[s] + gr[s]

            @pl.when(jnp.logical_not(late(t)))
            def _():
                total_copy(t).start()

    def block_factor(t):
        slot = t % 3

        @pl.when(jnp.logical_not(sends_plane(t)))
        def _():
            total_copy(t).wait_recv()

        @pl.when((r == 1) & (q == 1))
        def _():
            factor_over(t).wait_recv()

        g = gf[t % 8]
        ta = jnp.where(r == 0, tc[slot, 0], tb[t % 8])
        tbb = tc[slot, 1]
        upper = -full_dot(ta, full_dot(g, tbb))
        for i, piece in enumerate(split3(ta)):
            tp[0:NB, i * PW : i * PW + NB] = piece
        for i, piece in enumerate(split3(upper)):
            tp[0:NB, i * PW + NB : (i + 1) * PW] = piece
        for i, piece in enumerate(split3(tbb)):
            tp[NB:PW, i * PW : i * PW + NB] = jnp.zeros((NB, NB), BF16)
            tp[NB:PW, i * PW + NB : (i + 1) * PW] = piece

    def w_copy(t, g):
        return rcopy(ws.at[t % 2, g], wr.at[t % 2, g], w_snd.at[t % 2, g], w_rcv.at[t % 2, g], across)

    def coefficients(t, g):
        with jax.named_scope("wwait"):
            w_copy(t, g).wait_recv()
        w = ws[t % 2, g] + wr[t % 2, g]
        y = stacked(mm_nt, jnp.concatenate(split3(w), axis=0), [tp[:, i * PW : (i + 1) * PW] for i in range(3)])
        for i, piece in enumerate(split3(y)):
            yp[i * NB : (i + 1) * NB] = piece

    def piece_of(t, i, at):
        return vn[t % 3, at, i * PW : (i + 1) * PW]

    def chunk_at(c):
        return pl.ds(pl.multiple_of(c * CH, CH), CH)

    def passes(m, i, g, n, finish):
        units = m * CH // UNIT
        base = rows - m * CH
        w = None
        for c in range(units + (0 if n is None else LAG)):
            at = pl.ds(base + c * UNIT, UNIT)
            an = pl.ds(max(0, base + (c - LAG) * UNIT), UNIT)
            u = None
            for j in range(3):
                k3 = (3 - j) * NB
                if n is not None and c >= LAG:
                    w = add_rows(w, mm(xp[g, 0:k3, an], piece_of(n, j, an)), NB)
                if c < units:
                    u = add_rows(u, mm_nt(yp[0:k3], piece_of(i, j, at)), NB)
            if c < units:
                finish(at, xt[g, :, at] - u)
        if n is not None:
            ws[n % 2, g] += w

    def product(n, g, at):
        w = None
        for j in range(3):
            w = add_rows(w, mm(xp[g, 0 : (3 - j) * NB, at], piece_of(n, j, at)), NB)
        ws[n % 2, g] += w

    def both(i, g):
        n = i + 1

        @pl.when(sb_of(n) < sb_of(i))
        def _():
            product(n, g, chunk_at(sb_of(n)))

        for m in range(1, nsb + 1):

            @pl.when(height(i) == m)
            def _(m=m):
                passes(m, i, g, n, lambda at, x: put_x(g, x, at))

    def out_copy(g, c):
        return pltpu.make_async_copy(zl.at[g, chunk_at(c), :], out_ref.at[chunk_at(c), lanes(g)], o_sem.at[g, c])

    def last(i, g):
        def finish(at, x):
            zl[g, at, :] = x.T

        passes(nsb, i, g, None, finish)

        def out(c, _):
            out_copy(g, c).start()
            return 0

        lax.fori_loop(0, nsb, out, 0)

    def step(i, _):
        n = i + 1
        early = i < AHEAD
        b = jnp.where(early, i + 2, n)
        brings = (i != AHEAD) & (b < npair)

        @pl.when(i < npair - 1)
        def _():
            with jax.named_scope("svc"):
                service(i)

        @pl.when(brings)
        def _():
            with jax.named_scope("loads"):
                start_loads(b)

        @pl.when(i >= 0)
        def _():
            with jax.named_scope("bfac"):
                block_factor(i)

        @pl.when(n == npair)
        def _():
            lax.fori_loop(max(0, npair - SLOTS), npair, lambda t, _: (all_sent(t), 0)[1], 0)

        @pl.when((n >= 0) & (n < npair) & (n % RING == 0))
        def _():
            with jax.named_scope("admit"):
                admit(sb_of(n))

        def group(g, _):
            @pl.when((g == jnp.where(early, 1, 0)) & brings)
            def _():
                with jax.named_scope("prep"):
                    prep(b)
                with jax.named_scope("gram"):
                    gram_part(b)

            @pl.when(i >= 0)
            def _():
                with jax.named_scope("coef"):
                    coefficients(i, g)

            @pl.when((n >= 0) & (n < npair))
            def _():
                @pl.when(n >= 2)
                def _():
                    w_copy(n - 2, g).wait_send()

                ws[n % 2, g] = jnp.zeros((NB, PW), F32)

            @pl.when(i == -1)
            def _():
                product(n, g, chunk_at(nsb - 1))

            @pl.when((i >= 0) & (n < npair))
            def _():
                with jax.named_scope("both"):
                    both(i, g)

            @pl.when((g == jnp.where(early, 1, 0)) & brings)
            def _():
                with jax.named_scope("gplane"):
                    gram_plane(b)

            @pl.when((n >= 0) & (n < npair))
            def _():
                w_copy(n, g).start()

                @pl.when(g == jnp.where(i <= AHEAD, 0, 1))
                def _():
                    with jax.named_scope("fshare"):
                        share_factor(n)
                    with jax.named_scope("gtot"):
                        gram_total(n)

            @pl.when(n == npair)
            def _():
                with jax.named_scope("last"):
                    last(i, g)

            return 0

        lax.fori_loop(0, 2, group, 0)

        @pl.when((n >= RING + 1) & (n + RING + 1 < npair))
        def _():
            z_piece(n + RING + 1).start()

        @pl.when((n >= 0) & (n % RING == 2) & (n + RING < npair))
        def _():
            z_local(sb_of(n) - 1).start()

        return 0

    barrier = pltpu.get_barrier_semaphore()
    for dev in (at_ring(rho + 1), at_ring(rho + RING - 1), partner, across):
        pl.semaphore_signal(barrier, inc=1, device_id=dev, device_id_type=MESH_ID)
    pl.semaphore_wait(barrier, 4)

    for j in range(min(2 * RING + 2, npair)):
        z_piece(j).start()
    z_local(nsb - 1).start()
    with jax.named_scope("heads"):
        make_heads()
    lax.fori_loop(-2, npair, step, 0)

    for t in (npair - 2, npair - 1):
        for g in range(2):
            w_copy(t, g).wait_send()
    for t in (npair - 2, npair - 1):
        part_copy(t).wait_send()

        @pl.when(sends_plane(t))
        def _(t=t):
            plane_copy(t).wait_send()

    newest = min(npair - 1, AHEAD + 1)
    for t in range(max(0, npair - 8), newest + 1):

        @pl.when(t % 2 == q)
        def _(t=t):
            total_copy(t).wait_send()

    for t in range(npair - 3, npair):

        @pl.when((r == 0) & (q == 0))
        def _(t=t):
            factor_across(t).wait_send()

    for t in range(npair - 2, npair):

        @pl.when((r == 1) & (q == 0))
        def _(t=t):
            factor_over(t).wait_send()

    def out_done(c, _):
        for g in range(2):
            out_copy(g, c).wait()
        return 0

    lax.fori_loop(0, nsb, out_done, 0)


def solution(mesh):
    def local(v, t, z):
        rows, cols = v.shape
        nsb = cols // NB
        npair = nsb * RING
        hbm = pl.BlockSpec(memory_space=pltpu.MemorySpace.HBM)
        out, _ = pl.pallas_call(
            functools.partial(body, nsb),
            out_shape=(
                jax.ShapeDtypeStruct((rows, PW), F32),
                jax.ShapeDtypeStruct((2, npair, rows, NB), F32),
            ),
            in_specs=[hbm] * 3,
            out_specs=(hbm, hbm),
            scratch_shapes=[
                pltpu.VMEM((2, rows, NB), F32),
                pltpu.VMEM((2, NB, rows), F32),
                pltpu.VMEM((2, 3 * NB, rows), BF16),
                pltpu.VMEM((rows, PW), F32),
                pltpu.VMEM((3, rows, 3 * PW), BF16),
                pltpu.VMEM((8, NB, NB), F32),
                pltpu.VMEM((3, 2, NB, NB), F32),
                pltpu.VMEM((PW, 3 * PW), BF16),
                pltpu.VMEM((2, 2, NB, PW), F32),
                pltpu.VMEM((2, 2, NB, PW), F32),
                pltpu.VMEM((2, NB, NB), F32),
                pltpu.VMEM((2, NB, NB), F32),
                pltpu.VMEM((2, NB, NB), F32),
                pltpu.VMEM((2, NB, NB), F32),
                pltpu.VMEM((8, NB, NB), F32),
                pltpu.VMEM((3 * NB, PW), BF16),
                pltpu.VMEM((nsb, NB, NB), F32),
                pltpu.VMEM((nsb, NB, NB), F32),
            ],
            compiler_params=pltpu.CompilerParams(
                collective_id=0, has_side_effects=True, vmem_limit_bytes=60 * 2**20),
            name="backtransform",
        )(v, t, z)
        return out

    return jax.shard_map(local, mesh=mesh,
                         in_specs=(P("row", "col"), P("col", None, None), P(None, ("col", "row"))),
                         out_specs=P("row", "col"), check_vma=False)
```
